256 devices in a mesh: grp: 4 (over y), dev: 64 (over z, x, core).
Axes of the slice: x: 4, y: 4, z: 8, core: 2. Of those that a mesh axis runs over, the one named last changes fastest.
Arguments:
- pool_latent: bfloat16 [512, 256, 512], P(('grp', 'dev')), may hold values from -6 to 6
- pool_rope: bfloat16 [512, 64, 256], P(('grp', 'dev')), may hold values from -6 to 6
- q_nope: bfloat16 [1024, 16384], P(None, 'dev'), may hold values from -6 to 6
- q_rope: bfloat16 [1024, 8192], P(None, 'dev'), may hold values from -9 to 9
- w_uk: bfloat16 [512, 16384], P(None, 'dev'), may hold values from -0.25 to 0.25
- w_uv: bfloat16 [512, 16384], P(None, 'dev'), may hold values from -0.25 to 0.25
- w_o: bfloat16 [16384, 7168], P('dev'), may hold values from -0.046875 to 0.046875
- block_table: int32 [64, 8], replicated, may hold values from 0 to 511, as said below
- lengths: int32 [64], replicated, may hold values from 2 to 2048, as said below
- preempted: int32 [32], replicated, may hold values from 0 to 63, as said below
- assignment: int32 [32], replicated, may hold values from 0 to 3, as said below
Outputs:
- mixed: bfloat16 [1024, 7168], P('grp', 'dev')
The draws below stay inside these ranges and needn't reach their ends.
Inputs may be any that keep to these rules, and one draw needn't show every extreme that they name: `preempted`: distinct slots. `assignment`: each group receives exactly 8 requests. `block_table`: every page number 0 to 511 appears exactly once in the table; page p lies on the device with index p // 2 along grp+dev, at position p % 2 there. For every group and every index along dev, exactly 1 of the pages listed for the slots of that group's requests lie on devices with that index along dev. `lengths`: in every draw all requests of one group hold more than (7) * 256 tokens.
All inputs are finite; a program needn't handle non-finite values.
Results may differ from the reference program's by a relative error of at most 0.015.
Values may be sent and summed in bfloat16 or wider, within the bound.
No kernel may reach another device: no remote copies, remote signals or barrier semaphores. Data moves between devices by JAX's collectives and lax.ppermute only.
A program may use at most 128 MiB of HBM per device.

```python
import math
import jax
import jax.numpy as jnp
from jax import lax

D = 7168
H = 128
DC = 512
DR = 64
DN = 128
DV = 128
BLK = 256
NB = 8
REQ_G = 8
QR = 32
REQ = 32
SLOTS = 64
QROWS = 1024
GB = 64
C2 = 1
PG_DEV = 2
PAGES = 512


def layout_tables(key):
    groups = REQ // REQ_G
    columns = GB // C2
    slot_order = jax.random.permutation(jax.random.fold_in(key, 11), SLOTS).astype(jnp.int32)
    chosen = slot_order[:REQ]
    spare = slot_order[REQ:]
    group_order = jax.random.permutation(jax.random.fold_in(key, 12), REQ).astype(jnp.int32)
    assignment = group_order // REQ_G
    rank = group_order % REQ_G
    heavy = jax.random.randint(jax.random.fold_in(key, 13), (), 0, groups, dtype=jnp.int32)
    free_len = jax.random.randint(jax.random.fold_in(key, 14), (SLOTS,), 2, NB * BLK + 1, dtype=jnp.int32)
    full_len = jax.random.randint(jax.random.fold_in(key, 15), (REQ,), (NB - 1) * BLK + 1, NB * BLK + 1, dtype=jnp.int32)
    request_len = jnp.where(assignment == heavy, full_len, free_len[chosen])
    lengths = free_len.at[chosen].set(request_len)
    column_slots = groups * PG_DEV
    column_keys = jax.random.split(jax.random.fold_in(key, 16), columns)
    perms = jax.vmap(lambda k: jax.random.permutation(k, column_slots))(column_keys).astype(jnp.int32)
    row_of = perms // PG_DEV
    unit_of = perms % PG_DEV
    column_ids = jnp.arange(columns, dtype=jnp.int32)[:, None]
    page_at = (row_of * columns + column_ids) * PG_DEV + unit_of
    block_ids = jnp.arange(NB, dtype=jnp.int32)[None, :]
    k_chosen = rank[:, None] * NB + block_ids
    chosen_pages = page_at[k_chosen % columns, assignment[:, None] * C2 + k_chosen // columns]
    k_spare = jnp.arange(REQ, dtype=jnp.int32)[:, None] * NB + block_ids
    spare_pages = page_at[k_spare % columns, groups * C2 + k_spare // columns]
    table = jnp.zeros((SLOTS, NB), jnp.int32).at[chosen].set(chosen_pages).at[spare].set(spare_pages)
    return (chosen, assignment, lengths, table)


def draw_block_table(key, part):
    return layout_tables(key)[3]


def draw_lengths(key, part):
    return layout_tables(key)[2]


def draw_preempted(key, part):
    return layout_tables(key)[0]


def draw_assignment(key, part):
    return layout_tables(key)[1]


def draw_pool_rope(key, part):
    base = jnp.clip(jax.random.normal(jax.random.fold_in(key, 22), (PAGES, DR, BLK), jnp.float32), -6.0, 6.0)
    return base.astype(jnp.bfloat16)


def draw_q_rope(key, part):
    base = jnp.clip(jax.random.normal(jax.random.fold_in(key, 23), (QROWS, H * DR), jnp.float32), -8.0, 8.0)
    return base.astype(jnp.bfloat16)


def shard_levels(rng, extent, cuts, low, largest):
    def one(axis_at, shards_of):
        draws = jax.random.uniform(jax.random.fold_in(jax.random.fold_in(rng, 6), axis_at), (shards_of,), jnp.float32, low / len(cuts), largest / len(cuts))
        return jnp.repeat(jnp.exp(draws), extent[axis_at] // shards_of).reshape((-1,) + (1,) * (len(extent) - axis_at - 1))

    gain = one(*cuts[0])
    for cut in cuts[1:]:
        gain = gain * one(*cut)
    return gain


def normal_values(own_key, dims, deviation, most, cuts=(), kind=jnp.bfloat16):
    drawn = jax.random.normal(own_key, dims, jnp.float32) * deviation
    if len(cuts) > 0:
        drawn = shard_levels(own_key, dims, cuts, -0.22, 0.18) * drawn
    return jnp.clip(drawn, min=-most, max=most).astype(kind)


def setup_inputs(seed: int = 0) -> dict:
    keys = jax.random.split(jax.random.key(seed), 12)
    return {
        "pool_latent": normal_values(keys[0], (PAGES, BLK, DC), 1.0, 6.0, ((0, 256),)),
        "pool_rope": draw_pool_rope(jax.random.fold_in(keys[11], 71), 0),
        "q_nope": normal_values(keys[2], (QROWS, H * DN), 1.0, 6.0, ((1, 64),)),
        "q_rope": draw_q_rope(jax.random.fold_in(keys[11], 71), 0),
        "w_uk": normal_values(keys[4], (DC, H * DN), DC ** -0.5, 0.25, ((1, 64),)),
        "w_uv": normal_values(keys[5], (DC, H * DV), DC ** -0.5, 0.25, ((1, 64),)),
        "w_o": normal_values(keys[6], (H * DV, D), (H * DV) ** -0.5, 0.046875, ((0, 64),)),
        "block_table": draw_block_table(jax.random.fold_in(keys[11], 71), 0),
        "lengths": draw_lengths(jax.random.fold_in(keys[11], 71), 0),
        "preempted": draw_preempted(jax.random.fold_in(keys[11], 71), 0),
        "assignment": draw_assignment(jax.random.fold_in(keys[11], 71), 0),
    }


NEG = -1e+30

def reference(pool_latent, pool_rope, q_nope, q_rope, w_uk, w_uv, w_o, block_table, lengths, preempted, assignment):
    scale = 1.0 / math.sqrt(DN + DR)
    req_ids = jnp.arange(REQ, dtype=jnp.int32)
    earlier = (assignment[:, None] == assignment[None, :]) & (req_ids[None, :] < req_ids[:, None])
    rank = lax.optimization_barrier(jnp.sum(earlier.astype(jnp.int32), axis=1))
    dest = (assignment * REQ_G + rank).astype(jnp.int32)
    w_key = w_uk.astype(jnp.float32).reshape(DC, H, DN)
    w_val = w_uv.astype(jnp.float32).reshape(DC, H, DV)
    positions = jnp.arange(NB * BLK, dtype=jnp.int32)

    def one_request(index):
        slot = preempted[index]
        pages = block_table[slot]
        length = lengths[slot]
        latent = pool_latent[pages].reshape(NB * BLK, DC).astype(jnp.float32)
        rope = jnp.transpose(pool_rope[pages], (0, 2, 1)).reshape(NB * BLK, DR).astype(jnp.float32)
        start = (index * QR).astype(jnp.int32)
        query_lo = lax.dynamic_slice_in_dim(q_nope, start, QR, 0).astype(jnp.float32).reshape(QR, H, DN)
        query_hi = lax.dynamic_slice_in_dim(q_rope, start, QR, 0).astype(jnp.float32).reshape(QR, H, DR)
        q_lat = jnp.einsum('thn,chn->thc', query_lo, w_key)
        q_lat = lax.optimization_barrier(q_lat.astype(jnp.bfloat16)).astype(jnp.float32)
        score = jnp.einsum('thc,kc->thk', q_lat, latent) + jnp.einsum('thr,kr->thk', query_hi, rope)
        score = score * scale
        valid = positions[None, None, :] < length
        score = jnp.where(valid, score, NEG)
        top = lax.optimization_barrier(jnp.max(score, axis=2, keepdims=True))
        expo = jnp.where(valid, jnp.exp(score - top), 0.0)
        total = lax.optimization_barrier(jnp.sum(expo, axis=2))
        weights = lax.optimization_barrier(expo.astype(jnp.bfloat16)).astype(jnp.float32)
        o_lat = jnp.einsum('thk,kc->thc', weights, latent) / total[:, :, None]
        o_lat = lax.optimization_barrier(o_lat.astype(jnp.bfloat16)).astype(jnp.float32)
        heads = jnp.einsum('thc,chv->thv', o_lat, w_val).astype(jnp.bfloat16)
        return heads.reshape(QR, H * DV)
    heads_all = lax.map(one_request, req_ids)
    source = jnp.zeros((REQ,), jnp.int32).at[dest].set(req_ids)
    ordered = heads_all[source].reshape(QROWS, H * DV)
    return jnp.dot(ordered, w_o, preferred_element_type=jnp.float32).astype(jnp.bfloat16)
```

```python
import functools
import math

import jax
import jax.numpy as jnp
from jax import lax
from jax.experimental import pallas as pl
from jax.experimental.pallas import tpu as pltpu
from jax.sharding import Mesh
from jax.sharding import PartitionSpec as P

DR = 64
DN = 128
DV = 128
NEG = -1e30
NZ, NX, NC = 8, 4, 2
NXC = NX * NC
DEV = ("z", "x", "c")
GRP_DEV = ("grp", "z", "x", "c")
XC = ("x", "c")
SMEM = pltpu.SMEM
VMEM = pltpu.VMEM
F32 = jnp.float32
BF16 = jnp.bfloat16
NT = (((1,), (1,)), ((), ()))


def spec(space):
    return pl.BlockSpec(memory_space=space)


SEND, PICK, RANK, VALID, MEMBER, COUNT = 0, 4, 8, 16, 24, 32
META = 40


def index_kernel(ids, table, lengths, preempted, assignment, meta, *, groups, blocks, block, pages_dev):
    group, column = ids[0], ids[1]
    columns = NZ * NXC

    def clear(i, carry):
        meta[i] = 0
        return carry

    lax.fori_loop(0, META, clear, 0)

    def one_request(i, carry):
        slot = preempted[i]
        owner = assignment[i]
        length = lengths[slot]
        rank = meta[COUNT + owner]
        meta[COUNT + owner] = rank + 1
        mine = owner == group

        @pl.when(mine)
        def _():
            meta[MEMBER + rank] = i

        for b in range(blocks):
            page = table[slot, b]
            holder = page // pages_dev
            row = holder // columns
            col = holder % columns

            @pl.when((row == group) & (col == column))
            def _():
                meta[SEND + (owner - group + groups) % groups] = page % pages_dev

            @pl.when(mine & (col % NXC == column % NXC))
            def _():
                z = col // NXC
                meta[RANK + z] = rank
                meta[VALID + z] = jnp.clip(length - b * block, 0, block)

                @pl.when(col == column)
                def _():
                    meta[PICK] = (group - row + groups) % groups

        return carry

    lax.fori_loop(0, preempted.shape[0], one_request, 0)


def pack_kernel(meta, latent, rope, *rest):
    outs, sem = rest[:-1], rest[-1]
    block = latent.shape[1]
    half = rope.shape[1] // 2
    copies = []
    for k, out in enumerate(outs):
        page = meta[SEND + k]
        parts = (
            (latent.at[page], out.at[pl.ds(0, block), :]),
            (rope.at[page, pl.ds(0, half), :], out.at[pl.ds(block, half), pl.ds(0, block)]),
            (rope.at[page, pl.ds(half, half), :], out.at[pl.ds(block, half), pl.ds(block, block)]),
        )
        for j, (src, dst) in enumerate(parts):
            copies.append(pltpu.make_async_copy(src, dst, sem.at[k, j]))
    for copy in copies:
        copy.start()
    for copy in copies:
        copy.wait()


def pick_kernel(meta, *rest):
    sources, out, sem = rest[:-2], rest[-2], rest[-1]
    for k, source in enumerate(sources):

        @pl.when(meta[PICK] == k)
        def _():
            copy = pltpu.make_async_copy(source, out.at[0], sem)
            copy.start()
            copy.wait()


def query_kernel(meta, q_nope, q_rope, w_uk, out, rows):
    per_group = out.shape[0]
    q_rows = out.shape[1] // 2
    width = w_uk.shape[0]
    lane = lax.broadcasted_iota(jnp.int32, (q_rows, 2 * DR), 1)
    for r in range(per_group):
        start = pl.multiple_of(meta[MEMBER + r] * q_rows, q_rows)
        rows[r * q_rows : (r + 1) * q_rows, :] = q_nope[pl.ds(start, q_rows), :]
        hi = q_rope[pl.ds(start, q_rows), :]
        for h in range(2):
            live = (lane >= h * DR) & (lane < (h + 1) * DR)
            out[r, h * q_rows : (h + 1) * q_rows, width:] = jnp.where(live, hi, jnp.zeros_like(hi))
    for h in range(2):
        lat = lax.dot_general(
            rows[:, h * DN : (h + 1) * DN],
            w_uk[:, h * DN : (h + 1) * DN],
            NT,
            preferred_element_type=F32,
        ).astype(BF16)
        for r in range(per_group):
            out[r, h * q_rows : (h + 1) * q_rows, :width] = lat[r * q_rows : (r + 1) * q_rows, :]


def attention_kernel(meta, pages, *rest, scale):
    queries, w_uv = rest[:NXC], rest[NXC : 2 * NXC]
    keep, send, lse_keep, lse_send, acc, top, total = rest[2 * NXC :]
    per_group, heads_rows, width = acc.shape
    pair = heads_rows // NXC
    q_rows = pair // 2
    block = pages.shape[1] * 8 // 9
    half = pages.shape[1] - block

    acc[...] = jnp.zeros_like(acc)
    top[...] = jnp.full_like(top, NEG)
    total[...] = jnp.zeros_like(total)

    def one_page(z, carry):
        r = meta[RANK + z]
        valid = meta[VALID + z]

        @pl.when(valid > 0)
        def _():
            latent = pages[z, :block, :]
            tail = pages[z, block:, :]
            rope = jnp.concatenate([tail[:, :block], tail[:, block:]], axis=0)
            rope = jnp.concatenate([rope, rope], axis=0)
            query = jnp.concatenate([q[r] for q in queries], axis=0)
            score = lax.dot_general(query[:, :width], latent, NT, preferred_element_type=F32)
            score = score + jnp.dot(query[:, width:], rope, preferred_element_type=F32)
            token = lax.broadcasted_iota(jnp.int32, score.shape, 1)
            live = token < valid
            score = jnp.where(live, score * scale, NEG)
            old = top[r][:, :1]
            new = jnp.maximum(old, jnp.max(score, axis=1, keepdims=True))
            expo = jnp.where(live, jnp.exp(score - new), 0.0)
            fade = jnp.exp(old - new)
            top[r] = jnp.broadcast_to(new, top.shape[1:])
            total[r] = total[r] * fade + jnp.sum(expo, axis=1, keepdims=True)
            acc[r] = acc[r] * fade + jnp.dot(
                expo.astype(BF16), latent, preferred_element_type=F32
            )

        return carry

    lax.fori_loop(0, NZ, one_page, 0)

    for s in range(NXC):
        out, lse = (keep, lse_keep) if s % 2 == 0 else (send, lse_send)
        for h in range(2):
            lo = s * pair + h * q_rows
            rows = per_group * q_rows
            weight = total[:, lo : lo + q_rows, :].reshape(rows, total.shape[2])
            high = top[:, lo : lo + q_rows, :].reshape(rows, top.shape[2])
            value = acc[:, lo : lo + q_rows, :].reshape(rows, width)
            some = weight > 0.0
            safe = jnp.where(some, weight, 1.0)
            value = (value / safe[:, :1]).astype(BF16)
            head = jnp.dot(value, w_uv[s][:, h * DV : (h + 1) * DV], preferred_element_type=F32)
            out[s // 2, :, h * DV : (h + 1) * DV] = head.astype(BF16)
            stat = jnp.where(some, high + jnp.log(safe), NEG)
            lse[(s // 2) * 2 + h : (s // 2) * 2 + h + 1, :] = stat.T[:1, :]


def output_kernel(*refs):
    weights, heads, out = refs[:NXC], refs[NXC:-1], refs[-1]
    mixed = None
    for w, h in zip(weights, heads):
        term = lax.dot_general(w[...], h[...], NT, preferred_element_type=F32)
        mixed = term if mixed is None else mixed + term
    out[...] = mixed.astype(BF16)


def sent(x, axis, size, k):
    return lax.ppermute(x, axis, [(i, i ^ k) for i in range(size)])


def gathered(x):
    near = [x] + [sent(x, "x", NX, k) for k in range(1, NX)]
    far = [sent(a, "c", NC, 1) for a in near]
    return [a for pair in zip(near, far) for a in pair]


def over_rows(stat):
    return jnp.repeat(stat.T, DV, axis=1)


def merged(parts, stats):
    high = functools.reduce(jnp.maximum, stats)
    shares = [jnp.exp(s - high) for s in stats]
    whole = functools.reduce(jnp.add, shares)
    out = sum(over_rows(w / whole) * p.astype(F32) for w, p in zip(shares, parts))
    return out.astype(BF16), high + jnp.log(whole)


def local(
    pool_latent,
    pool_rope,
    q_nope,
    q_rope,
    w_uk,
    w_uv,
    w_o,
    block_table,
    lengths,
    preempted,
    assignment,
):
    groups = lax.axis_size("grp")
    group = lax.axis_index("grp")
    column = lax.axis_index(DEV)
    place = lax.axis_index(XC)
    pages_dev, block, width = pool_latent.shape
    requests = preempted.shape[0]
    blocks = block_table.shape[1]
    per_group = requests // groups
    query_rows = q_nope.shape[0] // requests
    rows = per_group * query_rows
    pair = 2 * query_rows
    scale = 1.0 / math.sqrt(DN + DR)
    page_rows = block + DR // 2

    ids = jnp.stack([group, column]).astype(jnp.int32)
    meta = pl.pallas_call(
        functools.partial(
            index_kernel, groups=groups, blocks=blocks, block=block, pages_dev=pages_dev
        ),
        out_shape=jax.ShapeDtypeStruct((META,), jnp.int32),
        in_specs=[spec(SMEM)] * 5,
        out_specs=spec(SMEM),
        name="index",
    )(ids, block_table, lengths, preempted, assignment)

    page_type = jax.ShapeDtypeStruct((page_rows, width), BF16)
    packed = pl.pallas_call(
        pack_kernel,
        out_shape=[page_type] * groups,
        in_specs=[spec(SMEM)] + [spec(pl.ANY)] * 2,
        out_specs=[spec(pl.ANY)] * groups,
        scratch_shapes=[pltpu.SemaphoreType.DMA((groups, 3))],
        name="pack",
    )(meta, pool_latent, pool_rope)
    arrived = [packed[0]] + [
        lax.ppermute(packed[k], "grp", [(i, (i + k) % groups) for i in range(groups)])
        for k in range(1, groups)
    ]
    own = pl.pallas_call(
        pick_kernel,
        out_shape=jax.ShapeDtypeStruct((1, page_rows, width), BF16),
        in_specs=[spec(SMEM)] + [spec(pl.ANY)] * groups,
        out_specs=spec(pl.ANY),
        scratch_shapes=[pltpu.SemaphoreType.DMA],
        name="pick",
    )(meta, *arrived)
    pages = lax.all_gather(own, "z", axis=0, tiled=True)

    query = pl.pallas_call(
        query_kernel,
        out_shape=jax.ShapeDtypeStruct((per_group, pair, width + 2 * DR), BF16),
        in_specs=[spec(SMEM)] + [spec(VMEM)] * 3,
        out_specs=spec(VMEM),
        scratch_shapes=[VMEM((rows, 2 * DN), BF16)],
        name="query",
    )(meta, q_nope, q_rope, w_uk)
    queries = gathered(query)
    values = gathered(w_uv)

    half_type = jax.ShapeDtypeStruct((NX, rows, 2 * DV), BF16)
    stat_type = jax.ShapeDtypeStruct((NXC, rows), F32)
    keep, send, lse_keep, lse_send = pl.pallas_call(
        functools.partial(attention_kernel, scale=scale),
        out_shape=[half_type, half_type, stat_type, stat_type],
        in_specs=[spec(SMEM)] + [spec(VMEM)] * (1 + 2 * NXC),
        out_specs=[spec(VMEM)] * 4,
        scratch_shapes=[
            VMEM((per_group, NXC * pair, width), F32),
            VMEM((per_group, NXC * pair, 128), F32),
            VMEM((per_group, NXC * pair, 128), F32),
        ],
        compiler_params=pltpu.CompilerParams(vmem_limit_bytes=48 << 20),
        name="attention",
    )(meta, pages, *queries, *values)

    w_cols = w_o.T.reshape(NZ, NXC, w_o.shape[1] // (NZ * NXC), w_o.shape[0])
    weights = []
    for s in range(NXC):
        part = lax.dynamic_index_in_dim(w_cols, place ^ s, 1, keepdims=False)
        part = part.reshape(-1, w_o.shape[0])
        weights.append(sent(part, XC, NXC, s) if s else part)

    got = sent(send, "c", NC, 1)
    lse_got = sent(lse_send, "c", NC, 1)
    chip = [
        merged(
            (keep[k], got[k]), (lse_keep[2 * k : 2 * k + 2], lse_got[2 * k : 2 * k + 2])
        )
        for k in range(NX)
    ]
    parts, stats = [chip[0][0]], [chip[0][1]]
    for k in range(1, NX):
        parts.append(sent(chip[k][0], "x", NX, k))
        stats.append(sent(chip[k][1], "x", NX, k))
    heads, _ = merged(parts, stats)
    all_heads = gathered(heads)

    mixed = pl.pallas_call(
        output_kernel,
        out_shape=jax.ShapeDtypeStruct((weights[0].shape[0], rows), BF16),
        in_specs=[spec(VMEM)] * (2 * NXC),
        out_specs=spec(VMEM),
        name="output",
    )(*weights, *all_heads)
    mixed = lax.all_to_all(mixed, "z", split_axis=0, concat_axis=0, tiled=True)
    mixed = mixed.reshape(NZ, -1, rows).astype(F32).sum(axis=0)
    return mixed.T.astype(BF16)


def solution(mesh):
    split = Mesh(mesh.devices.reshape(mesh.shape["grp"], NZ, NX, NC), GRP_DEV)
    return jax.shard_map(
        local,
        mesh=split,
        in_specs=(
            P(GRP_DEV, None, None),
            P(GRP_DEV, None, None),
            P(None, DEV),
            P(None, DEV),
            P(None, DEV),
            P(None, DEV),
            P(DEV, None),
            P(),
            P(),
            P(),
            P(),
        ),
        out_specs=P("grp", DEV),
        check_vma=False,
    )
```

```python
import functools
import math

import jax
import jax.numpy as jnp
from jax import lax
from jax.experimental import pallas as pl
from jax.experimental.pallas import tpu as pltpu
from jax.sharding import Mesh
from jax.sharding import PartitionSpec as P

DR = 64
DN = 128
DV = 128
NEG = -1e30
NZ, NX, NC = 8, 4, 2
NXC = NX * NC
DEV = ("z", "x", "c")
GRP_DEV = ("grp", "z", "x", "c")
XC = ("x", "c")
SMEM = pltpu.SMEM
VMEM = pltpu.VMEM
F32 = jnp.float32
BF16 = jnp.bfloat16
NT = (((1,), (1,)), ((), ()))


def spec(space):
    return pl.BlockSpec(memory_space=space)


SEND, PICK, RANK, VALID, MEMBER, COUNT, SPARE = 0, 4, 8, 16, 24, 32, 40
META = 41
TAIL = 16


def index_kernel(ids, table, lengths, preempted, assignment, meta, *, groups, blocks, block, pages_dev):
    group, column = ids[0], ids[1]
    columns = NZ * NXC
    me = group * columns + column
    place = column & (NXC - 1)
    for i in range(SPARE):
        meta[i] = 0

    def one_request(i, carry):
        slot = preempted[i]
        owner = assignment[i]
        rank = meta[COUNT + owner]
        meta[COUNT + owner] = rank + 1
        ahead = SEND + ((owner - group) & (groups - 1))
        for b in range(blocks):
            page = table[slot, b]
            holder = lax.shift_right_logical(page, pages_dev.bit_length() - 1)
            meta[jnp.where(holder == me, ahead, SPARE)] = page & (pages_dev - 1)

        @pl.when(owner == group)
        def _():
            length = lengths[slot]
            meta[MEMBER + rank] = i
            for b in range(blocks):
                holder = lax.shift_right_logical(table[slot, b], pages_dev.bit_length() - 1)
                col = holder & (columns - 1)
                row = lax.shift_right_logical(holder, columns.bit_length() - 1)
                z = lax.shift_right_logical(col, NXC.bit_length() - 1)
                near = (col & (NXC - 1)) == place
                meta[jnp.where(near, RANK + z, SPARE)] = rank
                meta[jnp.where(near, VALID + z, SPARE)] = jnp.clip(length - b * block, 0, block)
                meta[jnp.where(col == column, PICK, SPARE)] = (group - row) & (groups - 1)

        return carry

    lax.fori_loop(0, preempted.shape[0], one_request, 0)


def pack_kernel(meta, latent, rope, *outs):
    block = latent.shape[1]
    half = rope.shape[1] // 2
    for k, out in enumerate(outs):
        page = meta[SEND + k]
        out[:block, :] = latent[page]
        out[block:, :block] = rope[page, :half, :]
        out[block:, block:] = rope[page, half:, :]


def pick_kernel(meta, *rest):
    sources, out = rest[:-1], rest[-1]
    for k, source in enumerate(sources):

        @pl.when(meta[PICK] == k)
        def _():
            out[0] = source[...]


def rows_kernel(meta, q_nope, q_rope, out, *, q_rows):
    width = q_nope.shape[1]
    for r in range(out.shape[0] // q_rows):
        start = pl.multiple_of(meta[MEMBER + r] * q_rows, q_rows)
        out[r * q_rows : (r + 1) * q_rows, :width] = q_nope[pl.ds(start, q_rows), :]
        out[r * q_rows : (r + 1) * q_rows, width:] = q_rope[pl.ds(start, q_rows), :]


def query_kernel(*refs):
    rows, keys, out = refs[:NXC], refs[NXC:-1], refs[-1]
    per_group = out.shape[0]
    pair = out.shape[1] // NXC
    q_rows = pair // 2
    width = keys[0].shape[0]
    lane = lax.broadcasted_iota(jnp.int32, (rows[0].shape[0], 2 * DR), 1)
    for s in range(NXC):
        hi = rows[s][:, 2 * DN :]
        for h in range(2):
            live = (lane >= h * DR) & (lane < (h + 1) * DR)
            tail = jnp.where(live, hi, jnp.zeros_like(hi))
            lat = lax.dot_general(
                rows[s][:, h * DN : (h + 1) * DN],
                keys[s][:, h * DN : (h + 1) * DN],
                NT,
                preferred_element_type=F32,
            ).astype(BF16)
            lo = s * pair + h * q_rows
            out[:, lo : lo + q_rows, :width] = lat.reshape(per_group, q_rows, width)
            out[:, lo : lo + q_rows, width:] = tail.reshape(per_group, q_rows, 2 * DR)


def three_parts(x):
    high = x.astype(BF16).astype(F32)
    rest = x - high
    middle = rest.astype(BF16).astype(F32)
    return [high, middle, rest - middle]


def stored_stats(stats):
    rows = [p for s in stats for p in three_parts(s)]
    fill = jnp.zeros((TAIL - len(rows), rows[0].shape[1]), F32)
    return jnp.concatenate(rows + [fill], axis=0).astype(BF16)


def read_stats(tail):
    tail = tail.astype(F32)
    return [tail[3 * h : 3 * h + 1] + tail[3 * h + 1 : 3 * h + 2] + tail[3 * h + 2 : 3 * h + 3] for h in range(2)]


def attention_kernel(meta, query, pages_hbm, *rest, scale):
    values = rest[:NXC]
    keep, send, acc, top, total, pages, w_uv, sem, w_sem = rest[NXC:]
    per_group, heads_rows, width = acc.shape
    pair = heads_rows // NXC
    q_rows = pair // 2
    rows = per_group * q_rows
    block = pages.shape[1] * 8 // 9

    loads = [pltpu.make_async_copy(pages_hbm.at[z], pages.at[z], sem.at[z]) for z in range(NZ)]
    loads_w = [
        pltpu.make_async_copy(v.at[:, pl.ds(2 * DN, 2 * DV)], w_uv.at[s], w_sem.at[s])
        for s, v in enumerate(values)
    ]
    for load in loads + loads_w:
        load.start()

    acc[...] = jnp.zeros_like(acc)
    top[...] = jnp.full_like(top, NEG)
    total[...] = jnp.zeros_like(total)

    for z in range(NZ):
        r = meta[RANK + z]
        valid = meta[VALID + z]
        loads[z].wait()

        @pl.when(valid > 0)
        def _():
            latent = pages[z, :block, :]
            tail = pages[z, block:, :]
            rope = jnp.concatenate([tail[:, :block], tail[:, block:]], axis=0)
            rope = jnp.concatenate([rope, rope], axis=0)
            q = query[r]
            score = lax.dot_general(q[:, :width], latent, NT, preferred_element_type=F32)
            score = score + jnp.dot(q[:, width:], rope, preferred_element_type=F32)
            token = lax.broadcasted_iota(jnp.int32, score.shape, 1)
            live = token < valid
            score = jnp.where(live, score * scale, NEG)
            old = top[r][:, :1]
            new = jnp.maximum(old, jnp.max(score, axis=1, keepdims=True))
            expo = jnp.where(live, jnp.exp(score - new), 0.0)
            fade = jnp.exp(old - new)
            top[r] = jnp.broadcast_to(new, top.shape[1:])
            total[r] = total[r] * fade + jnp.sum(expo, axis=1, keepdims=True)
            acc[r] = acc[r] * fade + jnp.dot(
                expo.astype(BF16), latent, preferred_element_type=F32
            )

    for s in range(NXC):
        out = keep if s % 2 == 0 else send
        loads_w[s].wait()
        stats = []
        for h in range(2):
            lo = s * pair + h * q_rows
            weight = total[:, lo : lo + q_rows, :].reshape(rows, total.shape[2])
            high = top[:, lo : lo + q_rows, :].reshape(rows, top.shape[2])
            value = acc[:, lo : lo + q_rows, :].reshape(rows, width)
            some = weight > 0.0
            safe = jnp.where(some, weight, 1.0)
            value = (value / safe[:, :1]).astype(BF16)
            head = jnp.dot(value, w_uv[s, :, h * DV : (h + 1) * DV], preferred_element_type=F32)
            out[s // 2, :rows, h * DV : (h + 1) * DV] = head.astype(BF16)
            stat = jnp.where(some, high + jnp.log(safe), NEG)
            stats.append(stat.T[:1, :])
        out[s // 2, rows:, :] = stored_stats(stats)


def merge(parts, tails):
    rows = parts[0].shape[0]
    stats = [read_stats(t) for t in tails]
    high = [functools.reduce(jnp.maximum, [s[h] for s in stats]) for h in range(2)]
    shares = [[jnp.exp(s[h] - high[h]) for s in stats] for h in range(2)]
    whole = [functools.reduce(jnp.add, shares[h]) for h in range(2)]
    lines = [w / whole[h] for h in range(2) for w in shares[h]]
    fill = jnp.zeros((128 - len(lines), rows), F32)
    table = jnp.concatenate(lines + [fill], axis=0).T
    halves = []
    for h in range(2):
        sides = [p[:, h * DV : (h + 1) * DV].astype(F32) for p in parts]
        first = h * len(parts)
        halves.append(sum(table[:, first + i : first + i + 1] * p for i, p in enumerate(sides)))
    return halves, [high[h] + jnp.log(whole[h]) for h in range(2)]


def chip_kernel(keep, got, *outs):
    for k, out in enumerate(outs):
        rows = out.shape[0] - TAIL
        halves, stats = merge(
            [keep[k, :rows, :], got[k, :rows, :]], [keep[k, rows:, :], got[k, rows:, :]]
        )
        for h, half in enumerate(halves):
            out[:rows, h * DV : (h + 1) * DV] = half.astype(BF16)
        out[rows:, :] = stored_stats(stats)


def heads_kernel(*refs):
    parts, out = refs[:-1], refs[-1]
    rows = out.shape[0]
    halves, _ = merge([p[:rows, :] for p in parts], [p[rows:, :] for p in parts])
    for h, half in enumerate(halves):
        out[:, h * DV : (h + 1) * DV] = half.astype(BF16)


def output_kernel(*refs):
    weights, near, far, out = refs[:NXC], refs[NXC : NXC + NX], refs[-2], refs[-1]
    mixed = None
    for s, w in enumerate(weights):
        heads = near[s // 2][...] if s % 2 == 0 else far[s // 2]
        term = lax.dot_general(w[...], heads, NT, preferred_element_type=F32)
        mixed = term if mixed is None else mixed + term
    out[...] = mixed.astype(BF16)


def sent(x, axis, size, k):
    return lax.ppermute(x, axis, [(i, i ^ k) for i in range(size)])


def gathered(x):
    near = [x] + [sent(x, "x", NX, k) for k in range(1, NX)]
    far = [sent(a, "c", NC, 1) for a in near]
    return [a for pair in zip(near, far) for a in pair]


def local(
    pool_latent,
    pool_rope,
    q_nope,
    q_rope,
    w_uk,
    w_uv,
    w_o,
    block_table,
    lengths,
    preempted,
    assignment,
):
    groups = lax.axis_size("grp")
    group = lax.axis_index("grp")
    column = lax.axis_index(DEV)
    place = lax.axis_index(XC)
    pages_dev, block, width = pool_latent.shape
    requests = preempted.shape[0]
    blocks = block_table.shape[1]
    per_group = requests // groups
    query_rows = q_nope.shape[0] // requests
    rows = per_group * query_rows
    pair = 2 * query_rows
    scale = 1.0 / math.sqrt(DN + DR)
    page_rows = block + DR // 2

    small = pltpu.CompilerParams(vmem_limit_bytes=16 << 20)
    ids = jnp.stack([group, column]).astype(jnp.int32)
    meta = pl.pallas_call(
        functools.partial(
            index_kernel, groups=groups, blocks=blocks, block=block, pages_dev=pages_dev
        ),
        out_shape=jax.ShapeDtypeStruct((META,), jnp.int32),
        in_specs=[spec(SMEM)] * 5,
        out_specs=spec(SMEM),
        name="index",
    )(ids, block_table, lengths, preempted, assignment)

    projections = gathered(jnp.concatenate([w_uk, w_uv], axis=1))

    page_type = jax.ShapeDtypeStruct((page_rows, width), BF16)
    packed = pl.pallas_call(
        pack_kernel,
        out_shape=[page_type] * groups,
        in_specs=[spec(SMEM)] + [spec(VMEM)] * 2,
        out_specs=[spec(VMEM)] * groups,
        compiler_params=small,
        name="pack",
    )(meta, pool_latent, pool_rope)
    arrived = [packed[0]] + [
        lax.ppermute(packed[k], "grp", [(i, (i + k) % groups) for i in range(groups)])
        for k in range(1, groups)
    ]

    own_rows = pl.pallas_call(
        functools.partial(rows_kernel, q_rows=query_rows),
        out_shape=jax.ShapeDtypeStruct((rows, 2 * DN + 2 * DR), BF16),
        in_specs=[spec(SMEM)] + [spec(VMEM)] * 2,
        out_specs=spec(VMEM),
        compiler_params=small,
        name="rows",
    )(meta, q_nope, q_rope)
    all_rows = gathered(own_rows)

    w_cols = w_o.T.reshape(NZ, NXC, w_o.shape[1] // (NZ * NXC), w_o.shape[0])
    pieces = []
    for s in range(NXC):
        part = lax.dynamic_index_in_dim(w_cols, place ^ s, 1, keepdims=False)
        pieces.append(part.reshape(-1, w_o.shape[0]))
    arrived, pieces = lax.optimization_barrier((arrived, pieces))
    weights = [sent(part, XC, NXC, s) if s else part for s, part in enumerate(pieces)]

    own = pl.pallas_call(
        pick_kernel,
        out_shape=jax.ShapeDtypeStruct((1, page_rows, width), BF16),
        in_specs=[spec(SMEM)] + [spec(VMEM)] * groups,
        out_specs=spec(VMEM),
        compiler_params=small,
        name="pick",
    )(meta, *arrived)
    pages = lax.all_gather(own, "z", axis=0, tiled=True)

    query = pl.pallas_call(
        query_kernel,
        out_shape=jax.ShapeDtypeStruct((per_group, NXC * pair, width + 2 * DR), BF16),
        in_specs=[spec(VMEM)] * (2 * NXC),
        out_specs=spec(VMEM),
        compiler_params=small,
        name="query",
    )(*all_rows, *projections)

    pages, weights = lax.optimization_barrier((pages, weights))
    half_type = jax.ShapeDtypeStruct((NX, rows + TAIL, 2 * DV), BF16)
    keep, send = pl.pallas_call(
        functools.partial(attention_kernel, scale=scale),
        out_shape=[half_type, half_type],
        in_specs=[spec(SMEM), spec(VMEM)] + [spec(pl.ANY)] * (1 + NXC),
        out_specs=[spec(VMEM)] * 2,
        scratch_shapes=[
            VMEM((per_group, NXC * pair, width), F32),
            VMEM((per_group, NXC * pair, 128), F32),
            VMEM((per_group, NXC * pair, 128), F32),
            VMEM((NZ, page_rows, width), BF16),
            VMEM((NXC, width, 2 * DV), BF16),
            pltpu.SemaphoreType.DMA((NZ,)),
            pltpu.SemaphoreType.DMA((NXC,)),
        ],
        compiler_params=pltpu.CompilerParams(vmem_limit_bytes=32 << 20),
        name="attention",
    )(meta, query, pages, *projections)

    got = sent(send, "c", NC, 1)
    part_type = jax.ShapeDtypeStruct((rows + TAIL, 2 * DV), BF16)
    chip = pl.pallas_call(
        chip_kernel,
        out_shape=[part_type] * NX,
        in_specs=[spec(VMEM)] * 2,
        out_specs=[spec(VMEM)] * NX,
        compiler_params=small,
        name="chip",
    )(keep, got)
    heads = pl.pallas_call(
        heads_kernel,
        out_shape=jax.ShapeDtypeStruct((rows, 2 * DV), BF16),
        in_specs=[spec(VMEM)] * NX,
        out_specs=spec(VMEM),
        compiler_params=small,
        name="heads",
    )(chip[0], *[sent(chip[k], "x", NX, k) for k in range(1, NX)])
    near = [heads] + [sent(heads, "x", NX, k) for k in range(1, NX)]
    far = sent(jnp.stack(near), "c", NC, 1)

    mixed = pl.pallas_call(
        output_kernel,
        out_shape=jax.ShapeDtypeStruct((weights[0].shape[0], rows), BF16),
        in_specs=[spec(VMEM)] * (NXC + NX + 1),
        out_specs=spec(VMEM),
        compiler_params=small,
        name="output",
    )(*weights, *near, far)
    mixed = lax.all_to_all(mixed, "z", split_axis=0, concat_axis=0, tiled=True)
    mixed = mixed.reshape(NZ, -1, rows).astype(F32).sum(axis=0)
    return mixed.T.astype(BF16)


def solution(mesh):
    split = Mesh(mesh.devices.reshape(mesh.shape["grp"], NZ, NX, NC), GRP_DEV)
    return jax.shard_map(
        local,
        mesh=split,
        in_specs=(
            P(GRP_DEV, None, None),
            P(GRP_DEV, None, None),
            P(None, DEV),
            P(None, DEV),
            P(None, DEV),
            P(None, DEV),
            P(DEV, None),
            P(),
            P(),
            P(),
            P(),
        ),
        out_specs=P("grp", DEV),
        check_vma=False,
    )
```

```python
import functools
import math

import jax
import jax.numpy as jnp
from jax import lax
from jax.experimental import pallas as pl
from jax.experimental.pallas import tpu as pltpu
from jax.sharding import Mesh
from jax.sharding import PartitionSpec as P

DR = 64
DN = 128
DV = 128
NEG = -1e30
NZ, NX, NC = 8, 4, 2
NXC = NX * NC
DEV = ("z", "x", "c")
GRP_DEV = ("grp", "z", "x", "c")
XC = ("x", "c")
SMEM = pltpu.SMEM
VMEM = pltpu.VMEM
F32 = jnp.float32
BF16 = jnp.bfloat16
NT = (((1,), (1,)), ((), ()))


def spec(space):
    return pl.BlockSpec(memory_space=space)


SEND, PICK, PLACE, RANK, VALID, MEMBER, COUNT, SPARE = 0, 4, 5, 8, 16, 24, 32, 40
META = 41
TAIL = 16


def fill_table(meta, ids, table, lengths, preempted, assignment, *, groups, block, pages_dev):
    group, column = ids[0], ids[1]
    blocks = table.shape[0]
    columns = NZ * NXC
    me = group * columns + column
    place = column & (NXC - 1)
    plane = lax.shift_right_logical(column, NXC.bit_length() - 1)
    for i in range(SPARE):
        meta[i] = 0
    meta[PLACE] = place

    def one_request(i, carry):
        slot = preempted[i]
        owner = assignment[i]
        rank = meta[COUNT + owner]
        meta[COUNT + owner] = rank + 1
        ahead = SEND + ((owner - group) & (groups - 1))
        for b in range(blocks):
            page = table[b, slot]
            holder = lax.shift_right_logical(page, pages_dev.bit_length() - 1)
            meta[jnp.where(holder == me, ahead, SPARE)] = page & (pages_dev - 1)

        @pl.when(owner == group)
        def _():
            length = lengths[slot]
            meta[MEMBER + rank] = i
            for b in range(blocks):
                holder = lax.shift_right_logical(table[b, slot], pages_dev.bit_length() - 1)
                col = holder & (columns - 1)
                row = lax.shift_right_logical(holder, columns.bit_length() - 1)
                z = (lax.shift_right_logical(col, NXC.bit_length() - 1) - plane) & (NZ - 1)
                near = (col & (NXC - 1)) == place
                meta[jnp.where(near, RANK + z, SPARE)] = rank
                meta[jnp.where(near, VALID + z, SPARE)] = jnp.clip(length - b * block, 0, block)
                meta[jnp.where(col == column, PICK, SPARE)] = (group - row) & (groups - 1)

        return carry

    lax.fori_loop(0, preempted.shape[0], one_request, 0)


def prepare_kernel(ids, *refs, groups):
    tables_hbm, (latent_hbm, rope_hbm, q_nope, q_rope), rest = refs[:4], refs[4:8], refs[8:]
    meta, own_rows = rest[:2]
    outs = rest[2 : 2 + groups]
    table, lengths, preempted, assignment, latent, rope, sem, row_sem, table_sem = rest[2 + groups :]
    tables = (table, lengths, preempted, assignment)
    pages_dev, block, _ = latent.shape
    half = rope.shape[1] // 2
    q_rows = q_nope.shape[0] // preempted.shape[0]
    width = q_nope.shape[1]
    loads = [
        pltpu.make_async_copy(latent_hbm, latent, sem.at[0]),
        pltpu.make_async_copy(rope_hbm, rope, sem.at[1]),
    ]
    first = [
        pltpu.make_async_copy(src, dst, table_sem.at[i])
        for i, (src, dst) in enumerate(zip(tables_hbm, tables))
    ]
    for load in first + loads:
        load.start()
    for load in first:
        load.wait()
    fill_table(
        meta, ids, table, lengths, preempted, assignment,
        groups=groups, block=block, pages_dev=pages_dev,
    )
    moves = []
    for r in range(own_rows.shape[0] // q_rows):
        start = pl.multiple_of(meta[MEMBER + r] * q_rows, q_rows)
        for j, (source, lo, hi) in enumerate(((q_nope, 0, width), (q_rope, width, own_rows.shape[1]))):
            moves.append(
                pltpu.make_async_copy(
                    source.at[pl.ds(start, q_rows), :],
                    own_rows.at[pl.ds(r * q_rows, q_rows), pl.ds(lo, hi - lo)],
                    row_sem.at[r, j],
                )
            )
    for move in moves:
        move.start()
    for load in loads:
        load.wait()
    for k, out in enumerate(outs):
        page = meta[SEND + k]
        out[:block, :] = latent[page]
        out[block:, :block] = rope[page, :half, :]
        out[block:, block:] = rope[page, half:, :]
    for move in moves:
        move.wait()


def pick_kernel(meta, *rest):
    sources, out = rest[:-1], rest[-1]
    for k, source in enumerate(sources):

        @pl.when(meta[PICK] == k)
        def _():
            out[...] = source[...]


def query_kernel(meta, *refs):
    near, far, keys_hbm, out, keys, sem = refs[:NX], *refs[NX:]
    per_group = out.shape[0]
    pair = out.shape[1] // NXC
    q_rows = pair // 2
    width = keys.shape[1]
    loads = [
        pltpu.make_async_copy(
            keys_hbm.at[meta[PLACE] ^ s, :, pl.ds(0, 2 * DN)], keys.at[s], sem.at[s]
        )
        for s in range(NXC)
    ]
    for load in loads:
        load.start()
    lane = lax.broadcasted_iota(jnp.int32, (near[0].shape[0], 2 * DR), 1)
    for s in range(NXC):
        rows = near[s // 2] if s % 2 == 0 else far.at[s // 2]
        loads[s].wait()
        hi = rows[:, 2 * DN :]
        for h in range(2):
            live = (lane >= h * DR) & (lane < (h + 1) * DR)
            tail = jnp.where(live, hi, jnp.zeros_like(hi))
            lat = lax.dot_general(
                rows[:, h * DN : (h + 1) * DN],
                keys[s, :, h * DN : (h + 1) * DN],
                NT,
                preferred_element_type=F32,
            ).astype(BF16)
            lo = s * pair + h * q_rows
            out[:, lo : lo + q_rows, :width] = lat.reshape(per_group, q_rows, width)
            out[:, lo : lo + q_rows, width:] = tail.reshape(per_group, q_rows, 2 * DR)


def three_parts(x):
    high = x.astype(BF16).astype(F32)
    rest = x - high
    middle = rest.astype(BF16).astype(F32)
    return [high, middle, rest - middle]


def stored_stats(stats):
    rows = [p for s in stats for p in three_parts(s)]
    fill = jnp.zeros((TAIL - len(rows), rows[0].shape[1]), F32)
    return jnp.concatenate(rows + [fill], axis=0).astype(BF16)


def read_stats(tail):
    tail = tail.astype(F32)
    return [tail[3 * h : 3 * h + 1] + tail[3 * h + 1 : 3 * h + 2] + tail[3 * h + 2 : 3 * h + 3] for h in range(2)]


def attention_kernel(meta, query, values, *rest, scale):
    sources = rest[: NZ + 1]
    keep, send, acc, top, total, pages, w_uv, sem, w_sem = rest[NZ + 1 :]
    per_group, heads_rows, width = acc.shape
    pair = heads_rows // NXC
    q_rows = pair // 2
    rows = per_group * q_rows
    block = pages.shape[1] * 8 // 9

    middle = NZ // 2
    split = pages.shape[1] // 2
    loads = {
        z: [pltpu.make_async_copy(sources[z], pages.at[z], sem.at[z])] for z in range(NZ) if z != middle
    }
    loads[middle] = [
        pltpu.make_async_copy(sources[middle], pages.at[middle, pl.ds(0, split), :], sem.at[middle]),
        pltpu.make_async_copy(sources[NZ], pages.at[middle, pl.ds(split, split), :], sem.at[NZ]),
    ]
    order = [0] + [z for k in range(1, middle) for z in (k, NZ - k)] + [middle]
    loads_w = [
        pltpu.make_async_copy(
            values.at[meta[PLACE] ^ s, :, pl.ds(2 * DN, 2 * DV)], w_uv.at[s], w_sem.at[s]
        )
        for s in range(NXC)
    ]
    for load in [c for z in order for c in loads[z]] + loads_w:
        load.start()

    acc[...] = jnp.zeros_like(acc)
    top[...] = jnp.full_like(top, NEG)
    total[...] = jnp.zeros_like(total)

    for z in order:
        r = meta[RANK + z]
        valid = meta[VALID + z]
        for load in loads[z]:
            load.wait()

        @pl.when(valid > 0)
        def _():
            latent = pages[z, :block, :]
            tail = pages[z, block:, :]
            rope = jnp.concatenate([tail[:, :block], tail[:, block:]], axis=0)
            rope = jnp.concatenate([rope, rope], axis=0)
            q = query[r]
            score = lax.dot_general(q[:, :width], latent, NT, preferred_element_type=F32)
            score = score + jnp.dot(q[:, width:], rope, preferred_element_type=F32)
            token = lax.broadcasted_iota(jnp.int32, score.shape, 1)
            live = token < valid
            score = jnp.where(live, score * scale, NEG)
            old = top[r][:, :1]
            new = jnp.maximum(old, jnp.max(score, axis=1, keepdims=True))
            expo = jnp.where(live, jnp.exp(score - new), 0.0)
            fade = jnp.exp(old - new)
            top[r] = jnp.broadcast_to(new, top.shape[1:])
            total[r] = total[r] * fade + jnp.sum(expo, axis=1, keepdims=True)
            acc[r] = acc[r] * fade + jnp.dot(
                expo.astype(BF16), latent, preferred_element_type=F32
            )

    for s in range(NXC):
        out = keep if s % 2 == 0 else send
        loads_w[s].wait()
        stats = []
        for h in range(2):
            lo = s * pair + h * q_rows
            weight = total[:, lo : lo + q_rows, :].reshape(rows, total.shape[2])
            high = top[:, lo : lo + q_rows, :].reshape(rows, top.shape[2])
            value = acc[:, lo : lo + q_rows, :].reshape(rows, width)
            some = weight > 0.0
            safe = jnp.where(some, weight, 1.0)
            value = (value * (1.0 / safe)[:, :1]).astype(BF16)
            head = jnp.dot(value, w_uv[s, :, h * DV : (h + 1) * DV], preferred_element_type=F32)
            out[s // 2, :rows, h * DV : (h + 1) * DV] = head.astype(BF16)
            stat = jnp.where(some, high + jnp.log(safe), NEG)
            stats.append(stat.T[:1, :])
        out[s // 2, rows:, :] = stored_stats(stats)


def merge(parts, tails):
    rows = parts[0].shape[0]
    stats = [read_stats(t) for t in tails]
    high = [functools.reduce(jnp.maximum, [s[h] for s in stats]) for h in range(2)]
    shares = [[jnp.exp(s[h] - high[h]) for s in stats] for h in range(2)]
    whole = [functools.reduce(jnp.add, shares[h]) for h in range(2)]
    lines = [w / whole[h] for h in range(2) for w in shares[h]]
    fill = jnp.zeros((128 - len(lines), rows), F32)
    table = jnp.concatenate(lines + [fill], axis=0).T
    halves = []
    for h in range(2):
        sides = [p[:, h * DV : (h + 1) * DV].astype(F32) for p in parts]
        first = h * len(parts)
        halves.append(sum(table[:, first + i : first + i + 1] * p for i, p in enumerate(sides)))
    return halves, [high[h] + jnp.log(whole[h]) for h in range(2)]


def chip_kernel(keep, got, *outs):
    for k, out in enumerate(outs):
        rows = out.shape[0] - TAIL
        halves, stats = merge(
            [keep[k, :rows, :], got[k, :rows, :]], [keep[k, rows:, :], got[k, rows:, :]]
        )
        for h, half in enumerate(halves):
            out[:rows, h * DV : (h + 1) * DV] = half.astype(BF16)
        out[rows:, :] = stored_stats(stats)


def heads_kernel(*refs):
    parts, out = refs[:-1], refs[-1]
    rows = out.shape[0]
    halves, _ = merge([p[:rows, :] for p in parts], [p[rows:, :] for p in parts])
    for h, half in enumerate(halves):
        out[:, h * DV : (h + 1) * DV] = half.astype(BF16)


def output_kernel(weights, *refs):
    near, far, out = refs[:NX], refs[-2], refs[-1]
    share = weights.shape[3]
    for y in range(weights.shape[0]):
        mixed = None
        for s in range(NXC):
            heads = near[s // 2][...] if s % 2 == 0 else far[s // 2]
            term = lax.dot_general(weights[y, s % 2, s // 2], heads, NT, preferred_element_type=F32)
            mixed = term if mixed is None else mixed + term
        out[y * share : (y + 1) * share, :] = mixed.astype(BF16)


def after(x, *others):
    return lax.optimization_barrier((x, *others))[0]


def in_hbm(x):
    return pltpu.with_memory_space_constraint(x, pltpu.HBM)


def sent(x, axis, size, k):
    return lax.ppermute(x, axis, [(i, i ^ k) for i in range(size)])


def gathered(x):
    near = [x] + [sent(x, "x", NX, k) for k in range(1, NX)]
    return near, sent(jnp.stack(near), "c", NC, 1)


def shifted(x, k):
    return lax.ppermute(x, "z", [(i, (i + k) % NZ) for i in range(NZ)])


def local(
    pool_latent,
    pool_rope,
    q_nope,
    q_rope,
    w_uk,
    w_uv,
    w_o,
    block_table,
    lengths,
    preempted,
    assignment,
):
    groups = lax.axis_size("grp")
    group = lax.axis_index("grp")
    column = lax.axis_index(DEV)
    place = lax.axis_index(XC)
    pages_dev, block, width = pool_latent.shape
    requests = preempted.shape[0]
    blocks = block_table.shape[1]
    per_group = requests // groups
    query_rows = q_nope.shape[0] // requests
    rows = per_group * query_rows
    pair = 2 * query_rows
    scale = 1.0 / math.sqrt(DN + DR)
    page_rows = block + DR // 2

    small = pltpu.CompilerParams(vmem_limit_bytes=16 << 20)
    projections = in_hbm(lax.all_gather(jnp.concatenate([w_uk, w_uv], axis=1), XC, axis=0))

    ids = jnp.stack([group, column]).astype(jnp.int32)
    page_type = jax.ShapeDtypeStruct((page_rows, width), BF16)
    meta, own_rows, *packed = pl.pallas_call(
        functools.partial(prepare_kernel, groups=groups),
        out_shape=[
            jax.ShapeDtypeStruct((META,), jnp.int32),
            jax.ShapeDtypeStruct((rows, 2 * DN + 2 * DR), BF16),
        ]
        + [page_type] * groups,
        in_specs=[spec(SMEM)] + [spec(pltpu.HBM)] * 8,
        out_specs=[spec(SMEM)] + [spec(VMEM)] * (1 + groups),
        scratch_shapes=[
            SMEM(block_table.T.shape, jnp.int32),
            SMEM(lengths.shape, jnp.int32),
            SMEM(preempted.shape, jnp.int32),
            SMEM(assignment.shape, jnp.int32),
            VMEM(pool_latent.shape, BF16),
            VMEM(pool_rope.shape, BF16),
            pltpu.SemaphoreType.DMA((2,)),
            pltpu.SemaphoreType.DMA((per_group, 2)),
            pltpu.SemaphoreType.DMA((4,)),
        ],
        compiler_params=small,
        name="prepare",
    )(ids, *[in_hbm(a) for a in (block_table.T, lengths, preempted, assignment, pool_latent, pool_rope, q_nope, q_rope)])

    arrived = [packed[0]] + [
        lax.ppermute(packed[k], "grp", [(i, (i + k) % groups) for i in range(groups)])
        for k in range(1, groups)
    ]
    near_rows = [own_rows] + [sent(own_rows, "x", NX, k) for k in range(1, NX)]

    share = w_o.shape[1] // groups
    planes = NZ // groups
    w_part = lax.dynamic_slice_in_dim(w_o, group * share, share, 1)
    w_cols = w_part.T.reshape(planes, NX, NC, share // (planes * NXC), w_o.shape[0])
    pieces = [
        lax.dynamic_index_in_dim(w_cols, (place // NC) ^ k, 1, keepdims=False) for k in range(NX)
    ]
    arrived, near_rows, pieces = lax.optimization_barrier((arrived, near_rows, pieces))

    own = pl.pallas_call(
        pick_kernel,
        out_shape=page_type,
        in_specs=[spec(SMEM)] + [spec(VMEM)] * groups,
        out_specs=spec(VMEM),
        compiler_params=small,
        name="pick",
    )(meta, *arrived)

    far_rows = sent(jnp.stack(near_rows), "c", NC, 1)
    own, pieces = lax.optimization_barrier((own, pieces))
    below, above = [own], [own]
    for k in range(1, NZ // 2):
        below.append(shifted(below[-1], 1))
        above.append(shifted(above[-1], -1))
    low = shifted(below[-1][: page_rows // 2], 1)
    high = shifted(above[-1][page_rows // 2 :], -1)
    pages = [own] + above[1:] + [low] + below[:0:-1] + [high]

    columns = jnp.stack([sent(part, "x", NX, k) if k else part for k, part in enumerate(pieces)])
    columns = after(columns, above[2], below[2])
    core = place % NC
    mine = lax.dynamic_index_in_dim(columns, core, 2, keepdims=False)
    theirs = sent(lax.dynamic_index_in_dim(columns, 1 - core, 2, keepdims=False), "c", NC, 1)
    quarter = jnp.stack([mine, theirs]).reshape(NC, NX, share // NXC, w_o.shape[0])
    weights = lax.all_gather(after(quarter, above[3], below[3]), "grp", axis=0)

    query = pl.pallas_call(
        query_kernel,
        out_shape=jax.ShapeDtypeStruct((per_group, NXC * pair, width + 2 * DR), BF16),
        in_specs=[spec(SMEM)] + [spec(VMEM)] * (NX + 1) + [spec(pltpu.HBM)],
        out_specs=spec(VMEM),
        scratch_shapes=[
            VMEM((NXC, width, 2 * DN), BF16),
            pltpu.SemaphoreType.DMA((NXC,)),
        ],
        compiler_params=small,
        name="query",
    )(meta, *near_rows, far_rows, projections)

    half_type = jax.ShapeDtypeStruct((NX, rows + TAIL, 2 * DV), BF16)
    keep, send = pl.pallas_call(
        functools.partial(attention_kernel, scale=scale),
        out_shape=[half_type, half_type],
        in_specs=[spec(SMEM), spec(VMEM), spec(pltpu.HBM)] + [spec(pl.ANY)] * (1 + NZ),
        out_specs=[spec(VMEM)] * 2,
        scratch_shapes=[
            VMEM((per_group, NXC * pair, width), F32),
            VMEM((per_group, NXC * pair, 128), F32),
            VMEM((per_group, NXC * pair, 128), F32),
            VMEM((NZ, page_rows, width), BF16),
            VMEM((NXC, width, 2 * DV), BF16),
            pltpu.SemaphoreType.DMA((NZ + 1,)),
            pltpu.SemaphoreType.DMA((NXC,)),
        ],
        compiler_params=pltpu.CompilerParams(vmem_limit_bytes=32 << 20),
        name="attention",
    )(meta, query, projections, *pages)

    got = sent(send, "c", NC, 1)
    part_type = jax.ShapeDtypeStruct((rows + TAIL, 2 * DV), BF16)
    chip = pl.pallas_call(
        chip_kernel,
        out_shape=[part_type] * NX,
        in_specs=[spec(VMEM)] * 2,
        out_specs=[spec(VMEM)] * NX,
        compiler_params=small,
        name="chip",
    )(keep, got)
    heads = pl.pallas_call(
        heads_kernel,
        out_shape=jax.ShapeDtypeStruct((rows, 2 * DV), BF16),
        in_specs=[spec(VMEM)] * NX,
        out_specs=spec(VMEM),
        compiler_params=small,
        name="heads",
    )(chip[0], *[sent(chip[k], "x", NX, k) for k in range(1, NX)])
    near, far = gathered(heads)

    mixed = pl.pallas_call(
        output_kernel,
        out_shape=jax.ShapeDtypeStruct((w_o.shape[1] // NXC, rows), BF16),
        in_specs=[spec(VMEM)] * (NX + 2),
        out_specs=spec(VMEM),
        compiler_params=small,
        name="output",
    )(weights, *near, far)
    mixed = lax.all_to_all(mixed, "z", split_axis=0, concat_axis=0, tiled=True)
    mixed = mixed.reshape(NZ, -1, rows).astype(F32).sum(axis=0)
    return mixed.T.astype(BF16)


def solution(mesh):
    split = Mesh(mesh.devices.reshape(mesh.shape["grp"], NZ, NX, NC), GRP_DEV)
    return jax.shard_map(
        local,
        mesh=split,
        in_specs=(
            P(GRP_DEV, None, None),
            P(GRP_DEV, None, None),
            P(None, DEV),
            P(None, DEV),
            P(None, DEV),
            P(None, DEV),
            P(DEV, None),
            P(),
            P(),
            P(),
            P(),
        ),
        out_specs=P("grp", DEV),
        check_vma=False,
    )
```

```python
import functools
import math

import jax
import jax.numpy as jnp
from jax import lax
from jax.experimental import pallas as pl
from jax.experimental.pallas import tpu as pltpu
from jax.sharding import Mesh
from jax.sharding import PartitionSpec as P

DR = 64
DN = 128
DV = 128
NEG = -1e30
NZ, NX, NC = 8, 4, 2
NXC = NX * NC
DEV = ("z", "x", "c")
GRP_DEV = ("grp", "z", "x", "c")
XC = ("x", "c")
SMEM = pltpu.SMEM
VMEM = pltpu.VMEM
F32 = jnp.float32
BF16 = jnp.bfloat16
NT = (((1,), (1,)), ((), ()))


def spec(space):
    return pl.BlockSpec(memory_space=space)


SEND, PICK, PLACE, SPOT, RANK, VALID, MEMBER, COUNT, SPARE = 0, 4, 5, 6, 8, 16, 24, 32, 40
META = 41
TAIL = 16


def fill_table(meta, ids, table, lengths, preempted, assignment, *, groups, block, pages_dev):
    group, column = ids[0], ids[1]
    blocks = table.shape[0]
    columns = NZ * NXC
    me = group * columns + column
    place = column & (NXC - 1)
    plane = lax.shift_right_logical(column, NXC.bit_length() - 1)
    for i in range(SPARE):
        meta[i] = 0
    meta[PLACE] = place
    meta[SPOT] = lax.shift_right_logical(place, NC.bit_length() - 1)

    def one_request(i, carry):
        slot = preempted[i]
        owner = assignment[i]
        rank = meta[COUNT + owner]
        meta[COUNT + owner] = rank + 1
        ahead = SEND + ((owner - group) & (groups - 1))
        for b in range(blocks):
            page = table[b, slot]
            holder = lax.shift_right_logical(page, pages_dev.bit_length() - 1)
            meta[jnp.where(holder == me, ahead, SPARE)] = page & (pages_dev - 1)

        @pl.when(owner == group)
        def _():
            length = lengths[slot]
            meta[MEMBER + rank] = i
            for b in range(blocks):
                holder = lax.shift_right_logical(table[b, slot], pages_dev.bit_length() - 1)
                col = holder & (columns - 1)
                row = lax.shift_right_logical(holder, columns.bit_length() - 1)
                z = (lax.shift_right_logical(col, NXC.bit_length() - 1) - plane) & (NZ - 1)
                near = (col & (NXC - 1)) == place
                meta[jnp.where(near, RANK + z, SPARE)] = rank
                meta[jnp.where(near, VALID + z, SPARE)] = jnp.clip(length - b * block, 0, block)
                meta[jnp.where(col == column, PICK, SPARE)] = (group - row) & (groups - 1)

        return carry

    lax.fori_loop(0, preempted.shape[0], one_request, 0)


def prepare_kernel(ids, *refs, groups):
    tables_hbm, (latent_hbm, rope_hbm, q_nope, q_rope), rest = refs[:4], refs[4:8], refs[8:]
    meta, own_rows = rest[:2]
    outs = rest[2 : 2 + groups]
    table, lengths, preempted, assignment, latent, rope, sem, row_sem, table_sem = rest[2 + groups :]
    tables = (table, lengths, preempted, assignment)
    pages_dev, block, _ = latent.shape
    half = rope.shape[1] // 2
    q_rows = q_nope.shape[0] // preempted.shape[0]
    width = q_nope.shape[1]
    loads = [
        pltpu.make_async_copy(latent_hbm, latent, sem.at[0]),
        pltpu.make_async_copy(rope_hbm, rope, sem.at[1]),
    ]
    first = [
        pltpu.make_async_copy(src, dst, table_sem.at[i])
        for i, (src, dst) in enumerate(zip(tables_hbm, tables))
    ]
    for load in first + loads:
        load.start()
    for load in first:
        load.wait()
    fill_table(
        meta, ids, table, lengths, preempted, assignment,
        groups=groups, block=block, pages_dev=pages_dev,
    )
    moves = []
    for r in range(own_rows.shape[0] // q_rows):
        start = pl.multiple_of(meta[MEMBER + r] * q_rows, q_rows)
        for j, (source, lo, hi) in enumerate(((q_nope, 0, width), (q_rope, width, own_rows.shape[1]))):
            moves.append(
                pltpu.make_async_copy(
                    source.at[pl.ds(start, q_rows), :],
                    own_rows.at[pl.ds(r * q_rows, q_rows), pl.ds(lo, hi - lo)],
                    row_sem.at[r, j],
                )
            )
    for move in moves:
        move.start()
    for load in loads:
        load.wait()
    for k, out in enumerate(outs):
        page = meta[SEND + k]
        out[:block, :] = latent[page]
        out[block:, :block] = rope[page, :half, :]
        out[block:, block:] = rope[page, half:, :]
    for move in moves:
        move.wait()


def pick_kernel(meta, *rest):
    sources, (first, second) = rest[:-2], rest[-2:]
    half = first.shape[0]
    for k, source in enumerate(sources):

        @pl.when(meta[PICK] == k)
        def _():
            first[...] = source[:half, :]
            second[...] = source[half:, :]


def part_of(near, far, s):
    return near[s // 2] if s % 2 == 0 else far.at[s // 2]


def placed(near, far, s, meta):
    return (near, far)[s % NC].at[meta[SPOT] ^ (s // NC)]


def query_kernel(meta, *refs):
    near, far, near_source, far_source, out, keys, sem = refs[:NX], *refs[NX:]
    per_group = out.shape[0]
    pair = out.shape[1] // NXC
    q_rows = pair // 2
    width = keys.shape[1]
    loads = [
        pltpu.make_async_copy(
            placed(near_source, far_source, s, meta).at[0], keys.at[s], sem.at[s]
        )
        for s in range(NXC)
    ]
    for load in loads:
        load.start()
    lane = lax.broadcasted_iota(jnp.int32, (near[0].shape[0], 2 * DR), 1)
    for s in range(NXC):
        rows = part_of(near, far, s)
        loads[s].wait()
        hi = rows[:, 2 * DN :]
        for h in range(2):
            live = (lane >= h * DR) & (lane < (h + 1) * DR)
            tail = jnp.where(live, hi, jnp.zeros_like(hi))
            lat = lax.dot_general(
                rows[:, h * DN : (h + 1) * DN],
                keys[s, :, h * DN : (h + 1) * DN],
                NT,
                preferred_element_type=F32,
            ).astype(BF16)
            lo = s * pair + h * q_rows
            out[:, lo : lo + q_rows, :width] = lat.reshape(per_group, q_rows, width)
            out[:, lo : lo + q_rows, width:] = tail.reshape(per_group, q_rows, 2 * DR)


def three_parts(x):
    high = x.astype(BF16).astype(F32)
    rest = x - high
    middle = rest.astype(BF16).astype(F32)
    return [high, middle, rest - middle]


def stored_stats(stats):
    rows = [p for s in stats for p in three_parts(s)]
    fill = jnp.zeros((TAIL - len(rows), rows[0].shape[1]), F32)
    return jnp.concatenate(rows + [fill], axis=0).astype(BF16)


def read_stats(tail):
    tail = tail.astype(F32)
    return [tail[3 * h : 3 * h + 1] + tail[3 * h + 1 : 3 * h + 2] + tail[3 * h + 2 : 3 * h + 3] for h in range(2)]


def attention_kernel(meta, query, *rest, scale):
    near, far, firsts, seconds = *rest[:2], rest[2 : 2 + NZ], rest[2 + NZ : -9]
    keep, send, acc, top, total, pages, w_uv, sem, w_sem = rest[-9:]
    per_group, heads_rows, width = acc.shape
    pair = heads_rows // NXC
    q_rows = pair // 2
    rows = per_group * q_rows
    block = pages.shape[1] * 8 // 9

    middle = NZ // 2
    split = pages.shape[1] // 2
    loads = [
        [
            pltpu.make_async_copy(firsts[z], pages.at[z, pl.ds(0, split), :], sem.at[z, 0]),
            pltpu.make_async_copy(seconds[z], pages.at[z, pl.ds(split, split), :], sem.at[z, 1]),
        ]
        for z in range(NZ)
    ]
    order = [0] + [z for k in range(1, middle) for z in (k, NZ - k)] + [middle]
    loads_w = [
        pltpu.make_async_copy(
            placed(near, far, s, meta).at[1], w_uv.at[s], w_sem.at[s]
        )
        for s in range(NXC)
    ]
    for load in [load for z in order for load in loads[z]] + loads_w:
        load.start()

    acc[...] = jnp.zeros_like(acc)
    top[...] = jnp.full_like(top, NEG)
    total[...] = jnp.zeros_like(total)

    for z in order:
        r = meta[RANK + z]
        valid = meta[VALID + z]
        for load in loads[z]:
            load.wait()

        @pl.when(valid > 0)
        def _():
            latent = pages[z, :block, :]
            tail = pages[z, block:, :]
            rope = jnp.concatenate([tail[:, :block], tail[:, block:]], axis=0)
            rope = jnp.concatenate([rope, rope], axis=0)
            q = query[r]
            score = lax.dot_general(q[:, :width], latent, NT, preferred_element_type=F32)
            score = score + jnp.dot(q[:, width:], rope, preferred_element_type=F32)
            token = lax.broadcasted_iota(jnp.int32, score.shape, 1)
            live = token < valid
            score = jnp.where(live, score * scale, NEG)
            old = top[r][:, :1]
            new = jnp.maximum(old, jnp.max(score, axis=1, keepdims=True))
            expo = jnp.where(live, jnp.exp(score - new), 0.0)
            fade = jnp.exp(old - new)
            top[r] = jnp.broadcast_to(new, top.shape[1:])
            total[r] = total[r] * fade + jnp.sum(expo, axis=1, keepdims=True)
            acc[r] = acc[r] * fade + jnp.dot(
                expo.astype(BF16), latent, preferred_element_type=F32
            )

    for s in range(NXC):
        out = keep if s % 2 == 0 else send
        loads_w[s].wait()
        stats = []
        for h in range(2):
            lo = s * pair + h * q_rows
            weight = total[:, lo : lo + q_rows, :].reshape(rows, total.shape[2])
            high = top[:, lo : lo + q_rows, :].reshape(rows, top.shape[2])
            value = acc[:, lo : lo + q_rows, :].reshape(rows, width)
            some = weight > 0.0
            safe = jnp.where(some, weight, 1.0)
            value = (value * (1.0 / safe)[:, :1]).astype(BF16)
            head = jnp.dot(value, w_uv[s, :, h * DV : (h + 1) * DV], preferred_element_type=F32)
            out[s // 2, :rows, h * DV : (h + 1) * DV] = head.astype(BF16)
            stat = jnp.where(some, high + jnp.log(safe), NEG)
            stats.append(stat.T[:1, :])
        out[s // 2, rows:, :] = stored_stats(stats)


def merge(parts, tails):
    rows = parts[0].shape[0]
    stats = [read_stats(t) for t in tails]
    high = [functools.reduce(jnp.maximum, [s[h] for s in stats]) for h in range(2)]
    shares = [[jnp.exp(s[h] - high[h]) for s in stats] for h in range(2)]
    whole = [functools.reduce(jnp.add, shares[h]) for h in range(2)]
    lines = [w / whole[h] for h in range(2) for w in shares[h]]
    fill = jnp.zeros((128 - len(lines), rows), F32)
    table = jnp.concatenate(lines + [fill], axis=0).T
    halves = []
    for h in range(2):
        sides = [p[:, h * DV : (h + 1) * DV].astype(F32) for p in parts]
        first = h * len(parts)
        halves.append(sum(table[:, first + i : first + i + 1] * p for i, p in enumerate(sides)))
    return halves, [high[h] + jnp.log(whole[h]) for h in range(2)]


def chip_kernel(keep, got, *outs):
    for k, out in enumerate(outs):
        rows = out.shape[0] - TAIL
        halves, stats = merge(
            [keep[k, :rows, :], got[k, :rows, :]], [keep[k, rows:, :], got[k, rows:, :]]
        )
        for h, half in enumerate(halves):
            out[:rows, h * DV : (h + 1) * DV] = half.astype(BF16)
        out[rows:, :] = stored_stats(stats)


def heads_kernel(*refs):
    parts, out = refs[:-1], refs[-1]
    rows = out.shape[0]
    halves, _ = merge([p[:rows, :] for p in parts], [p[rows:, :] for p in parts])
    for h, half in enumerate(halves):
        out[:, h * DV : (h + 1) * DV] = half.astype(BF16)


def output_kernel(meta, source, *refs):
    near, far, out, weights, sem = refs[:NX], *refs[NX:]
    share = weights.shape[3]
    loads = [
        pltpu.make_async_copy(source.at[y], weights.at[y], sem.at[y])
        for y in range(weights.shape[0])
    ]
    for load in loads:
        load.start()
    for y, load in enumerate(loads):
        load.wait()
        mixed = None
        for s in range(NXC):
            heads = part_of(near, far, s)[...]
            weight = weights[y, s % NC, meta[SPOT] ^ (s // NC)]
            term = lax.dot_general(weight, heads, NT, preferred_element_type=F32)
            mixed = term if mixed is None else mixed + term
        out[y * share : (y + 1) * share, :] = mixed.astype(BF16)


def after(x, *others):
    return lax.optimization_barrier((x, *others))[0]


def in_hbm(x):
    return pltpu.with_memory_space_constraint(x, pltpu.HBM)


def sent(x, axis, size, k):
    return lax.ppermute(x, axis, [(i, i ^ k) for i in range(size)])


def gathered(x):
    near = [x] + [sent(x, "x", NX, k) for k in range(1, NX)]
    return near, sent(jnp.stack(near), "c", NC, 1)


def spread(x, axis, size):
    copies = jnp.broadcast_to(x, (size, *x.shape))
    return lax.all_to_all(copies, axis, split_axis=0, concat_axis=0)


def shifted(x, k):
    return lax.ppermute(x, "z", [(i, (i + k) % NZ) for i in range(NZ)])


def local(
    pool_latent,
    pool_rope,
    q_nope,
    q_rope,
    w_uk,
    w_uv,
    w_o,
    block_table,
    lengths,
    preempted,
    assignment,
):
    groups = lax.axis_size("grp")
    group = lax.axis_index("grp")
    column = lax.axis_index(DEV)
    place = lax.axis_index(XC)
    pages_dev, block, width = pool_latent.shape
    requests = preempted.shape[0]
    blocks = block_table.shape[1]
    per_group = requests // groups
    query_rows = q_nope.shape[0] // requests
    rows = per_group * query_rows
    pair = 2 * query_rows
    scale = 1.0 / math.sqrt(DN + DR)
    page_rows = block + DR // 2

    small = pltpu.CompilerParams(vmem_limit_bytes=16 << 20)
    copies = jnp.broadcast_to(jnp.concatenate([w_uk, w_uv]), (NX, 2 * width, w_uk.shape[1]))
    copies = copies.reshape(NX, 2, *w_uk.shape)
    near_both = lax.all_to_all(copies, "x", split_axis=0, concat_axis=0)

    ids = jnp.stack([group, column]).astype(jnp.int32)
    page_type = jax.ShapeDtypeStruct((page_rows, width), BF16)
    meta, own_rows, *packed = pl.pallas_call(
        functools.partial(prepare_kernel, groups=groups),
        out_shape=[
            jax.ShapeDtypeStruct((META,), jnp.int32),
            jax.ShapeDtypeStruct((rows, 2 * DN + 2 * DR), BF16),
        ]
        + [page_type] * groups,
        in_specs=[spec(SMEM)] + [spec(pltpu.HBM)] * 8,
        out_specs=[spec(SMEM)] + [spec(VMEM)] * (1 + groups),
        scratch_shapes=[
            SMEM(block_table.T.shape, jnp.int32),
            SMEM(lengths.shape, jnp.int32),
            SMEM(preempted.shape, jnp.int32),
            SMEM(assignment.shape, jnp.int32),
            VMEM(pool_latent.shape, BF16),
            VMEM(pool_rope.shape, BF16),
            pltpu.SemaphoreType.DMA((2,)),
            pltpu.SemaphoreType.DMA((per_group, 2)),
            pltpu.SemaphoreType.DMA((4,)),
        ],
        compiler_params=small,
        name="prepare",
    )(ids, *[in_hbm(a) for a in (block_table.T, lengths, preempted, assignment, pool_latent, pool_rope, q_nope, q_rope)])

    arrived = [packed[0]] + [
        lax.ppermute(packed[k], "grp", [(i, (i + k) % groups) for i in range(groups)])
        for k in range(1, groups)
    ]
    near_rows = [own_rows] + [sent(own_rows, "x", NX, k) for k in range(1, NX)]

    share = w_o.shape[1] // groups
    planes = NZ // groups
    w_part = lax.dynamic_slice_in_dim(w_o, group * share, share, 1)
    w_cols = w_part.T.reshape(planes, NX, NC, share // (planes * NXC), w_o.shape[0])
    pieces = w_cols.transpose(1, 2, 0, 3, 4)
    arrived, near_rows, pieces, copies = lax.optimization_barrier((arrived, near_rows, pieces, copies))

    half_page = jax.ShapeDtypeStruct((page_rows // 2, width), BF16)
    halves = pl.pallas_call(
        pick_kernel,
        out_shape=[half_page] * 2,
        in_specs=[spec(SMEM)] + [spec(VMEM)] * groups,
        out_specs=[spec(VMEM)] * 2,
        compiler_params=small,
        name="pick",
    )(meta, *arrived)

    far_rows = sent(jnp.stack(near_rows), "c", NC, 1)
    far_both = sent(near_both, "c", NC, 1)
    below, above = [halves], [halves]
    for k in range(1, NZ // 2):
        below.append([shifted(h, 1) for h in below[-1]])
        above.append([shifted(h, -1) for h in above[-1]])
    middle = [shifted(below[-1][0], 1), shifted(above[-1][1], -1)]
    pages = [halves] + above[1:] + [middle] + below[:0:-1]

    pieces = after(pieces, near_both, above[2], below[2])
    columns = lax.all_to_all(pieces, "x", split_axis=0, concat_axis=0)
    columns = after(columns, above[3], below[3])
    core = place % NC
    mine = lax.dynamic_index_in_dim(columns, core, 1, keepdims=False)
    theirs = sent(lax.dynamic_index_in_dim(columns, 1 - core, 1, keepdims=False), "c", NC, 1)
    quarter = jnp.stack([mine, theirs]).reshape(NC, NX, share // NXC, w_o.shape[0])
    weights = spread(quarter, "grp", groups)

    query = pl.pallas_call(
        query_kernel,
        out_shape=jax.ShapeDtypeStruct((per_group, NXC * pair, width + 2 * DR), BF16),
        in_specs=[spec(SMEM)] + [spec(VMEM)] * (NX + 1) + [spec(pl.ANY)] * 2,
        out_specs=spec(VMEM),
        scratch_shapes=[
            VMEM((NXC, width, 2 * DN), BF16),
            pltpu.SemaphoreType.DMA((NXC,)),
        ],
        compiler_params=small,
        name="query",
    )(meta, *near_rows, far_rows, in_hbm(near_both), in_hbm(far_both))

    half_type = jax.ShapeDtypeStruct((NX, rows + TAIL, 2 * DV), BF16)
    keep, send = pl.pallas_call(
        functools.partial(attention_kernel, scale=scale),
        out_shape=[half_type, half_type],
        in_specs=[spec(SMEM), spec(VMEM)] + [spec(pl.ANY)] * (2 + 2 * NZ),
        out_specs=[spec(VMEM)] * 2,
        scratch_shapes=[
            VMEM((per_group, NXC * pair, width), F32),
            VMEM((per_group, NXC * pair, 128), F32),
            VMEM((per_group, NXC * pair, 128), F32),
            VMEM((NZ, page_rows, width), BF16),
            VMEM((NXC, width, 2 * DV), BF16),
            pltpu.SemaphoreType.DMA((NZ, 2)),
            pltpu.SemaphoreType.DMA((NXC,)),
        ],
        compiler_params=pltpu.CompilerParams(vmem_limit_bytes=32 << 20),
        name="attention",
    )(meta, query, in_hbm(near_both), in_hbm(far_both), *[p[0] for p in pages], *[p[1] for p in pages])

    got = sent(send, "c", NC, 1)
    part_type = jax.ShapeDtypeStruct((rows + TAIL, 2 * DV), BF16)
    chip = pl.pallas_call(
        chip_kernel,
        out_shape=[part_type] * NX,
        in_specs=[spec(VMEM)] * 2,
        out_specs=[spec(VMEM)] * NX,
        compiler_params=small,
        name="chip",
    )(keep, got)
    heads = pl.pallas_call(
        heads_kernel,
        out_shape=jax.ShapeDtypeStruct((rows, 2 * DV), BF16),
        in_specs=[spec(VMEM)] * NX,
        out_specs=spec(VMEM),
        compiler_params=small,
        name="heads",
    )(chip[0], *[sent(chip[k], "x", NX, k) for k in range(1, NX)])
    near, far = gathered(heads)

    mixed = pl.pallas_call(
        output_kernel,
        out_shape=jax.ShapeDtypeStruct((w_o.shape[1] // NXC, rows), BF16),
        in_specs=[spec(SMEM), spec(pl.ANY)] + [spec(VMEM)] * (NX + 1),
        out_specs=spec(VMEM),
        scratch_shapes=[
            VMEM((groups, *quarter.shape), BF16),
            pltpu.SemaphoreType.DMA((groups,)),
        ],
        compiler_params=small,
        name="output",
    )(meta, in_hbm(weights), *near, far)
    mixed = lax.all_to_all(mixed, "z", split_axis=0, concat_axis=0, tiled=True)
    mixed = mixed.reshape(NZ, -1, rows).astype(F32).sum(axis=0)
    return mixed.T.astype(BF16)


def solution(mesh):
    split = Mesh(mesh.devices.reshape(mesh.shape["grp"], NZ, NX, NC), GRP_DEV)
    return jax.shard_map(
        local,
        mesh=split,
        in_specs=(
            P(GRP_DEV, None, None),
            P(GRP_DEV, None, None),
            P(None, DEV),
            P(None, DEV),
            P(None, DEV),
            P(None, DEV),
            P(DEV, None),
            P(),
            P(),
            P(),
            P(),
        ),
        out_specs=P("grp", DEV),
        check_vma=False,
    )
```

```python
import functools
import math

import jax
import jax.numpy as jnp
from jax import lax
from jax.experimental import pallas as pl
from jax.experimental.pallas import tpu as pltpu
from jax.sharding import Mesh
from jax.sharding import PartitionSpec as P

DR = 64
DN = 128
DV = 128
NEG = -1e30
NZ, NX, NC = 8, 4, 2
NXC = NX * NC
DEV = ("z", "x", "c")
GRP_DEV = ("grp", "z", "x", "c")
XC = ("x", "c")
SMEM = pltpu.SMEM
VMEM = pltpu.VMEM
F32 = jnp.float32
BF16 = jnp.bfloat16
NT = (((1,), (1,)), ((), ()))


def spec(space):
    return pl.BlockSpec(memory_space=space)


SEND, PICK, PLACE, SPOT, RANK, VALID, MEMBER, COUNT, SPARE = 0, 4, 5, 6, 8, 16, 24, 32, 40
META = 41
TAIL = 16


def fill_table(meta, ids, table, lengths, preempted, assignment, *, groups, block, pages_dev):
    group, column = ids[0], ids[1]
    blocks = table.shape[0]
    columns = NZ * NXC
    me = group * columns + column
    place = column & (NXC - 1)
    plane = lax.shift_right_logical(column, NXC.bit_length() - 1)
    for i in range(SPARE):
        meta[i] = 0
    meta[PLACE] = place
    meta[SPOT] = lax.shift_right_logical(place, NC.bit_length() - 1)

    def one_request(i, carry):
        slot = preempted[i]
        owner = assignment[i]
        rank = meta[COUNT + owner]
        meta[COUNT + owner] = rank + 1
        ahead = SEND + ((owner - group) & (groups - 1))
        for b in range(blocks):
            page = table[b, slot]
            holder = lax.shift_right_logical(page, pages_dev.bit_length() - 1)
            meta[jnp.where(holder == me, ahead, SPARE)] = page & (pages_dev - 1)

        @pl.when(owner == group)
        def _():
            length = lengths[slot]
            meta[MEMBER + rank] = i
            for b in range(blocks):
                holder = lax.shift_right_logical(table[b, slot], pages_dev.bit_length() - 1)
                col = holder & (columns - 1)
                row = lax.shift_right_logical(holder, columns.bit_length() - 1)
                z = (lax.shift_right_logical(col, NXC.bit_length() - 1) - plane) & (NZ - 1)
                near = (col & (NXC - 1)) == place
                meta[jnp.where(near, RANK + z, SPARE)] = rank
                meta[jnp.where(near, VALID + z, SPARE)] = jnp.clip(length - b * block, 0, block)
                meta[jnp.where(col == column, PICK, SPARE)] = (group - row) & (groups - 1)

        return carry

    lax.fori_loop(0, preempted.shape[0], one_request, 0)


def prepare_kernel(ids, *refs, groups):
    tables_hbm, (latent_hbm, rope_hbm, q_nope, q_rope, w_uk, w_uv), rest = refs[:4], refs[4:10], refs[10:]
    meta, copies = rest[:2]
    outs = rest[2 : 2 + groups]
    table, lengths, preempted, assignment, latent, rope, sem, row_sem, table_sem, w_sem = rest[2 + groups :]
    tables = (table, lengths, preempted, assignment)
    pages_dev, block, _ = latent.shape
    half = rope.shape[1] // 2
    q_rows = q_nope.shape[0] // preempted.shape[0]
    depth = w_uk.shape[0]
    queries = copies.shape[1] - 4 * depth
    rows = queries // 3
    for_all = [
        pltpu.make_async_copy(
            w.at[:, pl.ds(h * DN, DN)],
            copies.at[k, pl.ds(queries + (2 * i + h) * depth, depth), :],
            w_sem.at[k, 2 * i + h],
        )
        for i, w in enumerate((w_uk, w_uv))
        for h in range(2)
        for k in range(copies.shape[0])
    ]
    loads = [
        pltpu.make_async_copy(latent_hbm, latent, sem.at[0]),
        pltpu.make_async_copy(rope_hbm, rope, sem.at[1]),
    ]
    first = [
        pltpu.make_async_copy(src, dst, table_sem.at[i])
        for i, (src, dst) in enumerate(zip(tables_hbm, tables))
    ]
    for load in first + loads + for_all:
        load.start()
    for load in first:
        load.wait()
    fill_table(
        meta, ids, table, lengths, preempted, assignment,
        groups=groups, block=block, pages_dev=pages_dev,
    )
    moves = []
    for r in range(rows // q_rows):
        start = pl.multiple_of(meta[MEMBER + r] * q_rows, q_rows)
        for j in range(3):
            source = q_rope if j == 2 else q_nope.at[:, pl.ds(j * DN, DN)]
            moves.append(
                pltpu.make_async_copy(
                    source.at[pl.ds(start, q_rows), :],
                    copies.at[0, pl.ds(j * rows + r * q_rows, q_rows), :],
                    row_sem.at[r, j],
                )
            )
    for move in moves:
        move.start()
    for load in loads:
        load.wait()
    for k, out in enumerate(outs):
        page = meta[SEND + k]
        out[:block, :] = latent[page]
        out[block:, :block] = rope[page, :half, :]
        out[block:, block:] = rope[page, half:, :]
    for move in moves:
        move.wait()
    for k in range(1, copies.shape[0]):
        copies[k, :queries, :] = copies[0, :queries, :]
    for load in for_all:
        load.wait()


def pick_kernel(meta, *rest):
    sources, (first, second) = rest[:-2], rest[-2:]
    half = first.shape[0]
    for k, source in enumerate(sources):

        @pl.when(meta[PICK] == k)
        def _():
            first[...] = source[:half, :]
            second[...] = source[half:, :]


def placed(near, far, s, meta):
    return (near, far)[s % NC].at[meta[SPOT] ^ (s // NC)]


def query_kernel(meta, near, far, out, got, sem):
    per_group = out.shape[0]
    pair = out.shape[1] // NXC
    q_rows = pair // 2
    width = out.shape[2] - 2 * DR
    rows = per_group * q_rows
    loads = [
        pltpu.make_async_copy(
            placed(near, far, s, meta).at[pl.ds(0, got.shape[1]), :], got.at[s], sem.at[s]
        )
        for s in range(NXC)
    ]
    for load in loads:
        load.start()
    lane = lax.broadcasted_iota(jnp.int32, (rows, 2 * DR), 1)
    for s in range(NXC):
        loads[s].wait()
        hi = got[s, 2 * rows : 3 * rows, :]
        for h in range(2):
            live = (lane >= h * DR) & (lane < (h + 1) * DR)
            tail = jnp.where(live, hi, jnp.zeros_like(hi))
            key = 3 * rows + h * width
            lat = lax.dot_general(
                got[s, h * rows : (h + 1) * rows, :],
                got[s, key : key + width, :],
                NT,
                preferred_element_type=F32,
            ).astype(BF16)
            lo = s * pair + h * q_rows
            out[:, lo : lo + q_rows, :width] = lat.reshape(per_group, q_rows, width)
            out[:, lo : lo + q_rows, width:] = tail.reshape(per_group, q_rows, 2 * DR)


def three_parts(x):
    high = x.astype(BF16).astype(F32)
    rest = x - high
    middle = rest.astype(BF16).astype(F32)
    return [high, middle, rest - middle]


def stored_stats(stats):
    rows = [p for s in stats for p in three_parts(s)]
    fill = jnp.zeros((TAIL - len(rows), rows[0].shape[1]), F32)
    return jnp.concatenate(rows + [fill], axis=0).astype(BF16)


def read_stats(tail):
    tail = tail.astype(F32)
    return [tail[3 * h : 3 * h + 1] + tail[3 * h + 1 : 3 * h + 2] + tail[3 * h + 2 : 3 * h + 3] for h in range(2)]


def attention_kernel(meta, query, *rest, scale):
    near, far, firsts, seconds = *rest[:2], rest[2 : 2 + NZ], rest[2 + NZ : -9]
    keep, send, acc, top, total, pages, w_uv, sem, w_sem = rest[-9:]
    per_group, heads_rows, width = acc.shape
    pair = heads_rows // NXC
    q_rows = pair // 2
    rows = per_group * q_rows
    block = pages.shape[1] * 8 // 9

    middle = NZ // 2
    split = pages.shape[1] // 2
    loads = [
        [
            pltpu.make_async_copy(firsts[z], pages.at[z, pl.ds(0, split), :], sem.at[z, 0]),
            pltpu.make_async_copy(seconds[z], pages.at[z, pl.ds(split, split), :], sem.at[z, 1]),
        ]
        for z in range(NZ)
    ]
    order = [0] + [z for k in range(1, middle) for z in (k, NZ - k)] + [middle]
    loads_w = [
        pltpu.make_async_copy(
            placed(near, far, s, meta).at[pl.ds(near.shape[1] - 2 * width, 2 * width), :],
            w_uv.at[s],
            w_sem.at[s],
        )
        for s in range(NXC)
    ]
    for load in [load for z in order for load in loads[z]] + loads_w:
        load.start()

    acc[...] = jnp.zeros_like(acc)
    top[...] = jnp.full_like(top, NEG)
    total[...] = jnp.zeros_like(total)

    for z in order:
        r = meta[RANK + z]
        valid = meta[VALID + z]
        for load in loads[z]:
            load.wait()

        @pl.when(valid > 0)
        def _():
            latent = pages[z, :block, :]
            tail = pages[z, block:, :]
            rope = jnp.concatenate([tail[:, :block], tail[:, block:]], axis=0)
            rope = jnp.concatenate([rope, rope], axis=0)
            q = query[r]
            score = lax.dot_general(q[:, :width], latent, NT, preferred_element_type=F32)
            score = score + jnp.dot(q[:, width:], rope, preferred_element_type=F32)
            token = lax.broadcasted_iota(jnp.int32, score.shape, 1)
            live = token < valid
            score = jnp.where(live, score * scale, NEG)
            old = top[r][:, :1]
            new = jnp.maximum(old, jnp.max(score, axis=1, keepdims=True))
            expo = jnp.where(live, jnp.exp(score - new), 0.0)
            fade = jnp.exp(old - new)
            top[r] = jnp.broadcast_to(new, top.shape[1:])
            total[r] = total[r] * fade + jnp.sum(expo, axis=1, keepdims=True)
            acc[r] = acc[r] * fade + jnp.dot(
                expo.astype(BF16), latent, preferred_element_type=F32
            )

    for s in range(NXC):
        out = keep if s % 2 == 0 else send
        loads_w[s].wait()
        stats = []
        for h in range(2):
            lo = s * pair + h * q_rows
            weight = total[:, lo : lo + q_rows, :].reshape(rows, total.shape[2])
            high = top[:, lo : lo + q_rows, :].reshape(rows, top.shape[2])
            value = acc[:, lo : lo + q_rows, :].reshape(rows, width)
            some = weight > 0.0
            safe = jnp.where(some, weight, 1.0)
            value = (value * (1.0 / safe)[:, :1]).astype(BF16)
            head = jnp.dot(value, w_uv[s, h * width : (h + 1) * width, :], preferred_element_type=F32)
            out[s // 2, :rows, h * DV : (h + 1) * DV] = head.astype(BF16)
            stat = jnp.where(some, high + jnp.log(safe), NEG)
            stats.append(stat.T[:1, :])
        out[s // 2, rows:, :] = stored_stats(stats)


def merge(parts, tails):
    rows = parts[0].shape[0]
    stats = [read_stats(t) for t in tails]
    high = [functools.reduce(jnp.maximum, [s[h] for s in stats]) for h in range(2)]
    shares = [[jnp.exp(s[h] - high[h]) for s in stats] for h in range(2)]
    whole = [functools.reduce(jnp.add, shares[h]) for h in range(2)]
    lines = [w / whole[h] for h in range(2) for w in shares[h]]
    fill = jnp.zeros((128 - len(lines), rows), F32)
    table = jnp.concatenate(lines + [fill], axis=0).T
    halves = []
    for h in range(2):
        sides = [p[:, h * DV : (h + 1) * DV].astype(F32) for p in parts]
        first = h * len(parts)
        halves.append(sum(table[:, first + i : first + i + 1] * p for i, p in enumerate(sides)))
    return halves, [high[h] + jnp.log(whole[h]) for h in range(2)]


def chip_kernel(keep, got, *outs):
    for k, out in enumerate(outs):
        rows = out.shape[0] - TAIL
        halves, stats = merge(
            [keep[k, :rows, :], got[k, :rows, :]], [keep[k, rows:, :], got[k, rows:, :]]
        )
        for h, half in enumerate(halves):
            out[:rows, h * DV : (h + 1) * DV] = half.astype(BF16)
        out[rows:, :] = stored_stats(stats)


def heads_kernel(*refs):
    parts, out = refs[:-1], refs[-1]
    rows = out.shape[0]
    halves, _ = merge([p[:rows, :] for p in parts], [p[rows:, :] for p in parts])
    for h, half in enumerate(halves):
        out[:, h * DV : (h + 1) * DV] = half.astype(BF16)


def columns_kernel(meta, w_hbm, mine, theirs, wide, tall, sem):
    load = pltpu.make_async_copy(w_hbm, wide, sem)
    load.start()
    load.wait()
    step = 256
    for i in range(wide.shape[1] // step):
        tall[i * step : (i + 1) * step, :] = wide[:, i * step : (i + 1) * step].T
    share = mine.shape[2]
    core = meta[PLACE] & (NC - 1)
    for x in range(NX):
        for z in range(NZ):
            at = ((z * NX + x) * NC) * share
            for c, (own, other) in enumerate(((mine, theirs), (theirs, mine))):

                @pl.when(core == c)
                def _():
                    own[x, z] = tall[at : at + share, :]
                    other[x, z] = tall[at + share : at + 2 * share, :]


def output_kernel(mine_hbm, theirs_hbm, near, far, out, mine, theirs, sem):
    loads = []
    for i, (src, dst) in enumerate(((mine_hbm, mine), (theirs_hbm, theirs))):
        for x in range(NX):
            loads.append(pltpu.make_async_copy(src.at[x], dst.at[x], sem.at[i, x]))
    for load in loads:
        load.start()
    share = mine.shape[2]
    for x in range(NX):
        loads[x].wait()
        loads[NX + x].wait()
        for z in range(0, NZ, 2):
            first = mine[x, z : z + 2].reshape(2 * share, -1)
            second = theirs[x, z : z + 2].reshape(2 * share, -1)
            mixed = lax.dot_general(first, near[...], NT, preferred_element_type=F32)
            mixed = mixed + lax.dot_general(second, far[...], NT, preferred_element_type=F32)
            out[x, z : z + 2] = mixed.astype(BF16).reshape(2, share, -1)


def after(x, *others):
    return lax.optimization_barrier((x, *others))[0]


def in_hbm(x):
    return pltpu.with_memory_space_constraint(x, pltpu.HBM)


def sent(x, axis, size, k):
    return lax.ppermute(x, axis, [(i, i ^ k) for i in range(size)])


def shifted(x, k):
    return lax.ppermute(x, "z", [(i, (i + k) % NZ) for i in range(NZ)])


def local(
    pool_latent,
    pool_rope,
    q_nope,
    q_rope,
    w_uk,
    w_uv,
    w_o,
    block_table,
    lengths,
    preempted,
    assignment,
):
    groups = lax.axis_size("grp")
    group = lax.axis_index("grp")
    column = lax.axis_index(DEV)
    place = lax.axis_index(XC)
    pages_dev, block, width = pool_latent.shape
    requests = preempted.shape[0]
    blocks = block_table.shape[1]
    per_group = requests // groups
    query_rows = q_nope.shape[0] // requests
    rows = per_group * query_rows
    pair = 2 * query_rows
    scale = 1.0 / math.sqrt(DN + DR)
    page_rows = block + DR // 2

    small = pltpu.CompilerParams(vmem_limit_bytes=16 << 20)
    ids = jnp.stack([group, column]).astype(jnp.int32)
    page_type = jax.ShapeDtypeStruct((page_rows, width), BF16)
    meta, copies, *packed = pl.pallas_call(
        functools.partial(prepare_kernel, groups=groups),
        out_shape=[
            jax.ShapeDtypeStruct((META,), jnp.int32),
            jax.ShapeDtypeStruct((NX, 3 * rows + 4 * width, DN), BF16),
        ]
        + [page_type] * groups,
        in_specs=[spec(SMEM)] + [spec(pltpu.HBM)] * 10,
        out_specs=[spec(SMEM)] + [spec(VMEM)] * (1 + groups),
        scratch_shapes=[
            SMEM(block_table.T.shape, jnp.int32),
            SMEM(lengths.shape, jnp.int32),
            SMEM(preempted.shape, jnp.int32),
            SMEM(assignment.shape, jnp.int32),
            VMEM(pool_latent.shape, BF16),
            VMEM(pool_rope.shape, BF16),
            pltpu.SemaphoreType.DMA((2,)),
            pltpu.SemaphoreType.DMA((per_group, 3)),
            pltpu.SemaphoreType.DMA((4,)),
            pltpu.SemaphoreType.DMA((NX, 4)),
        ],
        compiler_params=small,
        name="prepare",
    )(ids, *[in_hbm(a) for a in (block_table.T, lengths, preempted, assignment, pool_latent, pool_rope, q_nope, q_rope, w_uk, w_uv)])

    arrived = [packed[0]] + [
        lax.ppermute(packed[k], "grp", [(i, (i + k) % groups) for i in range(groups)])
        for k in range(1, groups)
    ]
    near_x = lax.all_to_all(copies, "x", split_axis=0, concat_axis=0)

    share = w_o.shape[1] // (NZ * NXC)
    column_type = jax.ShapeDtypeStruct((NX, NZ, share, w_o.shape[0]), BF16)
    mine, other = pl.pallas_call(
        columns_kernel,
        out_shape=[column_type] * 2,
        in_specs=[spec(SMEM), spec(pltpu.HBM)],
        out_specs=[spec(VMEM)] * 2,
        scratch_shapes=[
            VMEM(w_o.shape, BF16),
            VMEM(w_o.shape[::-1], BF16),
            pltpu.SemaphoreType.DMA,
        ],
        compiler_params=pltpu.CompilerParams(vmem_limit_bytes=24 << 20),
        name="columns",
    )(meta, in_hbm(w_o))
    arrived, mine, other = lax.optimization_barrier((arrived, mine, other))

    half_page = jax.ShapeDtypeStruct((page_rows // 2, width), BF16)
    halves = pl.pallas_call(
        pick_kernel,
        out_shape=[half_page] * 2,
        in_specs=[spec(SMEM)] + [spec(VMEM)] * groups,
        out_specs=[spec(VMEM)] * 2,
        compiler_params=small,
        name="pick",
    )(meta, *arrived)

    below, above = [halves], [halves]
    for k in range(1, NZ // 2):
        below.append([shifted(h, 1) for h in below[-1]])
        above.append([shifted(h, -1) for h in above[-1]])
    middle = [shifted(below[-1][0], 1), shifted(above[-1][1], -1)]
    pages = [halves] + above[1:] + [middle] + below[:0:-1]

    theirs = sent(after(other, above[2], below[2]), "c", NC, 1)
    far_x = sent(after(near_x, above[3], below[3]), "c", NC, 1)

    query = pl.pallas_call(
        query_kernel,
        out_shape=jax.ShapeDtypeStruct((per_group, NXC * pair, width + 2 * DR), BF16),
        in_specs=[spec(SMEM)] + [spec(pl.ANY)] * 2,
        out_specs=spec(VMEM),
        scratch_shapes=[
            VMEM((NXC, 3 * rows + 2 * width, DN), BF16),
            pltpu.SemaphoreType.DMA((NXC,)),
        ],
        compiler_params=small,
        name="query",
    )(meta, in_hbm(near_x), in_hbm(far_x))

    half_type = jax.ShapeDtypeStruct((NX, rows + TAIL, 2 * DV), BF16)
    keep, send = pl.pallas_call(
        functools.partial(attention_kernel, scale=scale),
        out_shape=[half_type, half_type],
        in_specs=[spec(SMEM), spec(VMEM)] + [spec(pl.ANY)] * (2 + 2 * NZ),
        out_specs=[spec(VMEM)] * 2,
        scratch_shapes=[
            VMEM((per_group, NXC * pair, width), F32),
            VMEM((per_group, NXC * pair, 128), F32),
            VMEM((per_group, NXC * pair, 128), F32),
            VMEM((NZ, page_rows, width), BF16),
            VMEM((NXC, 2 * width, DV), BF16),
            pltpu.SemaphoreType.DMA((NZ, 2)),
            pltpu.SemaphoreType.DMA((NXC,)),
        ],
        compiler_params=pltpu.CompilerParams(vmem_limit_bytes=32 << 20),
        name="attention",
    )(meta, query, in_hbm(near_x), in_hbm(far_x), *[p[0] for p in pages], *[p[1] for p in pages])

    got = sent(send, "c", NC, 1)
    part_type = jax.ShapeDtypeStruct((rows + TAIL, 2 * DV), BF16)
    chip = pl.pallas_call(
        chip_kernel,
        out_shape=[part_type] * NX,
        in_specs=[spec(VMEM)] * 2,
        out_specs=[spec(VMEM)] * NX,
        compiler_params=small,
        name="chip",
    )(keep, got)
    heads = pl.pallas_call(
        heads_kernel,
        out_shape=jax.ShapeDtypeStruct((rows, 2 * DV), BF16),
        in_specs=[spec(VMEM)] * NX,
        out_specs=spec(VMEM),
        compiler_params=small,
        name="heads",
    )(chip[0], *[sent(chip[k], "x", NX, k) for k in range(1, NX)])
    mixed = pl.pallas_call(
        output_kernel,
        out_shape=jax.ShapeDtypeStruct((NX, NZ, share, rows), BF16),
        in_specs=[spec(pl.ANY)] * 2 + [spec(VMEM)] * 2,
        out_specs=spec(VMEM),
        scratch_shapes=[
            VMEM(mine.shape, BF16),
            VMEM(mine.shape, BF16),
            pltpu.SemaphoreType.DMA((2, NX)),
        ],
        compiler_params=small,
        name="output",
    )(in_hbm(mine), in_hbm(theirs), heads, sent(heads, "c", NC, 1))
    mixed = lax.all_to_all(mixed, "x", split_axis=0, concat_axis=0)
    mixed = mixed.astype(F32).sum(axis=0).astype(BF16)
    mixed = lax.all_to_all(mixed, "z", split_axis=0, concat_axis=0, tiled=True)
    mixed = mixed.reshape(NZ, -1, rows).astype(F32).sum(axis=0)
    return mixed.T.astype(BF16)


def solution(mesh):
    split = Mesh(mesh.devices.reshape(mesh.shape["grp"], NZ, NX, NC), GRP_DEV)
    return jax.shard_map(
        local,
        mesh=split,
        in_specs=(
            P(GRP_DEV, None, None),
            P(GRP_DEV, None, None),
            P(None, DEV),
            P(None, DEV),
            P(None, DEV),
            P(None, DEV),
            P(DEV, None),
            P(),
            P(),
            P(),
            P(),
        ),
        out_specs=P("grp", DEV),
        check_vma=False,
    )
```

```python
import functools
import math

import jax
import jax.numpy as jnp
from jax import lax
from jax.experimental import pallas as pl
from jax.experimental.pallas import tpu as pltpu
from jax.sharding import Mesh
from jax.sharding import PartitionSpec as P

DR = 64
DN = 128
DV = 128
NEG = -1e30
NZ, NX, NC = 8, 4, 2
NXC = NX * NC
DEV = ("z", "x", "c")
GRP_DEV = ("grp", "z", "x", "c")
XC = ("x", "c")
SMEM = pltpu.SMEM
VMEM = pltpu.VMEM
F32 = jnp.float32
BF16 = jnp.bfloat16
NT = (((1,), (1,)), ((), ()))


def spec(space):
    return pl.BlockSpec(memory_space=space)


SEND, PICK, PLACE, SPOT, RANK, VALID, MEMBER, COUNT, SPARE = 0, 4, 5, 6, 8, 16, 24, 32, 40
META = 41
TAIL = 16


def fill_table(meta, ids, table, lengths, preempted, assignment, *, groups, block, pages_dev):
    group, column = ids[0], ids[1]
    blocks = table.shape[0]
    columns = NZ * NXC
    me = group * columns + column
    place = column & (NXC - 1)
    plane = lax.shift_right_logical(column, NXC.bit_length() - 1)
    for i in range(SPARE):
        meta[i] = 0
    meta[PLACE] = place
    meta[SPOT] = lax.shift_right_logical(place, NC.bit_length() - 1)

    def one_request(i, carry):
        slot = preempted[i]
        owner = assignment[i]
        rank = meta[COUNT + owner]
        meta[COUNT + owner] = rank + 1
        ahead = SEND + ((owner - group) & (groups - 1))
        for b in range(blocks):
            page = table[b, slot]
            holder = lax.shift_right_logical(page, pages_dev.bit_length() - 1)
            meta[jnp.where(holder == me, ahead, SPARE)] = page & (pages_dev - 1)

        @pl.when(owner == group)
        def _():
            length = lengths[slot]
            meta[MEMBER + rank] = i
            for b in range(blocks):
                holder = lax.shift_right_logical(table[b, slot], pages_dev.bit_length() - 1)
                col = holder & (columns - 1)
                row = lax.shift_right_logical(holder, columns.bit_length() - 1)
                z = (lax.shift_right_logical(col, NXC.bit_length() - 1) - plane) & (NZ - 1)
                near = (col & (NXC - 1)) == place
                meta[jnp.where(near, RANK + z, SPARE)] = rank
                meta[jnp.where(near, VALID + z, SPARE)] = jnp.clip(length - b * block, 0, block)
                meta[jnp.where(col == column, PICK, SPARE)] = (group - row) & (groups - 1)

        return carry

    lax.fori_loop(0, preempted.shape[0], one_request, 0)


def prepare_kernel(ids, *refs, groups):
    tables_hbm, (latent_hbm, rope_hbm, q_nope, q_rope, w_uk, w_uv), rest = refs[:4], refs[4:10], refs[10:]
    meta, copies = rest[:2]
    outs = rest[2 : 2 + groups]
    table, lengths, preempted, assignment, latent, rope, sem, row_sem, table_sem, w_sem = rest[2 + groups :]
    tables = (table, lengths, preempted, assignment)
    pages_dev, block, _ = latent.shape
    half = rope.shape[1] // 2
    q_rows = q_nope.shape[0] // preempted.shape[0]
    depth = w_uk.shape[0]
    queries = copies.shape[1] - 4 * depth
    rows = queries // 3
    for_all = [
        pltpu.make_async_copy(
            w.at[:, pl.ds(h * DN, DN)],
            copies.at[k, pl.ds(queries + (2 * i + h) * depth, depth), :],
            w_sem.at[k, 2 * i + h],
        )
        for i, w in enumerate((w_uk, w_uv))
        for h in range(2)
        for k in range(copies.shape[0])
    ]
    loads = [
        pltpu.make_async_copy(latent_hbm, latent, sem.at[0]),
        pltpu.make_async_copy(rope_hbm, rope, sem.at[1]),
    ]
    first = [
        pltpu.make_async_copy(src, dst, table_sem.at[i])
        for i, (src, dst) in enumerate(zip(tables_hbm, tables))
    ]
    for load in first + loads + for_all:
        load.start()
    for load in first:
        load.wait()
    fill_table(
        meta, ids, table, lengths, preempted, assignment,
        groups=groups, block=block, pages_dev=pages_dev,
    )
    moves = []
    for r in range(rows // q_rows):
        start = pl.multiple_of(meta[MEMBER + r] * q_rows, q_rows)
        for j in range(3):
            source = q_rope if j == 2 else q_nope.at[:, pl.ds(j * DN, DN)]
            moves.append(
                pltpu.make_async_copy(
                    source.at[pl.ds(start, q_rows), :],
                    copies.at[0, pl.ds(j * rows + r * q_rows, q_rows), :],
                    row_sem.at[r, j],
                )
            )
    for move in moves:
        move.start()
    for load in loads:
        load.wait()
    for k, out in enumerate(outs):
        page = meta[SEND + k]
        out[:block, :] = latent[page]
        out[block:, :block] = rope[page, :half, :]
        out[block:, block:] = rope[page, half:, :]
    for move in moves:
        move.wait()
    for k in range(1, copies.shape[0]):
        copies[k, :queries, :] = copies[0, :queries, :]
    for load in for_all:
        load.wait()


def pick_kernel(meta, *rest):
    sources, (first, second) = rest[:-2], rest[-2:]
    half = first.shape[0]
    for k, source in enumerate(sources):

        @pl.when(meta[PICK] == k)
        def _():
            first[...] = source[:half, :]
            second[...] = source[half:, :]


def placed(near, far, s, meta):
    return (near, far)[s % NC].at[meta[SPOT] ^ (s // NC)]


def query_kernel(meta, near, far, out, got, sem):
    per_group = out.shape[0]
    pair = out.shape[1] // NXC
    q_rows = pair // 2
    width = out.shape[2] - 2 * DR
    rows = per_group * q_rows
    loads = [
        pltpu.make_async_copy(
            placed(near, far, s, meta).at[pl.ds(0, got.shape[1]), :], got.at[s], sem.at[s]
        )
        for s in range(NXC)
    ]
    for load in loads:
        load.start()
    lane = lax.broadcasted_iota(jnp.int32, (rows, 2 * DR), 1)
    for s in range(NXC):
        loads[s].wait()
        hi = got[s, 2 * rows : 3 * rows, :]
        for h in range(2):
            live = (lane >= h * DR) & (lane < (h + 1) * DR)
            tail = jnp.where(live, hi, jnp.zeros_like(hi))
            key = 3 * rows + h * width
            lat = lax.dot_general(
                got[s, h * rows : (h + 1) * rows, :],
                got[s, key : key + width, :],
                NT,
                preferred_element_type=F32,
            ).astype(BF16)
            lo = s * pair + h * q_rows
            out[:, lo : lo + q_rows, :width] = lat.reshape(per_group, q_rows, width)
            out[:, lo : lo + q_rows, width:] = tail.reshape(per_group, q_rows, 2 * DR)


def three_parts(x):
    high = x.astype(BF16).astype(F32)
    rest = x - high
    middle = rest.astype(BF16).astype(F32)
    return [high, middle, rest - middle]


def stored_stats(stats):
    rows = [p for s in stats for p in three_parts(s)]
    fill = jnp.zeros((TAIL - len(rows), rows[0].shape[1]), F32)
    return jnp.concatenate(rows + [fill], axis=0).astype(BF16)


def read_stats(tail):
    tail = tail.astype(F32)
    return [tail[3 * h : 3 * h + 1] + tail[3 * h + 1 : 3 * h + 2] + tail[3 * h + 2 : 3 * h + 3] for h in range(2)]


def attention_kernel(meta, query, *rest, scale):
    near, far, firsts, seconds = *rest[:2], rest[2 : 2 + NZ], rest[2 + NZ : -9]
    keep, send, acc, top, total, pages, w_uv, sem, w_sem = rest[-9:]
    per_group, heads_rows, width = acc.shape
    pair = heads_rows // NXC
    q_rows = pair // 2
    rows = per_group * q_rows
    block = pages.shape[1] * 8 // 9

    middle = NZ // 2
    split = pages.shape[1] // 2
    loads = [
        [
            pltpu.make_async_copy(firsts[z], pages.at[z, pl.ds(0, split), :], sem.at[z, 0]),
            pltpu.make_async_copy(seconds[z], pages.at[z, pl.ds(split, split), :], sem.at[z, 1]),
        ]
        for z in range(NZ)
    ]
    order = [0] + [z for k in range(1, middle) for z in (k, NZ - k)] + [middle]
    loads_w = [
        pltpu.make_async_copy(
            placed(near, far, s, meta).at[pl.ds(near.shape[1] - 2 * width, 2 * width), :],
            w_uv.at[s],
            w_sem.at[s],
        )
        for s in range(NXC)
    ]
    for load in [load for z in order for load in loads[z]] + loads_w:
        load.start()

    acc[...] = jnp.zeros_like(acc)
    top[...] = jnp.full_like(top, NEG)
    total[...] = jnp.zeros_like(total)

    for z in order:
        r = meta[RANK + z]
        valid = meta[VALID + z]
        for load in loads[z]:
            load.wait()

        @pl.when(valid > 0)
        def _():
            latent = pages[z, :block, :]
            tail = pages[z, block:, :]
            rope = jnp.concatenate([tail[:, :block], tail[:, block:]], axis=0)
            rope = jnp.concatenate([rope, rope], axis=0)
            q = query[r]
            score = lax.dot_general(q[:, :width], latent, NT, preferred_element_type=F32)
            score = score + jnp.dot(q[:, width:], rope, preferred_element_type=F32)
            token = lax.broadcasted_iota(jnp.int32, score.shape, 1)
            live = token < valid
            score = jnp.where(live, score * scale, NEG)
            old = top[r][:, :1]
            new = jnp.maximum(old, jnp.max(score, axis=1, keepdims=True))
            expo = jnp.where(live, jnp.exp(score - new), 0.0)
            fade = jnp.exp(old - new)
            top[r] = jnp.broadcast_to(new, top.shape[1:])
            total[r] = total[r] * fade + jnp.sum(expo, axis=1, keepdims=True)
            acc[r] = acc[r] * fade + jnp.dot(
                expo.astype(BF16), latent, preferred_element_type=F32
            )

    for s in range(NXC):
        out = keep if s % 2 == 0 else send
        loads_w[s].wait()
        stats = []
        for h in range(2):
            lo = s * pair + h * q_rows
            weight = total[:, lo : lo + q_rows, :].reshape(rows, total.shape[2])
            high = top[:, lo : lo + q_rows, :].reshape(rows, top.shape[2])
            value = acc[:, lo : lo + q_rows, :].reshape(rows, width)
            some = weight > 0.0
            safe = jnp.where(some, weight, 1.0)
            value = (value * (1.0 / safe)[:, :1]).astype(BF16)
            head = jnp.dot(value, w_uv[s, h * width : (h + 1) * width, :], preferred_element_type=F32)
            out[s // 2, :rows, h * DV : (h + 1) * DV] = head.astype(BF16)
            stat = jnp.where(some, high + jnp.log(safe), NEG)
            stats.append(stat.T[:1, :])
        out[s // 2, rows:, :] = stored_stats(stats)


def merge(parts, tails):
    rows = parts[0].shape[0]
    stats = [read_stats(t) for t in tails]
    high = [functools.reduce(jnp.maximum, [s[h] for s in stats]) for h in range(2)]
    shares = [[jnp.exp(s[h] - high[h]) for s in stats] for h in range(2)]
    whole = [functools.reduce(jnp.add, shares[h]) for h in range(2)]
    lines = [w / whole[h] for h in range(2) for w in shares[h]]
    fill = jnp.zeros((128 - len(lines), rows), F32)
    table = jnp.concatenate(lines + [fill], axis=0).T
    halves = []
    for h in range(2):
        sides = [p[:, h * DV : (h + 1) * DV].astype(F32) for p in parts]
        first = h * len(parts)
        halves.append(sum(table[:, first + i : first + i + 1] * p for i, p in enumerate(sides)))
    return halves, [high[h] + jnp.log(whole[h]) for h in range(2)]


def chip_kernel(keep, got, *outs):
    for k, out in enumerate(outs):
        rows = out.shape[0] - TAIL
        halves, stats = merge(
            [keep[k, :rows, :], got[k, :rows, :]], [keep[k, rows:, :], got[k, rows:, :]]
        )
        for h, half in enumerate(halves):
            out[:rows, h * DV : (h + 1) * DV] = half.astype(BF16)
        out[rows:, :] = stored_stats(stats)


def heads_kernel(*refs):
    parts, out = refs[:-1], refs[-1]
    rows = out.shape[0]
    halves, _ = merge([p[:rows, :] for p in parts], [p[rows:, :] for p in parts])
    for h, half in enumerate(halves):
        out[:, h * DV : (h + 1) * DV] = half.astype(BF16)


def columns_kernel(w_hbm, out, wide, tall, sem):
    load = pltpu.make_async_copy(w_hbm, wide, sem)
    load.start()
    load.wait()
    step = 256
    for i in range(wide.shape[1] // step):
        tall[i * step : (i + 1) * step, :] = wide[:, i * step : (i + 1) * step].T
    share = out.shape[1] // NZ
    for z in range(NZ):
        for s in range(NXC):
            at = (z * NXC + s) * share
            out[s, z * share : (z + 1) * share, :] = tall[at : at + share, :]


def output_kernel(meta, source, *refs):
    near, far, out, weights, sem = refs[:NX], *refs[NX:]
    loads = [
        pltpu.make_async_copy(source.at[meta[PLACE] ^ s], weights.at[s], sem.at[s])
        for s in range(NXC)
    ]
    for load in loads:
        load.start()
    mixed = None
    for s, load in enumerate(loads):
        heads = near[s // NC][...] if s % NC == 0 else far[s // NC]
        load.wait()
        term = lax.dot_general(weights[s], heads, NT, preferred_element_type=F32)
        mixed = term if mixed is None else mixed + term
    out[...] = mixed.astype(BF16)


def after(x, *others):
    return lax.optimization_barrier((x, *others))[0]


def in_hbm(x):
    return pltpu.with_memory_space_constraint(x, pltpu.HBM)


def sent(x, axis, size, k):
    return lax.ppermute(x, axis, [(i, i ^ k) for i in range(size)])


def shifted(x, k):
    return lax.ppermute(x, "z", [(i, (i + k) % NZ) for i in range(NZ)])


def local(
    pool_latent,
    pool_rope,
    q_nope,
    q_rope,
    w_uk,
    w_uv,
    w_o,
    block_table,
    lengths,
    preempted,
    assignment,
):
    groups = lax.axis_size("grp")
    group = lax.axis_index("grp")
    column = lax.axis_index(DEV)
    place = lax.axis_index(XC)
    pages_dev, block, width = pool_latent.shape
    requests = preempted.shape[0]
    blocks = block_table.shape[1]
    per_group = requests // groups
    query_rows = q_nope.shape[0] // requests
    rows = per_group * query_rows
    pair = 2 * query_rows
    scale = 1.0 / math.sqrt(DN + DR)
    page_rows = block + DR // 2

    small = pltpu.CompilerParams(vmem_limit_bytes=16 << 20)
    ids = jnp.stack([group, column]).astype(jnp.int32)
    page_type = jax.ShapeDtypeStruct((page_rows, width), BF16)
    meta, copies, *packed = pl.pallas_call(
        functools.partial(prepare_kernel, groups=groups),
        out_shape=[
            jax.ShapeDtypeStruct((META,), jnp.int32),
            jax.ShapeDtypeStruct((NX, 3 * rows + 4 * width, DN), BF16),
        ]
        + [page_type] * groups,
        in_specs=[spec(SMEM)] + [spec(pltpu.HBM)] * 10,
        out_specs=[spec(SMEM)] + [spec(VMEM)] * (1 + groups),
        scratch_shapes=[
            SMEM(block_table.T.shape, jnp.int32),
            SMEM(lengths.shape, jnp.int32),
            SMEM(preempted.shape, jnp.int32),
            SMEM(assignment.shape, jnp.int32),
            VMEM(pool_latent.shape, BF16),
            VMEM(pool_rope.shape, BF16),
            pltpu.SemaphoreType.DMA((2,)),
            pltpu.SemaphoreType.DMA((per_group, 3)),
            pltpu.SemaphoreType.DMA((4,)),
            pltpu.SemaphoreType.DMA((NX, 4)),
        ],
        compiler_params=small,
        name="prepare",
    )(ids, *[in_hbm(a) for a in (block_table.T, lengths, preempted, assignment, pool_latent, pool_rope, q_nope, q_rope, w_uk, w_uv)])

    arrived = [packed[0]] + [
        lax.ppermute(packed[k], "grp", [(i, (i + k) % groups) for i in range(groups)])
        for k in range(1, groups)
    ]
    near_x = lax.all_to_all(copies, "x", split_axis=0, concat_axis=0)

    share = w_o.shape[1] // (NZ * NXC)
    w_cols = pl.pallas_call(
        columns_kernel,
        out_shape=jax.ShapeDtypeStruct((NXC, NZ * share, w_o.shape[0]), BF16),
        in_specs=[spec(pltpu.HBM)],
        out_specs=spec(VMEM),
        scratch_shapes=[
            VMEM(w_o.shape, BF16),
            VMEM(w_o.shape[::-1], BF16),
            pltpu.SemaphoreType.DMA,
        ],
        compiler_params=pltpu.CompilerParams(vmem_limit_bytes=24 << 20),
        name="columns",
    )(in_hbm(after(w_o, packed[0])))
    arrived, w_cols = lax.optimization_barrier((arrived, w_cols))

    half_page = jax.ShapeDtypeStruct((page_rows // 2, width), BF16)
    halves = pl.pallas_call(
        pick_kernel,
        out_shape=[half_page] * 2,
        in_specs=[spec(SMEM)] + [spec(VMEM)] * groups,
        out_specs=[spec(VMEM)] * 2,
        compiler_params=small,
        name="pick",
    )(meta, *arrived)

    below, above = [halves], [halves]
    for k in range(1, NZ // 2):
        below.append([shifted(h, 1) for h in below[-1]])
        above.append([shifted(h, -1) for h in above[-1]])
    middle = [shifted(below[-1][0], 1), shifted(above[-1][1], -1)]
    pages = [halves] + above[1:] + [middle] + below[:0:-1]

    far_x = sent(after(near_x, above[2], below[2]), "c", NC, 1)
    w_cols = after(w_cols, near_x, above[3], below[3])
    weights = lax.all_to_all(w_cols, XC, split_axis=0, concat_axis=0)

    query = pl.pallas_call(
        query_kernel,
        out_shape=jax.ShapeDtypeStruct((per_group, NXC * pair, width + 2 * DR), BF16),
        in_specs=[spec(SMEM)] + [spec(pl.ANY)] * 2,
        out_specs=spec(VMEM),
        scratch_shapes=[
            VMEM((NXC, 3 * rows + 2 * width, DN), BF16),
            pltpu.SemaphoreType.DMA((NXC,)),
        ],
        compiler_params=small,
        name="query",
    )(meta, in_hbm(near_x), in_hbm(far_x))

    half_type = jax.ShapeDtypeStruct((NX, rows + TAIL, 2 * DV), BF16)
    keep, send = pl.pallas_call(
        functools.partial(attention_kernel, scale=scale),
        out_shape=[half_type, half_type],
        in_specs=[spec(SMEM), spec(VMEM)] + [spec(pl.ANY)] * (2 + 2 * NZ),
        out_specs=[spec(VMEM)] * 2,
        scratch_shapes=[
            VMEM((per_group, NXC * pair, width), F32),
            VMEM((per_group, NXC * pair, 128), F32),
            VMEM((per_group, NXC * pair, 128), F32),
            VMEM((NZ, page_rows, width), BF16),
            VMEM((NXC, 2 * width, DV), BF16),
            pltpu.SemaphoreType.DMA((NZ, 2)),
            pltpu.SemaphoreType.DMA((NXC,)),
        ],
        compiler_params=pltpu.CompilerParams(vmem_limit_bytes=32 << 20),
        name="attention",
    )(meta, query, in_hbm(near_x), in_hbm(far_x), *[p[0] for p in pages], *[p[1] for p in pages])

    got = sent(send, "c", NC, 1)
    part_type = jax.ShapeDtypeStruct((rows + TAIL, 2 * DV), BF16)
    chip = pl.pallas_call(
        chip_kernel,
        out_shape=[part_type] * NX,
        in_specs=[spec(VMEM)] * 2,
        out_specs=[spec(VMEM)] * NX,
        compiler_params=small,
        name="chip",
    )(keep, got)
    heads = pl.pallas_call(
        heads_kernel,
        out_shape=jax.ShapeDtypeStruct((rows, 2 * DV), BF16),
        in_specs=[spec(VMEM)] * NX,
        out_specs=spec(VMEM),
        compiler_params=small,
        name="heads",
    )(chip[0], *[sent(chip[k], "x", NX, k) for k in range(1, NX)])
    near = [heads] + [sent(heads, "x", NX, k) for k in range(1, NX)]
    far = sent(jnp.stack(near), "c", NC, 1)
    mixed = pl.pallas_call(
        output_kernel,
        out_shape=jax.ShapeDtypeStruct((NZ * share, rows), BF16),
        in_specs=[spec(SMEM), spec(pl.ANY)] + [spec(VMEM)] * (NX + 1),
        out_specs=spec(VMEM),
        scratch_shapes=[VMEM(weights.shape, BF16), pltpu.SemaphoreType.DMA((NXC,))],
        compiler_params=small,
        name="output",
    )(meta, in_hbm(weights), *near, far)
    mixed = lax.all_to_all(mixed, "z", split_axis=0, concat_axis=0, tiled=True)
    mixed = mixed.reshape(NZ, -1, rows).astype(F32).sum(axis=0)
    return mixed.T.astype(BF16)


def solution(mesh):
    split = Mesh(mesh.devices.reshape(mesh.shape["grp"], NZ, NX, NC), GRP_DEV)
    return jax.shard_map(
        local,
        mesh=split,
        in_specs=(
            P(GRP_DEV, None, None),
            P(GRP_DEV, None, None),
            P(None, DEV),
            P(None, DEV),
            P(None, DEV),
            P(None, DEV),
            P(DEV, None),
            P(),
            P(),
            P(),
            P(),
        ),
        out_specs=P("grp", DEV),
        check_vma=False,
    )
```

```python
import functools
import math

import jax
import jax.numpy as jnp
from jax import lax
from jax.experimental import pallas as pl
from jax.experimental.pallas import tpu as pltpu
from jax.sharding import Mesh
from jax.sharding import PartitionSpec as P

DR = 64
DN = 128
DV = 128
NEG = -1e30
NZ, NX, NC = 8, 4, 2
NXC = NX * NC
DEV = ("z", "x", "c")
GRP_DEV = ("grp", "z", "x", "c")
XC = ("x", "c")
SMEM = pltpu.SMEM
VMEM = pltpu.VMEM
F32 = jnp.float32
BF16 = jnp.bfloat16
NT = (((1,), (1,)), ((), ()))


def spec(space):
    return pl.BlockSpec(memory_space=space)


SEND, PICK, PLACE, SPOT, RANK, VALID, MEMBER, COUNT, SPARE = 0, 4, 5, 6, 8, 16, 24, 32, 40
META = 41
TAIL = 16


def fill_table(meta, ids, table, lengths, preempted, assignment, *, groups, block, pages_dev):
    group, column = ids[0], ids[1]
    blocks = table.shape[0]
    columns = NZ * NXC
    me = group * columns + column
    place = column & (NXC - 1)
    plane = lax.shift_right_logical(column, NXC.bit_length() - 1)
    for i in range(SPARE):
        meta[i] = 0
    meta[PLACE] = place
    meta[SPOT] = lax.shift_right_logical(place, NC.bit_length() - 1)

    def one_request(i, carry):
        slot = preempted[i]
        owner = assignment[i]
        rank = meta[COUNT + owner]
        meta[COUNT + owner] = rank + 1
        ahead = SEND + ((owner - group) & (groups - 1))
        for b in range(blocks):
            page = table[b, slot]
            holder = lax.shift_right_logical(page, pages_dev.bit_length() - 1)
            meta[jnp.where(holder == me, ahead, SPARE)] = page & (pages_dev - 1)

        @pl.when(owner == group)
        def _():
            length = lengths[slot]
            meta[MEMBER + rank] = i
            for b in range(blocks):
                holder = lax.shift_right_logical(table[b, slot], pages_dev.bit_length() - 1)
                col = holder & (columns - 1)
                row = lax.shift_right_logical(holder, columns.bit_length() - 1)
                z = (lax.shift_right_logical(col, NXC.bit_length() - 1) - plane) & (NZ - 1)
                near = (col & (NXC - 1)) == place
                meta[jnp.where(near, RANK + z, SPARE)] = rank
                meta[jnp.where(near, VALID + z, SPARE)] = jnp.clip(length - b * block, 0, block)
                meta[jnp.where(col == column, PICK, SPARE)] = (group - row) & (groups - 1)

        return carry

    lax.fori_loop(0, preempted.shape[0], one_request, 0)


def prepare_kernel(ids, *refs, groups):
    tables_hbm, (latent_hbm, rope_hbm, q_nope, q_rope, w_uk, w_uv), rest = refs[:4], refs[4:10], refs[10:]
    meta, copies = rest[:2]
    outs = rest[2 : 2 + groups]
    table, lengths, preempted, assignment, latent, rope, sem, row_sem, table_sem, w_sem = rest[2 + groups :]
    tables = (table, lengths, preempted, assignment)
    pages_dev, block, _ = latent.shape
    half = rope.shape[1] // 2
    q_rows = q_nope.shape[0] // preempted.shape[0]
    depth = w_uk.shape[0]
    queries = copies.shape[1] - 4 * depth
    rows = queries // 3
    for_all = [
        pltpu.make_async_copy(
            w.at[:, pl.ds(h * DN, DN)],
            copies.at[k, pl.ds(queries + (2 * i + h) * depth, depth), :],
            w_sem.at[k, 2 * i + h],
        )
        for i, w in enumerate((w_uk, w_uv))
        for h in range(2)
        for k in range(copies.shape[0])
    ]
    loads = [
        pltpu.make_async_copy(latent_hbm, latent, sem.at[0]),
        pltpu.make_async_copy(rope_hbm, rope, sem.at[1]),
    ]
    first = [
        pltpu.make_async_copy(src, dst, table_sem.at[i])
        for i, (src, dst) in enumerate(zip(tables_hbm, tables))
    ]
    for load in first + loads + for_all:
        load.start()
    for load in first:
        load.wait()
    fill_table(
        meta, ids, table, lengths, preempted, assignment,
        groups=groups, block=block, pages_dev=pages_dev,
    )
    moves = []
    for r in range(rows // q_rows):
        start = pl.multiple_of(meta[MEMBER + r] * q_rows, q_rows)
        for j in range(3):
            source = q_rope if j == 2 else q_nope.at[:, pl.ds(j * DN, DN)]
            moves.append(
                pltpu.make_async_copy(
                    source.at[pl.ds(start, q_rows), :],
                    copies.at[0, pl.ds(j * rows + r * q_rows, q_rows), :],
                    row_sem.at[r, j],
                )
            )
    for move in moves:
        move.start()
    for load in loads:
        load.wait()
    for k, out in enumerate(outs):
        page = meta[SEND + k]
        out[:block, :] = latent[page]
        out[block:, :block] = rope[page, :half, :]
        out[block:, block:] = rope[page, half:, :]
    for move in moves:
        move.wait()
    for k in range(1, copies.shape[0]):
        copies[k, :queries, :] = copies[0, :queries, :]
    for load in for_all:
        load.wait()


def pick_kernel(meta, *rest):
    sources, (first, second) = rest[:-2], rest[-2:]
    half = first.shape[0]
    for k, source in enumerate(sources):

        @pl.when(meta[PICK] == k)
        def _():
            first[...] = source[:half, :]
            second[...] = source[half:, :]


def placed(near, far, s, meta):
    return (near, far)[s % NC].at[meta[SPOT] ^ (s // NC)]


def query_kernel(meta, near, far, out, got, sem):
    per_group = out.shape[0]
    pair = out.shape[1] // NXC
    q_rows = pair // 2
    width = out.shape[2] - 2 * DR
    rows = per_group * q_rows
    loads = [
        pltpu.make_async_copy(
            placed(near, far, s, meta).at[pl.ds(0, got.shape[1]), :], got.at[s], sem.at[s]
        )
        for s in range(NXC)
    ]
    for load in loads:
        load.start()
    lane = lax.broadcasted_iota(jnp.int32, (rows, 2 * DR), 1)
    for s in range(NXC):
        loads[s].wait()
        hi = got[s, 2 * rows : 3 * rows, :]
        for h in range(2):
            live = (lane >= h * DR) & (lane < (h + 1) * DR)
            tail = jnp.where(live, hi, jnp.zeros_like(hi))
            key = 3 * rows + h * width
            lat = lax.dot_general(
                got[s, h * rows : (h + 1) * rows, :],
                got[s, key : key + width, :],
                NT,
                preferred_element_type=F32,
            ).astype(BF16)
            lo = s * pair + h * q_rows
            out[:, lo : lo + q_rows, :width] = lat.reshape(per_group, q_rows, width)
            out[:, lo : lo + q_rows, width:] = tail.reshape(per_group, q_rows, 2 * DR)


def three_parts(x):
    high = x.astype(BF16).astype(F32)
    rest = x - high
    middle = rest.astype(BF16).astype(F32)
    return [high, middle, rest - middle]


def stored_stats(stats):
    rows = [p for s in stats for p in three_parts(s)]
    fill = jnp.zeros((TAIL - len(rows), rows[0].shape[1]), F32)
    return jnp.concatenate(rows + [fill], axis=0).astype(BF16)


def read_stats(tail):
    tail = tail.astype(F32)
    return [tail[3 * h : 3 * h + 1] + tail[3 * h + 1 : 3 * h + 2] + tail[3 * h + 2 : 3 * h + 3] for h in range(2)]


def attention_kernel(meta, query, *rest, scale):
    near, far, firsts, seconds = *rest[:2], rest[2 : 2 + NZ], rest[2 + NZ : -9]
    keep, send, acc, top, total, pages, w_uv, sem, w_sem = rest[-9:]
    per_group, heads_rows, width = acc.shape
    pair = heads_rows // NXC
    q_rows = pair // 2
    rows = per_group * q_rows
    block = pages.shape[1] * 8 // 9

    middle = NZ // 2
    split = pages.shape[1] // 2
    loads = [
        [
            pltpu.make_async_copy(firsts[z], pages.at[z, pl.ds(0, split), :], sem.at[z, 0]),
            pltpu.make_async_copy(seconds[z], pages.at[z, pl.ds(split, split), :], sem.at[z, 1]),
        ]
        for z in range(NZ)
    ]
    order = [0] + [z for k in range(1, middle) for z in (k, NZ - k)] + [middle]
    loads_w = [
        pltpu.make_async_copy(
            placed(near, far, s, meta).at[pl.ds(near.shape[1] - 2 * width, 2 * width), :],
            w_uv.at[s],
            w_sem.at[s],
        )
        for s in range(NXC)
    ]
    for load in [load for z in order for load in loads[z]] + loads_w:
        load.start()

    acc[...] = jnp.zeros_like(acc)
    top[...] = jnp.full_like(top, NEG)
    total[...] = jnp.zeros_like(total)

    for z in order:
        r = meta[RANK + z]
        valid = meta[VALID + z]
        for load in loads[z]:
            load.wait()

        @pl.when(valid > 0)
        def _():
            latent = pages[z, :block, :]
            tail = pages[z, block:, :]
            rope = jnp.concatenate([tail[:, :block], tail[:, block:]], axis=0)
            rope = jnp.concatenate([rope, rope], axis=0)
            q = query[r]
            score = lax.dot_general(q[:, :width], latent, NT, preferred_element_type=F32)
            score = score + jnp.dot(q[:, width:], rope, preferred_element_type=F32)
            token = lax.broadcasted_iota(jnp.int32, score.shape, 1)
            live = token < valid
            score = jnp.where(live, score * scale, NEG)
            old = top[r][:, :1]
            new = jnp.maximum(old, jnp.max(score, axis=1, keepdims=True))
            expo = jnp.where(live, jnp.exp(score - new), 0.0)
            fade = jnp.exp(old - new)
            top[r] = jnp.broadcast_to(new, top.shape[1:])
            total[r] = total[r] * fade + jnp.sum(expo, axis=1, keepdims=True)
            acc[r] = acc[r] * fade + jnp.dot(
                expo.astype(BF16), latent, preferred_element_type=F32
            )

    for s in range(NXC):
        out = keep if s % 2 == 0 else send
        loads_w[s].wait()
        stats = []
        for h in range(2):
            lo = s * pair + h * q_rows
            weight = total[:, lo : lo + q_rows, :].reshape(rows, total.shape[2])
            high = top[:, lo : lo + q_rows, :].reshape(rows, top.shape[2])
            value = acc[:, lo : lo + q_rows, :].reshape(rows, width)
            some = weight > 0.0
            safe = jnp.where(some, weight, 1.0)
            value = (value * (1.0 / safe)[:, :1]).astype(BF16)
            head = jnp.dot(value, w_uv[s, h * width : (h + 1) * width, :], preferred_element_type=F32)
            out[s // 2, :rows, h * DV : (h + 1) * DV] = head.astype(BF16)
            stat = jnp.where(some, high + jnp.log(safe), NEG)
            stats.append(stat.T[:1, :])
        out[s // 2, rows:, :] = stored_stats(stats)


def merge(parts, tails):
    rows = parts[0].shape[0]
    stats = [read_stats(t) for t in tails]
    high = [functools.reduce(jnp.maximum, [s[h] for s in stats]) for h in range(2)]
    shares = [[jnp.exp(s[h] - high[h]) for s in stats] for h in range(2)]
    whole = [functools.reduce(jnp.add, shares[h]) for h in range(2)]
    lines = [w / whole[h] for h in range(2) for w in shares[h]]
    fill = jnp.zeros((128 - len(lines), rows), F32)
    table = jnp.concatenate(lines + [fill], axis=0).T
    halves = []
    for h in range(2):
        sides = [p[:, h * DV : (h + 1) * DV].astype(F32) for p in parts]
        first = h * len(parts)
        halves.append(sum(table[:, first + i : first + i + 1] * p for i, p in enumerate(sides)))
    return halves, [high[h] + jnp.log(whole[h]) for h in range(2)]


def chip_kernel(keep, got, *outs):
    for k, out in enumerate(outs):
        rows = out.shape[0] - TAIL
        halves, stats = merge(
            [keep[k, :rows, :], got[k, :rows, :]], [keep[k, rows:, :], got[k, rows:, :]]
        )
        for h, half in enumerate(halves):
            out[:rows, h * DV : (h + 1) * DV] = half.astype(BF16)
        out[rows:, :] = stored_stats(stats)


def heads_kernel(*refs):
    parts, out = refs[:-1], refs[-1]
    rows = out.shape[0]
    halves, _ = merge([p[:rows, :] for p in parts], [p[rows:, :] for p in parts])
    for h, half in enumerate(halves):
        out[:, h * DV : (h + 1) * DV] = half.astype(BF16)


def columns_kernel(w_hbm, out, wide, tall, sem):
    load = pltpu.make_async_copy(w_hbm, wide, sem)
    load.start()
    load.wait()
    step = 256
    for i in range(wide.shape[1] // step):
        tall[i * step : (i + 1) * step, :] = wide[:, i * step : (i + 1) * step].T
    share = out.shape[1] // NZ
    for z in range(NZ):
        for s in range(NXC):
            at = (z * NXC + s) * share
            out[s, z * share : (z + 1) * share, :] = tall[at : at + share, :]


def output_kernel(meta, source, *refs):
    near, far, out, weights, sem = refs[:NX], *refs[NX:]
    loads = [
        pltpu.make_async_copy(source.at[meta[PLACE] ^ s], weights.at[s], sem.at[s])
        for s in range(NXC)
    ]
    for load in loads:
        load.start()
    mixed = None
    for s, load in enumerate(loads):
        heads = near[s // NC][...] if s % NC == 0 else far[s // NC]
        load.wait()
        term = lax.dot_general(weights[s], heads, NT, preferred_element_type=F32)
        mixed = term if mixed is None else mixed + term
    out[...] = mixed.astype(BF16)


def after(x, *others):
    return lax.optimization_barrier((x, *others))[0]


def in_hbm(x):
    return pltpu.with_memory_space_constraint(x, pltpu.HBM)


def sent(x, axis, size, k):
    return lax.ppermute(x, axis, [(i, i ^ k) for i in range(size)])


def shifted(x, k):
    return lax.ppermute(x, "z", [(i, (i + k) % NZ) for i in range(NZ)])


def local(
    pool_latent,
    pool_rope,
    q_nope,
    q_rope,
    w_uk,
    w_uv,
    w_o,
    block_table,
    lengths,
    preempted,
    assignment,
):
    groups = lax.axis_size("grp")
    group = lax.axis_index("grp")
    column = lax.axis_index(DEV)
    place = lax.axis_index(XC)
    pages_dev, block, width = pool_latent.shape
    requests = preempted.shape[0]
    blocks = block_table.shape[1]
    per_group = requests // groups
    query_rows = q_nope.shape[0] // requests
    rows = per_group * query_rows
    pair = 2 * query_rows
    scale = 1.0 / math.sqrt(DN + DR)
    page_rows = block + DR // 2

    small = pltpu.CompilerParams(vmem_limit_bytes=16 << 20)
    ids = jnp.stack([group, column]).astype(jnp.int32)
    page_type = jax.ShapeDtypeStruct((page_rows, width), BF16)
    meta, copies, *packed = pl.pallas_call(
        functools.partial(prepare_kernel, groups=groups),
        out_shape=[
            jax.ShapeDtypeStruct((META,), jnp.int32),
            jax.ShapeDtypeStruct((NX, 3 * rows + 4 * width, DN), BF16),
        ]
        + [page_type] * groups,
        in_specs=[spec(SMEM)] + [spec(pltpu.HBM)] * 10,
        out_specs=[spec(SMEM)] + [spec(VMEM)] * (1 + groups),
        scratch_shapes=[
            SMEM(block_table.T.shape, jnp.int32),
            SMEM(lengths.shape, jnp.int32),
            SMEM(preempted.shape, jnp.int32),
            SMEM(assignment.shape, jnp.int32),
            VMEM(pool_latent.shape, BF16),
            VMEM(pool_rope.shape, BF16),
            pltpu.SemaphoreType.DMA((2,)),
            pltpu.SemaphoreType.DMA((per_group, 3)),
            pltpu.SemaphoreType.DMA((4,)),
            pltpu.SemaphoreType.DMA((NX, 4)),
        ],
        compiler_params=small,
        name="prepare",
    )(ids, *[in_hbm(a) for a in (block_table.T, lengths, preempted, assignment, pool_latent, pool_rope, q_nope, q_rope, w_uk, w_uv)])

    arrived = [packed[0]] + [
        lax.ppermute(packed[k], "grp", [(i, (i + k) % groups) for i in range(groups)])
        for k in range(1, groups)
    ]
    near_x = lax.all_to_all(copies, "x", split_axis=0, concat_axis=0)

    share = w_o.shape[1] // (NZ * NXC)
    w_cols = pl.pallas_call(
        columns_kernel,
        out_shape=jax.ShapeDtypeStruct((NXC, NZ * share, w_o.shape[0]), BF16),
        in_specs=[spec(pltpu.HBM)],
        out_specs=spec(VMEM),
        scratch_shapes=[
            VMEM(w_o.shape, BF16),
            VMEM(w_o.shape[::-1], BF16),
            pltpu.SemaphoreType.DMA,
        ],
        compiler_params=pltpu.CompilerParams(vmem_limit_bytes=24 << 20),
        name="columns",
    )(in_hbm(after(w_o, packed[0])))
    arrived, w_cols = lax.optimization_barrier((arrived, w_cols))

    half_page = jax.ShapeDtypeStruct((page_rows // 2, width), BF16)
    halves = pl.pallas_call(
        pick_kernel,
        out_shape=[half_page] * 2,
        in_specs=[spec(SMEM)] + [spec(VMEM)] * groups,
        out_specs=[spec(VMEM)] * 2,
        compiler_params=small,
        name="pick",
    )(meta, *arrived)

    below, above = [halves], [halves]
    for k in range(1, NZ // 2):
        below.append([shifted(h, 1) for h in below[-1]])
        above.append([shifted(h, -1) for h in above[-1]])
    middle = [shifted(below[-1][0], 1), shifted(above[-1][1], -1)]
    pages = [halves] + above[1:] + [middle] + below[:0:-1]

    far_x = sent(after(near_x, above[2], below[2]), "c", NC, 1)
    w_cols = after(w_cols, near_x)
    weights = lax.all_to_all(w_cols, XC, split_axis=0, concat_axis=0)

    query = pl.pallas_call(
        query_kernel,
        out_shape=jax.ShapeDtypeStruct((per_group, NXC * pair, width + 2 * DR), BF16),
        in_specs=[spec(SMEM)] + [spec(pl.ANY)] * 2,
        out_specs=spec(VMEM),
        scratch_shapes=[
            VMEM((NXC, 3 * rows + 2 * width, DN), BF16),
            pltpu.SemaphoreType.DMA((NXC,)),
        ],
        compiler_params=small,
        name="query",
    )(meta, in_hbm(near_x), in_hbm(far_x))

    half_type = jax.ShapeDtypeStruct((NX, rows + TAIL, 2 * DV), BF16)
    keep, send = pl.pallas_call(
        functools.partial(attention_kernel, scale=scale),
        out_shape=[half_type, half_type],
        in_specs=[spec(SMEM), spec(VMEM)] + [spec(pl.ANY)] * (2 + 2 * NZ),
        out_specs=[spec(VMEM)] * 2,
        scratch_shapes=[
            VMEM((per_group, NXC * pair, width), F32),
            VMEM((per_group, NXC * pair, 128), F32),
            VMEM((per_group, NXC * pair, 128), F32),
            VMEM((NZ, page_rows, width), BF16),
            VMEM((NXC, 2 * width, DV), BF16),
            pltpu.SemaphoreType.DMA((NZ, 2)),
            pltpu.SemaphoreType.DMA((NXC,)),
        ],
        compiler_params=pltpu.CompilerParams(vmem_limit_bytes=32 << 20),
        name="attention",
    )(meta, query, in_hbm(near_x), in_hbm(far_x), *[p[0] for p in pages], *[p[1] for p in pages])

    got = sent(send, "c", NC, 1)
    part_type = jax.ShapeDtypeStruct((rows + TAIL, 2 * DV), BF16)
    chip = pl.pallas_call(
        chip_kernel,
        out_shape=[part_type] * NX,
        in_specs=[spec(VMEM)] * 2,
        out_specs=[spec(VMEM)] * NX,
        compiler_params=small,
        name="chip",
    )(keep, got)
    heads = pl.pallas_call(
        heads_kernel,
        out_shape=jax.ShapeDtypeStruct((rows, 2 * DV), BF16),
        in_specs=[spec(VMEM)] * NX,
        out_specs=spec(VMEM),
        compiler_params=small,
        name="heads",
    )(chip[0], *[sent(chip[k], "x", NX, k) for k in range(1, NX)])
    near = [heads] + [sent(heads, "x", NX, k) for k in range(1, NX)]
    far = sent(jnp.stack(near), "c", NC, 1)
    mixed = pl.pallas_call(
        output_kernel,
        out_shape=jax.ShapeDtypeStruct((NZ * share, rows), BF16),
        in_specs=[spec(SMEM), spec(pl.ANY)] + [spec(VMEM)] * (NX + 1),
        out_specs=spec(VMEM),
        scratch_shapes=[VMEM(weights.shape, BF16), pltpu.SemaphoreType.DMA((NXC,))],
        compiler_params=small,
        name="output",
    )(meta, in_hbm(weights), *near, far)
    mixed = lax.all_to_all(mixed, "z", split_axis=0, concat_axis=0, tiled=True)
    mixed = mixed.reshape(NZ, -1, rows).astype(F32).sum(axis=0)
    return mixed.T.astype(BF16)


def solution(mesh):
    split = Mesh(mesh.devices.reshape(mesh.shape["grp"], NZ, NX, NC), GRP_DEV)
    return jax.shard_map(
        local,
        mesh=split,
        in_specs=(
            P(GRP_DEV, None, None),
            P(GRP_DEV, None, None),
            P(None, DEV),
            P(None, DEV),
            P(None, DEV),
            P(None, DEV),
            P(DEV, None),
            P(),
            P(),
            P(),
            P(),
        ),
        out_specs=P("grp", DEV),
        check_vma=False,
    )
```

```python
import functools
import math

import jax
import jax.numpy as jnp
from jax import lax
from jax.experimental import pallas as pl
from jax.experimental.pallas import tpu as pltpu
from jax.sharding import Mesh
from jax.sharding import PartitionSpec as P

DR = 64
DN = 128
DV = 128
NEG = -1e30
LOG2E = math.log2(math.e)
NZ, NX, NC = 8, 4, 2
NXC = NX * NC
DEV = ("z", "x", "c")
GRP_DEV = ("grp", "z", "x", "c")
XC = ("x", "c")
SMEM = pltpu.SMEM
VMEM = pltpu.VMEM
F32 = jnp.float32
BF16 = jnp.bfloat16
NT = (((1,), (1,)), ((), ()))


def spec(space):
    return pl.BlockSpec(memory_space=space)


SEND, PICK, PLACE, SPOT, RANK, VALID, MEMBER, COUNT, SPARE = 0, 4, 5, 6, 8, 16, 24, 32, 40
META = 41
TAIL = 16


def fill_table(meta, ids, table, lengths, preempted, assignment, *, groups, block, pages_dev):
    group, column = ids[0], ids[1]
    blocks = table.shape[0]
    columns = NZ * NXC
    me = group * columns + column
    place = column & (NXC - 1)
    plane = lax.shift_right_logical(column, NXC.bit_length() - 1)
    for i in range(SPARE):
        meta[i] = 0
    meta[PLACE] = place
    meta[SPOT] = lax.shift_right_logical(place, NC.bit_length() - 1)

    def one_request(i, carry):
        slot = preempted[i]
        owner = assignment[i]
        rank = meta[COUNT + owner]
        meta[COUNT + owner] = rank + 1
        ahead = SEND + ((owner - group) & (groups - 1))
        for b in range(blocks):
            page = table[b, slot]
            holder = lax.shift_right_logical(page, pages_dev.bit_length() - 1)
            meta[jnp.where(holder == me, ahead, SPARE)] = page & (pages_dev - 1)

        @pl.when(owner == group)
        def _():
            length = lengths[slot]
            meta[MEMBER + rank] = i
            for b in range(blocks):
                holder = lax.shift_right_logical(table[b, slot], pages_dev.bit_length() - 1)
                col = holder & (columns - 1)
                row = lax.shift_right_logical(holder, columns.bit_length() - 1)
                z = (lax.shift_right_logical(col, NXC.bit_length() - 1) - plane) & (NZ - 1)
                near = (col & (NXC - 1)) == place
                meta[jnp.where(near, RANK + z, SPARE)] = rank
                meta[jnp.where(near, VALID + z, SPARE)] = jnp.clip(length - b * block, 0, block)
                meta[jnp.where(col == column, PICK, SPARE)] = (group - row) & (groups - 1)

        return carry

    lax.fori_loop(0, preempted.shape[0], one_request, 0)


def prepare_kernel(ids, *refs, groups):
    tables_hbm, (latent_hbm, rope_hbm, q_nope, q_rope, w_uk, w_uv), rest = refs[:4], refs[4:10], refs[10:]
    meta, copies = rest[:2]
    outs = rest[2 : 2 + groups]
    table, lengths, preempted, assignment, latent, rope, sem, row_sem, table_sem, w_sem = rest[2 + groups :]
    tables = (table, lengths, preempted, assignment)
    pages_dev, block, _ = latent.shape
    half = rope.shape[1] // 2
    q_rows = q_nope.shape[0] // preempted.shape[0]
    depth = w_uk.shape[0]
    queries = copies.shape[1] - 4 * depth
    rows = queries // 3
    for_all = [
        pltpu.make_async_copy(
            w.at[:, pl.ds(h * DN, DN)],
            copies.at[k, pl.ds(queries + (2 * i + h) * depth, depth), :],
            w_sem.at[k, 2 * i + h],
        )
        for i, w in enumerate((w_uk, w_uv))
        for h in range(2)
        for k in range(copies.shape[0])
    ]
    loads = [
        pltpu.make_async_copy(latent_hbm, latent, sem.at[0]),
        pltpu.make_async_copy(rope_hbm, rope, sem.at[1]),
    ]
    first = [
        pltpu.make_async_copy(src, dst, table_sem.at[i])
        for i, (src, dst) in enumerate(zip(tables_hbm, tables))
    ]
    for load in first + loads + for_all:
        load.start()
    for load in first:
        load.wait()
    fill_table(
        meta, ids, table, lengths, preempted, assignment,
        groups=groups, block=block, pages_dev=pages_dev,
    )
    moves = []
    for r in range(rows // q_rows):
        start = pl.multiple_of(meta[MEMBER + r] * q_rows, q_rows)
        for j in range(3):
            source = q_rope if j == 2 else q_nope.at[:, pl.ds(j * DN, DN)]
            moves.append(
                pltpu.make_async_copy(
                    source.at[pl.ds(start, q_rows), :],
                    copies.at[0, pl.ds(j * rows + r * q_rows, q_rows), :],
                    row_sem.at[r, j],
                )
            )
    for move in moves:
        move.start()
    for load in loads:
        load.wait()
    for k, out in enumerate(outs):
        page = meta[SEND + k]
        out[:block, :] = latent[page]
        out[block:, :block] = rope[page, :half, :]
        out[block:, block:] = rope[page, half:, :]
    for move in moves:
        move.wait()
    for k in range(1, copies.shape[0]):
        copies[k, :queries, :] = copies[0, :queries, :]
    for load in for_all:
        load.wait()


def pick_kernel(meta, *rest):
    sources, (first, second) = rest[:-2], rest[-2:]
    half = first.shape[0]
    for k, source in enumerate(sources):

        @pl.when(meta[PICK] == k)
        def _():
            first[...] = source[:half, :]
            second[...] = source[half:, :]


def placed(near, far, s, meta):
    return (near, far)[s % NC].at[meta[SPOT] ^ (s // NC)]


def query_kernel(meta, near, far, out, got, sem):
    per_group = out.shape[0]
    pair = out.shape[1] // NXC
    q_rows = pair // 2
    width = out.shape[2] - 2 * DR
    rows = per_group * q_rows
    loads = [
        pltpu.make_async_copy(
            placed(near, far, s, meta).at[pl.ds(0, got.shape[1]), :], got.at[s], sem.at[s]
        )
        for s in range(NXC)
    ]
    for load in loads:
        load.start()
    lane = lax.broadcasted_iota(jnp.int32, (rows, 2 * DR), 1)
    for s in range(NXC):
        loads[s].wait()
        hi = got[s, 2 * rows : 3 * rows, :]
        for h in range(2):
            live = (lane >= h * DR) & (lane < (h + 1) * DR)
            tail = jnp.where(live, hi, jnp.zeros_like(hi))
            key = 3 * rows + h * width
            lat = lax.dot_general(
                got[s, h * rows : (h + 1) * rows, :],
                got[s, key : key + width, :],
                NT,
                preferred_element_type=F32,
            ).astype(BF16)
            lo = s * pair + h * q_rows
            out[:, lo : lo + q_rows, :width] = lat.reshape(per_group, q_rows, width)
            out[:, lo : lo + q_rows, width:] = tail.reshape(per_group, q_rows, 2 * DR)


def three_parts(x):
    high = x.astype(BF16).astype(F32)
    rest = x - high
    middle = rest.astype(BF16).astype(F32)
    return [high, middle, rest - middle]


def stored_stats(stats):
    rows = [p for s in stats for p in three_parts(s)]
    fill = jnp.zeros((TAIL - len(rows), rows[0].shape[1]), F32)
    return jnp.concatenate(rows + [fill], axis=0).astype(BF16)


def read_stats(tail):
    tail = tail.astype(F32)
    return [tail[3 * h : 3 * h + 1] + tail[3 * h + 1 : 3 * h + 2] + tail[3 * h + 2 : 3 * h + 3] for h in range(2)]


def attention_kernel(meta, query, *rest, scale):
    near, far, firsts, seconds = *rest[:2], rest[2 : 2 + NZ], rest[2 + NZ : -9]
    keep, send, acc, top, total, pages, w_uv, sem, w_sem = rest[-9:]
    per_group, heads_rows, width = acc.shape
    q_rows = heads_rows // (2 * NXC)
    rows = per_group * q_rows
    block = pages.shape[1] * 8 // 9

    middle = NZ // 2
    order = [0] + [z for k in range(1, middle) for z in (k, NZ - k)] + [middle]
    split = pages.shape[1] // 2
    loads = [
        [
            pltpu.make_async_copy(firsts[z], pages.at[i, pl.ds(0, split), :], sem.at[i, 0]),
            pltpu.make_async_copy(seconds[z], pages.at[i, pl.ds(split, split), :], sem.at[i, 1]),
        ]
        for i, z in enumerate(order)
    ]
    loads_w = [
        pltpu.make_async_copy(
            placed(near, far, s, meta).at[pl.ds(near.shape[1] - 2 * width, 2 * width), :],
            w_uv.at[s],
            w_sem.at[s],
        )
        for s in range(NXC)
    ]
    for load in [load for pair in loads for load in pair] + loads_w:
        load.start()

    ranks = [meta[RANK + z] for z in order]
    valids = [meta[VALID + z] for z in order]
    for r in range(per_group):
        held = [(ranks[z] == r) & (valids[z] > 0) for z in range(NZ)]

        @pl.when(jnp.logical_not(functools.reduce(jnp.logical_or, held)))
        def _():
            acc[r] = jnp.zeros(acc.shape[1:], F32)
            top[r] = jnp.full(top.shape[1:], NEG, F32)
            total[r] = jnp.zeros(total.shape[1:], F32)

    def one_page(i, r, valid, first):
        latent = pages[i, :block, :]
        tail = pages[i, block:, :]
        rope = jnp.concatenate([tail[:, :block], tail[:, block:]], axis=0)
        rope = jnp.concatenate([rope, rope], axis=0)
        q = query[r]
        score = lax.dot_general(q[:, :width], latent, NT, preferred_element_type=F32)
        score = score + jnp.dot(q[:, width:], rope, preferred_element_type=F32)
        token = lax.broadcasted_iota(jnp.int32, score.shape, 1)
        score = jnp.where(token < valid, score * (scale * LOG2E), NEG)
        new = jnp.max(score, axis=1, keepdims=True)
        if not first:
            old = top[r][:, :1]
            new = jnp.maximum(old, new)
            fade = jnp.exp2(old - new)
        expo = jnp.exp2(score - new)
        weight = jnp.sum(expo, axis=1, keepdims=True)
        value = jnp.dot(expo.astype(BF16), latent, preferred_element_type=F32)
        top[r] = jnp.broadcast_to(new, top.shape[1:])
        if first:
            total[r] = jnp.broadcast_to(weight, total.shape[1:])
            acc[r] = value
        else:
            total[r] = total[r] * fade + weight
            acc[r] = acc[r] * fade + value

    def one_step(i, carry):
        z = jnp.where(i & 1 == 1, (i + 1) // 2, (NZ - i // 2) & (NZ - 1))
        r, valid = meta[RANK + z], meta[VALID + z]
        earlier = [(p < i) & (ranks[p] == r) & (valids[p] > 0) for p in range(NZ)]
        again = functools.reduce(jnp.logical_or, earlier)

        @pl.when((valid > 0) & jnp.logical_not(again))
        def _():
            one_page(i, r, valid, True)

        @pl.when((valid > 0) & again)
        def _():
            one_page(i, r, valid, False)

        return carry

    for load in [load for pair in loads for load in pair]:
        load.wait()
    lax.fori_loop(0, NZ, one_step, 0)

    lane = lax.broadcasted_iota(jnp.int32, (rows, total.shape[2]), 1)
    weights = jnp.zeros(lane.shape, F32)
    highs = jnp.full(lane.shape, NEG, F32)
    for j in range(2 * NXC):
        part = slice(j * q_rows, (j + 1) * q_rows)
        weights = jnp.where(lane == j, total[:, part, :].reshape(lane.shape), weights)
        highs = jnp.where(lane == j, top[:, part, :].reshape(lane.shape), highs)
    some = weights > 0.0
    safe = jnp.where(some, weights, 1.0)
    shares = 1.0 / safe
    stats = jnp.where(some, highs * (1.0 / LOG2E) + jnp.log(safe), NEG).T
    for s in range(NXC):
        out = keep if s % 2 == 0 else send
        loads_w[s].wait()
        for h in range(2):
            j = 2 * s + h
            value = acc[:, j * q_rows : (j + 1) * q_rows, :].reshape(rows, width)
            value = (value * shares[:, j : j + 1]).astype(BF16)
            head = jnp.dot(value, w_uv[s, h * width : (h + 1) * width, :], preferred_element_type=F32)
            out[s // 2, :rows, h * DV : (h + 1) * DV] = head.astype(BF16)
        out[s // 2, rows:, :] = stored_stats([stats[2 * s + h : 2 * s + h + 1, :] for h in range(2)])


def merge(parts, tails):
    rows = parts[0].shape[0]
    stats = [read_stats(t) for t in tails]
    high = [functools.reduce(jnp.maximum, [s[h] for s in stats]) for h in range(2)]
    shares = [[jnp.exp(s[h] - high[h]) for s in stats] for h in range(2)]
    whole = [functools.reduce(jnp.add, shares[h]) for h in range(2)]
    lines = [w / whole[h] for h in range(2) for w in shares[h]]
    fill = jnp.zeros((128 - len(lines), rows), F32)
    table = jnp.concatenate(lines + [fill], axis=0).T
    halves = []
    for h in range(2):
        sides = [p[:, h * DV : (h + 1) * DV].astype(F32) for p in parts]
        first = h * len(parts)
        halves.append(sum(table[:, first + i : first + i + 1] * p for i, p in enumerate(sides)))
    return halves, [high[h] + jnp.log(whole[h]) for h in range(2)]


def chip_kernel(keep, got, *outs):
    for k, out in enumerate(outs):
        rows = out.shape[0] - TAIL
        halves, stats = merge(
            [keep[k, :rows, :], got[k, :rows, :]], [keep[k, rows:, :], got[k, rows:, :]]
        )
        for h, half in enumerate(halves):
            out[:rows, h * DV : (h + 1) * DV] = half.astype(BF16)
        out[rows:, :] = stored_stats(stats)


def heads_kernel(*refs):
    parts, out = refs[:-1], refs[-1]
    rows = out.shape[0]
    halves, _ = merge([p[:rows, :] for p in parts], [p[rows:, :] for p in parts])
    for h, half in enumerate(halves):
        out[:, h * DV : (h + 1) * DV] = half.astype(BF16)


def columns_kernel(w_hbm, out, wide, tall, sem):
    load = pltpu.make_async_copy(w_hbm, wide, sem)
    load.start()
    load.wait()
    step = 256
    for i in range(wide.shape[1] // step):
        tall[i * step : (i + 1) * step, :] = wide[:, i * step : (i + 1) * step].T
    share = out.shape[1] // NZ
    for z in range(NZ):
        for s in range(NXC):
            at = (z * NXC + s) * share
            out[s, z * share : (z + 1) * share, :] = tall[at : at + share, :]


def output_kernel(meta, weights, *refs):
    near, far, out = refs[:NX], *refs[NX:]
    mixed = None
    for s in range(NXC):
        heads = near[s // NC][...] if s % NC == 0 else far[s // NC]
        weight = weights[meta[PLACE] ^ s]
        term = lax.dot_general(weight, heads, NT, preferred_element_type=F32)
        mixed = term if mixed is None else mixed + term
    out[...] = mixed.astype(BF16)


def after(x, *others):
    return lax.optimization_barrier((x, *others))[0]


def in_hbm(x):
    return pltpu.with_memory_space_constraint(x, pltpu.HBM)


def sent(x, axis, size, k):
    return lax.ppermute(x, axis, [(i, i ^ k) for i in range(size)])


def shifted(x, k):
    return lax.ppermute(x, "z", [(i, (i + k) % NZ) for i in range(NZ)])


def local(
    pool_latent,
    pool_rope,
    q_nope,
    q_rope,
    w_uk,
    w_uv,
    w_o,
    block_table,
    lengths,
    preempted,
    assignment,
):
    groups = lax.axis_size("grp")
    group = lax.axis_index("grp")
    column = lax.axis_index(DEV)
    place = lax.axis_index(XC)
    pages_dev, block, width = pool_latent.shape
    requests = preempted.shape[0]
    blocks = block_table.shape[1]
    per_group = requests // groups
    query_rows = q_nope.shape[0] // requests
    rows = per_group * query_rows
    pair = 2 * query_rows
    scale = 1.0 / math.sqrt(DN + DR)
    page_rows = block + DR // 2

    small = pltpu.CompilerParams(vmem_limit_bytes=16 << 20)
    ids = jnp.stack([group, column]).astype(jnp.int32)
    page_type = jax.ShapeDtypeStruct((page_rows, width), BF16)
    meta, copies, *packed = pl.pallas_call(
        functools.partial(prepare_kernel, groups=groups),
        out_shape=[
            jax.ShapeDtypeStruct((META,), jnp.int32),
            jax.ShapeDtypeStruct((NX, 3 * rows + 4 * width, DN), BF16),
        ]
        + [page_type] * groups,
        in_specs=[spec(SMEM)] + [spec(pltpu.HBM)] * 10,
        out_specs=[spec(SMEM)] + [spec(VMEM)] * (1 + groups),
        scratch_shapes=[
            SMEM(block_table.T.shape, jnp.int32),
            SMEM(lengths.shape, jnp.int32),
            SMEM(preempted.shape, jnp.int32),
            SMEM(assignment.shape, jnp.int32),
            VMEM(pool_latent.shape, BF16),
            VMEM(pool_rope.shape, BF16),
            pltpu.SemaphoreType.DMA((2,)),
            pltpu.SemaphoreType.DMA((per_group, 3)),
            pltpu.SemaphoreType.DMA((4,)),
            pltpu.SemaphoreType.DMA((NX, 4)),
        ],
        compiler_params=small,
        name="prepare",
    )(ids, *[in_hbm(a) for a in (block_table.T, lengths, preempted, assignment, pool_latent, pool_rope, q_nope, q_rope, w_uk, w_uv)])

    arrived = [packed[0]] + [
        lax.ppermute(packed[k], "grp", [(i, (i + k) % groups) for i in range(groups)])
        for k in range(1, groups)
    ]
    near_x = lax.all_to_all(copies, "x", split_axis=0, concat_axis=0)

    share = w_o.shape[1] // (NZ * NXC)
    w_cols = pl.pallas_call(
        columns_kernel,
        out_shape=jax.ShapeDtypeStruct((NXC, NZ * share, w_o.shape[0]), BF16),
        in_specs=[spec(pltpu.HBM)],
        out_specs=spec(VMEM),
        scratch_shapes=[
            VMEM(w_o.shape, BF16),
            VMEM(w_o.shape[::-1], BF16),
            pltpu.SemaphoreType.DMA,
        ],
        compiler_params=pltpu.CompilerParams(vmem_limit_bytes=24 << 20),
        name="columns",
    )(in_hbm(after(w_o, packed[0])))
    arrived, w_cols = lax.optimization_barrier((arrived, w_cols))

    half_page = jax.ShapeDtypeStruct((page_rows // 2, width), BF16)
    halves = pl.pallas_call(
        pick_kernel,
        out_shape=[half_page] * 2,
        in_specs=[spec(SMEM)] + [spec(VMEM)] * groups,
        out_specs=[spec(VMEM)] * 2,
        compiler_params=small,
        name="pick",
    )(meta, *arrived)

    below, above = [halves], [halves]
    for k in range(1, NZ // 2):
        below.append([shifted(h, 1) for h in below[-1]])
        above.append([shifted(h, -1) for h in above[-1]])
    middle = [shifted(below[-1][0], 1), shifted(above[-1][1], -1)]
    pages = [halves] + above[1:] + [middle] + below[:0:-1]

    far_x = sent(after(near_x, above[2], below[2]), "c", NC, 1)
    w_cols = after(w_cols, near_x)
    weights = lax.all_to_all(w_cols, XC, split_axis=0, concat_axis=0)

    query = pl.pallas_call(
        query_kernel,
        out_shape=jax.ShapeDtypeStruct((per_group, NXC * pair, width + 2 * DR), BF16),
        in_specs=[spec(SMEM)] + [spec(pl.ANY)] * 2,
        out_specs=spec(VMEM),
        scratch_shapes=[
            VMEM((NXC, 3 * rows + 2 * width, DN), BF16),
            pltpu.SemaphoreType.DMA((NXC,)),
        ],
        compiler_params=small,
        name="query",
    )(meta, in_hbm(near_x), in_hbm(far_x))

    half_type = jax.ShapeDtypeStruct((NX, rows + TAIL, 2 * DV), BF16)
    keep, send = pl.pallas_call(
        functools.partial(attention_kernel, scale=scale),
        out_shape=[half_type, half_type],
        in_specs=[spec(SMEM), spec(VMEM)] + [spec(pl.ANY)] * (2 + 2 * NZ),
        out_specs=[spec(VMEM)] * 2,
        scratch_shapes=[
            VMEM((per_group, NXC * pair, width), F32),
            VMEM((per_group, NXC * pair, 128), F32),
            VMEM((per_group, NXC * pair, 128), F32),
            VMEM((NZ, page_rows, width), BF16),
            VMEM((NXC, 2 * width, DV), BF16),
            pltpu.SemaphoreType.DMA((NZ, 2)),
            pltpu.SemaphoreType.DMA((NXC,)),
        ],
        compiler_params=pltpu.CompilerParams(vmem_limit_bytes=32 << 20),
        name="attention",
    )(meta, query, in_hbm(near_x), in_hbm(far_x), *[p[0] for p in pages], *[p[1] for p in pages])

    got = sent(send, "c", NC, 1)
    part_type = jax.ShapeDtypeStruct((rows + TAIL, 2 * DV), BF16)
    chip = pl.pallas_call(
        chip_kernel,
        out_shape=[part_type] * NX,
        in_specs=[spec(VMEM)] * 2,
        out_specs=[spec(VMEM)] * NX,
        compiler_params=small,
        name="chip",
    )(keep, got)
    heads = pl.pallas_call(
        heads_kernel,
        out_shape=jax.ShapeDtypeStruct((rows, 2 * DV), BF16),
        in_specs=[spec(VMEM)] * NX,
        out_specs=spec(VMEM),
        compiler_params=small,
        name="heads",
    )(chip[0], *[sent(chip[k], "x", NX, k) for k in range(1, NX)])
    heads, weights = lax.optimization_barrier((heads, weights))
    near = [heads] + [sent(heads, "x", NX, k) for k in range(1, NX)]
    far = sent(jnp.stack(near), "c", NC, 1)
    mixed = pl.pallas_call(
        output_kernel,
        out_shape=jax.ShapeDtypeStruct((NZ * share, rows), BF16),
        in_specs=[spec(SMEM)] + [spec(VMEM)] * (NX + 2),
        out_specs=spec(VMEM),
        compiler_params=small,
        name="output",
    )(meta, weights, *near, far)
    mixed = lax.all_to_all(mixed, "z", split_axis=0, concat_axis=0, tiled=True)
    mixed = mixed.reshape(NZ, -1, rows).astype(F32).sum(axis=0)
    return mixed.T.astype(BF16)


def solution(mesh):
    split = Mesh(mesh.devices.reshape(mesh.shape["grp"], NZ, NX, NC), GRP_DEV)
    return jax.shard_map(
        local,
        mesh=split,
        in_specs=(
            P(GRP_DEV, None, None),
            P(GRP_DEV, None, None),
            P(None, DEV),
            P(None, DEV),
            P(None, DEV),
            P(None, DEV),
            P(DEV, None),
            P(),
            P(),
            P(),
            P(),
        ),
        out_specs=P("grp", DEV),
        check_vma=False,
    )
```

```python
import functools
import math

import jax
import jax.numpy as jnp
from jax import lax
from jax.experimental import pallas as pl
from jax.experimental.pallas import tpu as pltpu
from jax.sharding import Mesh
from jax.sharding import PartitionSpec as P

DR = 64
DN = 128
DV = 128
NEG = -1e30
LOG2E = math.log2(math.e)
NZ, NX, NC = 8, 4, 2
NXC = NX * NC
DEV = ("z", "x", "c")
GRP_DEV = ("grp", "z", "x", "c")
XC = ("x", "c")
SMEM = pltpu.SMEM
VMEM = pltpu.VMEM
F32 = jnp.float32
BF16 = jnp.bfloat16
NT = (((1,), (1,)), ((), ()))


def spec(space):
    return pl.BlockSpec(memory_space=space)


SEND, PICK, PLACE, SPOT, RANK, VALID, MEMBER, COUNT, SPARE = 0, 4, 5, 6, 8, 16, 24, 32, 40
META = 41
TAIL = 16


def fill_members(meta, ids, assignment):
    for i in range(SPARE):
        meta[i] = 0

    def one_request(i, carry):
        owner = assignment[i]
        rank = meta[COUNT + owner]
        meta[COUNT + owner] = rank + 1
        meta[jnp.where(owner == ids[0], MEMBER + rank, SPARE)] = i
        return carry

    lax.fori_loop(0, assignment.shape[0], one_request, 0)


def fill_table(meta, ids, table, lengths, preempted, assignment, *, groups, block, pages_dev):
    group, column = ids[0], ids[1]
    blocks = table.shape[0]
    columns = NZ * NXC
    me = group * columns + column
    place = column & (NXC - 1)
    plane = lax.shift_right_logical(column, NXC.bit_length() - 1)
    meta[PLACE] = place
    meta[SPOT] = lax.shift_right_logical(place, NC.bit_length() - 1)

    def one_request(i, carry):
        slot = preempted[i]
        owner = assignment[i]
        ahead = SEND + ((owner - group) & (groups - 1))
        for b in range(blocks):
            page = table[b, slot]
            holder = lax.shift_right_logical(page, pages_dev.bit_length() - 1)
            meta[jnp.where(holder == me, ahead, SPARE)] = page & (pages_dev - 1)

        return carry

    lax.fori_loop(0, preempted.shape[0], one_request, 0)

    def one_member(rank, carry):
        slot = preempted[meta[MEMBER + rank]]
        length = lengths[slot]
        for b in range(blocks):
            holder = lax.shift_right_logical(table[b, slot], pages_dev.bit_length() - 1)
            col = holder & (columns - 1)
            row = lax.shift_right_logical(holder, columns.bit_length() - 1)
            z = (lax.shift_right_logical(col, NXC.bit_length() - 1) - plane) & (NZ - 1)
            near = (col & (NXC - 1)) == place
            meta[jnp.where(near, RANK + z, SPARE)] = rank
            meta[jnp.where(near, VALID + z, SPARE)] = jnp.clip(length - b * block, 0, block)
            meta[jnp.where(col == column, PICK, SPARE)] = (group - row) & (groups - 1)

        return carry

    lax.fori_loop(0, preempted.shape[0] // groups, one_member, 0)


def prepare_kernel(ids, *refs, groups):
    tables_hbm, (latent_hbm, rope_hbm, q_nope, q_rope, w_uk, w_uv), rest = refs[:4], refs[4:10], refs[10:]
    meta, copies = rest[:2]
    outs = rest[2 : 2 + groups]
    table, lengths, preempted, assignment, latent, rope, sem, row_sem, table_sem, w_sem = rest[2 + groups :]
    tables = (table, lengths, preempted, assignment)
    pages_dev, block, _ = latent.shape
    half = rope.shape[1] // 2
    q_rows = q_nope.shape[0] // preempted.shape[0]
    depth = w_uk.shape[0]
    queries = copies.shape[1] - 4 * depth
    rows = queries // 3
    for_all = [
        pltpu.make_async_copy(
            w.at[:, pl.ds(h * DN, DN)],
            copies.at[k, pl.ds(queries + (2 * i + h) * depth, depth), :],
            w_sem.at[k, 2 * i + h],
        )
        for i, w in enumerate((w_uk, w_uv))
        for h in range(2)
        for k in range(copies.shape[0])
    ]
    loads = [
        pltpu.make_async_copy(latent_hbm, latent, sem.at[0]),
        pltpu.make_async_copy(rope_hbm, rope, sem.at[1]),
    ]
    first = [
        pltpu.make_async_copy(src, dst, table_sem.at[i])
        for i, (src, dst) in enumerate(zip(tables_hbm, tables))
    ]
    for load in first + loads + for_all:
        load.start()
    for load in first:
        load.wait()
    fill_members(meta, ids, assignment)
    moves = []
    for r in range(rows // q_rows):
        start = pl.multiple_of(meta[MEMBER + r] * q_rows, q_rows)
        for j in range(3):
            source = q_rope if j == 2 else q_nope.at[:, pl.ds(j * DN, DN)]
            moves.append(
                pltpu.make_async_copy(
                    source.at[pl.ds(start, q_rows), :],
                    copies.at[0, pl.ds(j * rows + r * q_rows, q_rows), :],
                    row_sem.at[r, j],
                )
            )
    for move in moves:
        move.start()
    fill_table(
        meta, ids, table, lengths, preempted, assignment,
        groups=groups, block=block, pages_dev=pages_dev,
    )
    for load in loads:
        load.wait()
    for k, out in enumerate(outs):
        page = meta[SEND + k]
        out[:block, :] = latent[page]
        out[block:, :block] = rope[page, :half, :]
        out[block:, block:] = rope[page, half:, :]
    for move in moves:
        move.wait()
    for k in range(1, copies.shape[0]):
        copies[k, :queries, :] = copies[0, :queries, :]
    for load in for_all:
        load.wait()


def pick_kernel(meta, *rest):
    sources, (first, second) = rest[:-2], rest[-2:]
    half = first.shape[0]
    for k, source in enumerate(sources):

        @pl.when(meta[PICK] == k)
        def _():
            first[...] = source[:half, :]
            second[...] = source[half:, :]


def placed(near, far, s, meta):
    return (near, far)[s % NC].at[meta[SPOT] ^ (s // NC)]


def query_kernel(meta, near, far, out, got, sem):
    per_group = out.shape[0]
    pair = out.shape[1] // NXC
    q_rows = pair // 2
    width = out.shape[2] - 2 * DR
    rows = per_group * q_rows
    loads = [
        pltpu.make_async_copy(
            placed(near, far, s, meta).at[pl.ds(0, got.shape[1]), :], got.at[s], sem.at[s]
        )
        for s in range(NXC)
    ]
    for load in loads:
        load.start()
    lane = lax.broadcasted_iota(jnp.int32, (rows, 2 * DR), 1)
    for s in range(NXC):
        loads[s].wait()
        hi = got[s, 2 * rows : 3 * rows, :]
        for h in range(2):
            live = (lane >= h * DR) & (lane < (h + 1) * DR)
            tail = jnp.where(live, hi, jnp.zeros_like(hi))
            key = 3 * rows + h * width
            lat = lax.dot_general(
                got[s, h * rows : (h + 1) * rows, :],
                got[s, key : key + width, :],
                NT,
                preferred_element_type=F32,
            ).astype(BF16)
            lo = s * pair + h * q_rows
            out[:, lo : lo + q_rows, :width] = lat.reshape(per_group, q_rows, width)
            out[:, lo : lo + q_rows, width:] = tail.reshape(per_group, q_rows, 2 * DR)


def three_parts(x):
    high = x.astype(BF16).astype(F32)
    rest = x - high
    middle = rest.astype(BF16).astype(F32)
    return [high, middle, rest - middle]


def stored_stats(stats):
    rows = [p for s in stats for p in three_parts(s)]
    fill = jnp.zeros((TAIL - len(rows), rows[0].shape[1]), F32)
    return jnp.concatenate(rows + [fill], axis=0).astype(BF16)


def read_stats(tail):
    tail = tail.astype(F32)
    return [tail[3 * h : 3 * h + 1] + tail[3 * h + 1 : 3 * h + 2] + tail[3 * h + 2 : 3 * h + 3] for h in range(2)]


def attention_kernel(meta, query, *rest, scale):
    near, far, firsts, seconds = *rest[:2], rest[2 : 2 + NZ], rest[2 + NZ : -9]
    keep, send, acc, top, total, pages, w_uv, sem, w_sem = rest[-9:]
    per_group, heads_rows, width = acc.shape
    q_rows = heads_rows // (2 * NXC)
    rows = per_group * q_rows
    block = pages.shape[1] * 8 // 9

    middle = NZ // 2
    order = [0] + [z for k in range(1, middle) for z in (k, NZ - k)] + [middle]
    split = pages.shape[1] // 2
    loads = [
        [
            pltpu.make_async_copy(firsts[z], pages.at[i, pl.ds(0, split), :], sem.at[i, 0]),
            pltpu.make_async_copy(seconds[z], pages.at[i, pl.ds(split, split), :], sem.at[i, 1]),
        ]
        for i, z in enumerate(order)
    ]
    loads_w = [
        pltpu.make_async_copy(
            placed(near, far, s, meta).at[pl.ds(near.shape[1] - 2 * width, 2 * width), :],
            w_uv.at[s],
            w_sem.at[s],
        )
        for s in range(NXC)
    ]
    for load in [load for pair in loads for load in pair] + loads_w:
        load.start()

    ranks = [meta[RANK + z] for z in order]
    valids = [meta[VALID + z] for z in order]
    for r in range(per_group):
        held = [(ranks[z] == r) & (valids[z] > 0) for z in range(NZ)]

        @pl.when(jnp.logical_not(functools.reduce(jnp.logical_or, held)))
        def _():
            acc[r] = jnp.zeros(acc.shape[1:], F32)
            top[r] = jnp.full(top.shape[1:], NEG, F32)
            total[r] = jnp.zeros(total.shape[1:], F32)

    def one_page(i, r, valid, first):
        latent = pages[i, :block, :]
        tail = pages[i, block:, :]
        rope = jnp.concatenate([tail[:, :block], tail[:, block:]], axis=0)
        rope = jnp.concatenate([rope, rope], axis=0)
        q = query[r]
        score = lax.dot_general(q[:, :width], latent, NT, preferred_element_type=F32)
        score = score + jnp.dot(q[:, width:], rope, preferred_element_type=F32)
        token = lax.broadcasted_iota(jnp.int32, score.shape, 1)
        score = jnp.where(token < valid, score * (scale * LOG2E), NEG)
        new = jnp.max(score, axis=1, keepdims=True)
        if not first:
            old = top[r][:, :1]
            new = jnp.maximum(old, new)
            fade = jnp.exp2(old - new)
        expo = jnp.exp2(score - new)
        weight = jnp.sum(expo, axis=1, keepdims=True)
        value = jnp.dot(expo.astype(BF16), latent, preferred_element_type=F32)
        top[r] = jnp.broadcast_to(new, top.shape[1:])
        if first:
            total[r] = jnp.broadcast_to(weight, total.shape[1:])
            acc[r] = value
        else:
            total[r] = total[r] * fade + weight
            acc[r] = acc[r] * fade + value

    def one_step(i, carry):
        z = jnp.where(i & 1 == 1, (i + 1) // 2, (NZ - i // 2) & (NZ - 1))
        r, valid = meta[RANK + z], meta[VALID + z]
        earlier = [(p < i) & (ranks[p] == r) & (valids[p] > 0) for p in range(NZ)]
        again = functools.reduce(jnp.logical_or, earlier)

        @pl.when((valid > 0) & jnp.logical_not(again))
        def _():
            one_page(i, r, valid, True)

        @pl.when((valid > 0) & again)
        def _():
            one_page(i, r, valid, False)

        return carry

    for load in [load for pair in loads for load in pair]:
        load.wait()
    lax.fori_loop(0, NZ, one_step, 0)

    lane = lax.broadcasted_iota(jnp.int32, (rows, total.shape[2]), 1)
    weights = jnp.zeros(lane.shape, F32)
    highs = jnp.full(lane.shape, NEG, F32)
    for j in range(2 * NXC):
        part = slice(j * q_rows, (j + 1) * q_rows)
        weights = jnp.where(lane == j, total[:, part, :].reshape(lane.shape), weights)
        highs = jnp.where(lane == j, top[:, part, :].reshape(lane.shape), highs)
    some = weights > 0.0
    safe = jnp.where(some, weights, 1.0)
    shares = 1.0 / safe
    stats = jnp.where(some, highs * (1.0 / LOG2E) + jnp.log(safe), NEG).T
    for s in range(NXC):
        out = keep if s % 2 == 0 else send
        loads_w[s].wait()
        for h in range(2):
            j = 2 * s + h
            value = acc[:, j * q_rows : (j + 1) * q_rows, :].reshape(rows, width)
            value = (value * shares[:, j : j + 1]).astype(BF16)
            head = jnp.dot(value, w_uv[s, h * width : (h + 1) * width, :], preferred_element_type=F32)
            out[s // 2, :rows, h * DV : (h + 1) * DV] = head.astype(BF16)
        out[s // 2, rows:, :] = stored_stats([stats[2 * s + h : 2 * s + h + 1, :] for h in range(2)])


def merge(parts, tails):
    rows = parts[0].shape[0]
    stats = [read_stats(t) for t in tails]
    high = [functools.reduce(jnp.maximum, [s[h] for s in stats]) for h in range(2)]
    shares = [[jnp.exp(s[h] - high[h]) for s in stats] for h in range(2)]
    whole = [functools.reduce(jnp.add, shares[h]) for h in range(2)]
    lines = [w / whole[h] for h in range(2) for w in shares[h]]
    fill = jnp.zeros((128 - len(lines), rows), F32)
    table = jnp.concatenate(lines + [fill], axis=0).T
    halves = []
    for h in range(2):
        sides = [p[:, h * DV : (h + 1) * DV].astype(F32) for p in parts]
        first = h * len(parts)
        halves.append(sum(table[:, first + i : first + i + 1] * p for i, p in enumerate(sides)))
    return halves, [high[h] + jnp.log(whole[h]) for h in range(2)]


def chip_kernel(keep, got, *outs):
    for k, out in enumerate(outs):
        rows = out.shape[0] - TAIL
        halves, stats = merge(
            [keep[k, :rows, :], got[k, :rows, :]], [keep[k, rows:, :], got[k, rows:, :]]
        )
        for h, half in enumerate(halves):
            out[:rows, h * DV : (h + 1) * DV] = half.astype(BF16)
        out[rows:, :] = stored_stats(stats)


def heads_kernel(*refs):
    parts, out = refs[:-1], refs[-1]
    rows = out.shape[0]
    halves, _ = merge([p[:rows, :] for p in parts], [p[rows:, :] for p in parts])
    for h, half in enumerate(halves):
        out[:, h * DV : (h + 1) * DV] = half.astype(BF16)


def columns_kernel(w_hbm, out, wide, tall, sem):
    load = pltpu.make_async_copy(w_hbm, wide, sem)
    load.start()
    load.wait()
    step = 256
    for i in range(wide.shape[1] // step):
        tall[i * step : (i + 1) * step, :] = wide[:, i * step : (i + 1) * step].T
    share = out.shape[1] // NZ
    for z in range(NZ):
        for s in range(NXC):
            at = (z * NXC + s) * share
            out[s, z * share : (z + 1) * share, :] = tall[at : at + share, :]


def near_kernel(meta, weights, *refs):
    near, out = refs[:NX], refs[-1]
    mixed = None
    for k in range(NX):
        weight = weights[meta[PLACE] ^ (k * NC)]
        term = lax.dot_general(weight, near[k][...], NT, preferred_element_type=F32)
        mixed = term if mixed is None else mixed + term
    out[...] = mixed


def output_kernel(meta, weights, half, far, out):
    mixed = half[...]
    for k in range(NX):
        weight = weights[meta[PLACE] ^ (k * NC + 1)]
        mixed = mixed + lax.dot_general(weight, far[k], NT, preferred_element_type=F32)
    out[...] = mixed.astype(BF16)


def after(x, *others):
    return lax.optimization_barrier((x, *others))[0]


def in_hbm(x):
    return pltpu.with_memory_space_constraint(x, pltpu.HBM)


def sent(x, axis, size, k):
    return lax.ppermute(x, axis, [(i, i ^ k) for i in range(size)])


def shifted(x, k):
    return lax.ppermute(x, "z", [(i, (i + k) % NZ) for i in range(NZ)])


def local(
    pool_latent,
    pool_rope,
    q_nope,
    q_rope,
    w_uk,
    w_uv,
    w_o,
    block_table,
    lengths,
    preempted,
    assignment,
):
    groups = lax.axis_size("grp")
    group = lax.axis_index("grp")
    column = lax.axis_index(DEV)
    place = lax.axis_index(XC)
    pages_dev, block, width = pool_latent.shape
    requests = preempted.shape[0]
    blocks = block_table.shape[1]
    per_group = requests // groups
    query_rows = q_nope.shape[0] // requests
    rows = per_group * query_rows
    pair = 2 * query_rows
    scale = 1.0 / math.sqrt(DN + DR)
    page_rows = block + DR // 2

    small = pltpu.CompilerParams(vmem_limit_bytes=16 << 20)
    ids = jnp.stack([group, column]).astype(jnp.int32)
    page_type = jax.ShapeDtypeStruct((page_rows, width), BF16)
    meta, copies, *packed = pl.pallas_call(
        functools.partial(prepare_kernel, groups=groups),
        out_shape=[
            jax.ShapeDtypeStruct((META,), jnp.int32),
            jax.ShapeDtypeStruct((NX, 3 * rows + 4 * width, DN), BF16),
        ]
        + [page_type] * groups,
        in_specs=[spec(SMEM)] + [spec(pltpu.HBM)] * 10,
        out_specs=[spec(SMEM)] + [spec(VMEM)] * (1 + groups),
        scratch_shapes=[
            SMEM(block_table.T.shape, jnp.int32),
            SMEM(lengths.shape, jnp.int32),
            SMEM(preempted.shape, jnp.int32),
            SMEM(assignment.shape, jnp.int32),
            VMEM(pool_latent.shape, BF16),
            VMEM(pool_rope.shape, BF16),
            pltpu.SemaphoreType.DMA((2,)),
            pltpu.SemaphoreType.DMA((per_group, 3)),
            pltpu.SemaphoreType.DMA((4,)),
            pltpu.SemaphoreType.DMA((NX, 4)),
        ],
        compiler_params=small,
        name="prepare",
    )(ids, *[in_hbm(a) for a in (block_table.T, lengths, preempted, assignment, pool_latent, pool_rope, q_nope, q_rope, w_uk, w_uv)])

    arrived = [packed[0]] + [
        lax.ppermute(packed[k], "grp", [(i, (i + k) % groups) for i in range(groups)])
        for k in range(1, groups)
    ]
    near_x = lax.all_to_all(copies, "x", split_axis=0, concat_axis=0)

    share = w_o.shape[1] // (NZ * NXC)
    w_cols = pl.pallas_call(
        columns_kernel,
        out_shape=jax.ShapeDtypeStruct((NXC, NZ * share, w_o.shape[0]), BF16),
        in_specs=[spec(pltpu.HBM)],
        out_specs=spec(VMEM),
        scratch_shapes=[
            VMEM(w_o.shape, BF16),
            VMEM(w_o.shape[::-1], BF16),
            pltpu.SemaphoreType.DMA,
        ],
        compiler_params=pltpu.CompilerParams(vmem_limit_bytes=24 << 20),
        name="columns",
    )(in_hbm(after(w_o, packed[0])))
    arrived, w_cols = lax.optimization_barrier((arrived, w_cols))

    half_page = jax.ShapeDtypeStruct((page_rows // 2, width), BF16)
    halves = pl.pallas_call(
        pick_kernel,
        out_shape=[half_page] * 2,
        in_specs=[spec(SMEM)] + [spec(VMEM)] * groups,
        out_specs=[spec(VMEM)] * 2,
        compiler_params=small,
        name="pick",
    )(meta, *arrived)

    below, above = [halves], [halves]
    for k in range(1, NZ // 2):
        below.append([shifted(h, 1) for h in below[-1]])
        above.append([shifted(h, -1) for h in above[-1]])
    middle = [shifted(below[-1][0], 1), shifted(above[-1][1], -1)]
    pages = [halves] + above[1:] + [middle] + below[:0:-1]

    far_x = sent(after(near_x, above[2], below[2]), "c", NC, 1)
    w_cols = after(w_cols, near_x)
    weights = lax.all_to_all(w_cols, XC, split_axis=0, concat_axis=0)

    query = pl.pallas_call(
        query_kernel,
        out_shape=jax.ShapeDtypeStruct((per_group, NXC * pair, width + 2 * DR), BF16),
        in_specs=[spec(SMEM)] + [spec(pl.ANY)] * 2,
        out_specs=spec(VMEM),
        scratch_shapes=[
            VMEM((NXC, 3 * rows + 2 * width, DN), BF16),
            pltpu.SemaphoreType.DMA((NXC,)),
        ],
        compiler_params=small,
        name="query",
    )(meta, in_hbm(near_x), in_hbm(far_x))

    half_type = jax.ShapeDtypeStruct((NX, rows + TAIL, 2 * DV), BF16)
    keep, send = pl.pallas_call(
        functools.partial(attention_kernel, scale=scale),
        out_shape=[half_type, half_type],
        in_specs=[spec(SMEM), spec(VMEM)] + [spec(pl.ANY)] * (2 + 2 * NZ),
        out_specs=[spec(VMEM)] * 2,
        scratch_shapes=[
            VMEM((per_group, NXC * pair, width), F32),
            VMEM((per_group, NXC * pair, 128), F32),
            VMEM((per_group, NXC * pair, 128), F32),
            VMEM((NZ, page_rows, width), BF16),
            VMEM((NXC, 2 * width, DV), BF16),
            pltpu.SemaphoreType.DMA((NZ, 2)),
            pltpu.SemaphoreType.DMA((NXC,)),
        ],
        compiler_params=pltpu.CompilerParams(vmem_limit_bytes=32 << 20),
        name="attention",
    )(meta, query, in_hbm(near_x), in_hbm(far_x), *[p[0] for p in pages], *[p[1] for p in pages])

    got = sent(send, "c", NC, 1)
    part_type = jax.ShapeDtypeStruct((rows + TAIL, 2 * DV), BF16)
    chip = pl.pallas_call(
        chip_kernel,
        out_shape=[part_type] * NX,
        in_specs=[spec(VMEM)] * 2,
        out_specs=[spec(VMEM)] * NX,
        compiler_params=small,
        name="chip",
    )(keep, got)
    heads = pl.pallas_call(
        heads_kernel,
        out_shape=jax.ShapeDtypeStruct((rows, 2 * DV), BF16),
        in_specs=[spec(VMEM)] * NX,
        out_specs=spec(VMEM),
        compiler_params=small,
        name="heads",
    )(chip[0], *[sent(chip[k], "x", NX, k) for k in range(1, NX)])
    heads, weights = lax.optimization_barrier((heads, weights))
    near = [heads] + [sent(heads, "x", NX, k) for k in range(1, NX)]
    far = sent(jnp.stack(near), "c", NC, 1)
    half = pl.pallas_call(
        near_kernel,
        out_shape=jax.ShapeDtypeStruct((NZ * share, rows), F32),
        in_specs=[spec(SMEM)] + [spec(VMEM)] * (NX + 1),
        out_specs=spec(VMEM),
        compiler_params=small,
        name="near",
    )(meta, weights, *near)
    mixed = pl.pallas_call(
        output_kernel,
        out_shape=jax.ShapeDtypeStruct((NZ * share, rows), BF16),
        in_specs=[spec(SMEM)] + [spec(VMEM)] * 3,
        out_specs=spec(VMEM),
        compiler_params=small,
        name="output",
    )(meta, weights, half, far)
    mixed = lax.all_to_all(mixed, "z", split_axis=0, concat_axis=0, tiled=True)
    mixed = mixed.reshape(NZ, -1, rows).astype(F32).sum(axis=0)
    return mixed.T.astype(BF16)


def solution(mesh):
    split = Mesh(mesh.devices.reshape(mesh.shape["grp"], NZ, NX, NC), GRP_DEV)
    return jax.shard_map(
        local,
        mesh=split,
        in_specs=(
            P(GRP_DEV, None, None),
            P(GRP_DEV, None, None),
            P(None, DEV),
            P(None, DEV),
            P(None, DEV),
            P(None, DEV),
            P(DEV, None),
            P(),
            P(),
            P(),
            P(),
        ),
        out_specs=P("grp", DEV),
        check_vma=False,
    )
```

```python
import functools
import math

import jax
import jax.numpy as jnp
from jax import lax
from jax.experimental import pallas as pl
from jax.experimental.pallas import tpu as pltpu
from jax.sharding import Mesh
from jax.sharding import PartitionSpec as P

DR = 64
DN = 128
DV = 128
NEG = -1e30
LOG2E = math.log2(math.e)
NZ, NX, NC = 8, 4, 2
NXC = NX * NC
DEV = ("z", "x", "c")
GRP_DEV = ("grp", "z", "x", "c")
XC = ("x", "c")
SMEM = pltpu.SMEM
VMEM = pltpu.VMEM
F32 = jnp.float32
BF16 = jnp.bfloat16
NT = (((1,), (1,)), ((), ()))


def spec(space):
    return pl.BlockSpec(memory_space=space)


SEND, PICK, PLACE, SPOT, RANK, VALID, MEMBER, COUNT, SPARE = 0, 4, 5, 6, 8, 16, 24, 32, 40
META = 41
TAIL = 16


def fill_members(meta, ids, assignment):
    for i in range(SPARE):
        meta[i] = 0

    def one_request(i, carry):
        owner = assignment[i]
        rank = meta[COUNT + owner]
        meta[COUNT + owner] = rank + 1
        meta[jnp.where(owner == ids[0], MEMBER + rank, SPARE)] = i
        return carry

    lax.fori_loop(0, assignment.shape[0], one_request, 0)


def fill_table(meta, ids, table, lengths, preempted, assignment, *, groups, block, pages_dev):
    group, column = ids[0], ids[1]
    blocks = table.shape[0]
    columns = NZ * NXC
    me = group * columns + column
    place = column & (NXC - 1)
    plane = lax.shift_right_logical(column, NXC.bit_length() - 1)
    meta[PLACE] = place
    meta[SPOT] = lax.shift_right_logical(place, NC.bit_length() - 1)

    def one_request(i, carry):
        slot = preempted[i]
        owner = assignment[i]
        ahead = SEND + ((owner - group) & (groups - 1))
        for b in range(blocks):
            page = table[b, slot]
            holder = lax.shift_right_logical(page, pages_dev.bit_length() - 1)
            meta[jnp.where(holder == me, ahead, SPARE)] = page & (pages_dev - 1)

        return carry

    lax.fori_loop(0, preempted.shape[0], one_request, 0)

    def one_member(rank, carry):
        slot = preempted[meta[MEMBER + rank]]
        length = lengths[slot]
        for b in range(blocks):
            holder = lax.shift_right_logical(table[b, slot], pages_dev.bit_length() - 1)
            col = holder & (columns - 1)
            row = lax.shift_right_logical(holder, columns.bit_length() - 1)
            z = (lax.shift_right_logical(col, NXC.bit_length() - 1) - plane) & (NZ - 1)
            near = (col & (NXC - 1)) == place
            meta[jnp.where(near, RANK + z, SPARE)] = rank
            meta[jnp.where(near, VALID + z, SPARE)] = jnp.clip(length - b * block, 0, block)
            meta[jnp.where(col == column, PICK, SPARE)] = (group - row) & (groups - 1)

        return carry

    lax.fori_loop(0, preempted.shape[0] // groups, one_member, 0)


def package_kernel(ids, owners, q_nope, q_rope, w_uk, w_uv, copies, assignment, meta, row_sem, w_sem, sem):
    depth = w_uk.shape[0]
    queries = copies.shape[1] - 4 * depth
    rows = queries // 3
    q_rows = q_nope.shape[0] // assignment.shape[0]
    first = pltpu.make_async_copy(owners, assignment, sem)
    for_all = [
        pltpu.make_async_copy(
            w.at[:, pl.ds(h * DN, DN)],
            copies.at[k, pl.ds(queries + (2 * i + h) * depth, depth), :],
            w_sem.at[k, 2 * i + h],
        )
        for i, w in enumerate((w_uk, w_uv))
        for h in range(2)
        for k in range(copies.shape[0])
    ]
    for load in [first] + for_all:
        load.start()
    first.wait()
    fill_members(meta, ids, assignment)
    moves = []
    for r in range(rows // q_rows):
        start = pl.multiple_of(meta[MEMBER + r] * q_rows, q_rows)
        for j in range(3):
            source = q_rope if j == 2 else q_nope.at[:, pl.ds(j * DN, DN)]
            moves.append(
                pltpu.make_async_copy(
                    source.at[pl.ds(start, q_rows), :],
                    copies.at[0, pl.ds(j * rows + r * q_rows, q_rows), :],
                    row_sem.at[r, j],
                )
            )
    for move in moves:
        move.start()
    for move in moves:
        move.wait()
    for k in range(1, copies.shape[0]):
        copies[k, :queries, :] = copies[0, :queries, :]
    for load in for_all:
        load.wait()


def prepare_kernel(ids, *refs, groups):
    tables_hbm, (latent_hbm, rope_hbm), rest = refs[:4], refs[4:6], refs[6:]
    meta, outs = rest[0], rest[1 : 1 + groups]
    table, lengths, preempted, assignment, latent, rope, sem, table_sem = rest[1 + groups :]
    tables = (table, lengths, preempted, assignment)
    pages_dev, block, _ = latent.shape
    half = rope.shape[1] // 2
    loads = [
        pltpu.make_async_copy(latent_hbm, latent, sem.at[0]),
        pltpu.make_async_copy(rope_hbm, rope, sem.at[1]),
    ]
    first = [
        pltpu.make_async_copy(src, dst, table_sem.at[i])
        for i, (src, dst) in enumerate(zip(tables_hbm, tables))
    ]
    for load in first + loads:
        load.start()
    for load in first:
        load.wait()
    fill_members(meta, ids, assignment)
    fill_table(
        meta, ids, table, lengths, preempted, assignment,
        groups=groups, block=block, pages_dev=pages_dev,
    )
    for load in loads:
        load.wait()
    for k, out in enumerate(outs):
        page = meta[SEND + k]
        out[:block, :] = latent[page]
        out[block:, :block] = rope[page, :half, :]
        out[block:, block:] = rope[page, half:, :]


def pick_kernel(meta, *rest):
    sources, (first, second) = rest[:-2], rest[-2:]
    half = first.shape[0]
    for k, source in enumerate(sources):

        @pl.when(meta[PICK] == k)
        def _():
            first[...] = source[:half, :]
            second[...] = source[half:, :]


def placed(near, far, s, meta):
    return (near, far)[s % NC].at[meta[SPOT] ^ (s // NC)]


def query_kernel(meta, near, far, out, got, sem):
    per_group = out.shape[0]
    pair = out.shape[1] // NXC
    q_rows = pair // 2
    width = out.shape[2] - 2 * DR
    rows = per_group * q_rows
    loads = [
        pltpu.make_async_copy(
            placed(near, far, s, meta).at[pl.ds(0, got.shape[1]), :], got.at[s], sem.at[s]
        )
        for s in range(NXC)
    ]
    for load in loads:
        load.start()
    lane = lax.broadcasted_iota(jnp.int32, (rows, 2 * DR), 1)
    for s in range(NXC):
        loads[s].wait()
        hi = got[s, 2 * rows : 3 * rows, :]
        for h in range(2):
            live = (lane >= h * DR) & (lane < (h + 1) * DR)
            tail = jnp.where(live, hi, jnp.zeros_like(hi))
            key = 3 * rows + h * width
            lat = lax.dot_general(
                got[s, h * rows : (h + 1) * rows, :],
                got[s, key : key + width, :],
                NT,
                preferred_element_type=F32,
            ).astype(BF16)
            lo = s * pair + h * q_rows
            out[:, lo : lo + q_rows, :width] = lat.reshape(per_group, q_rows, width)
            out[:, lo : lo + q_rows, width:] = tail.reshape(per_group, q_rows, 2 * DR)


def three_parts(x):
    high = x.astype(BF16).astype(F32)
    rest = x - high
    middle = rest.astype(BF16).astype(F32)
    return [high, middle, rest - middle]


def stored_stats(stats):
    rows = [p for s in stats for p in three_parts(s)]
    fill = jnp.zeros((TAIL - len(rows), rows[0].shape[1]), F32)
    return jnp.concatenate(rows + [fill], axis=0).astype(BF16)


def read_stats(tail):
    tail = tail.astype(F32)
    return [tail[3 * h : 3 * h + 1] + tail[3 * h + 1 : 3 * h + 2] + tail[3 * h + 2 : 3 * h + 3] for h in range(2)]


def attention_kernel(meta, query, *rest, scale):
    near, far, firsts, seconds = *rest[:2], rest[2 : 2 + NZ], rest[2 + NZ : -9]
    keep, send, acc, top, total, pages, w_uv, sem, w_sem = rest[-9:]
    per_group, heads_rows, width = acc.shape
    q_rows = heads_rows // (2 * NXC)
    rows = per_group * q_rows
    block = pages.shape[1] * 8 // 9

    middle = NZ // 2
    order = [0] + [z for k in range(1, middle) for z in (k, NZ - k)] + [middle]
    split = pages.shape[1] // 2
    loads = [
        [
            pltpu.make_async_copy(firsts[z], pages.at[i, pl.ds(0, split), :], sem.at[i, 0]),
            pltpu.make_async_copy(seconds[z], pages.at[i, pl.ds(split, split), :], sem.at[i, 1]),
        ]
        for i, z in enumerate(order)
    ]
    loads_w = [
        pltpu.make_async_copy(
            placed(near, far, s, meta).at[pl.ds(near.shape[1] - 2 * width, 2 * width), :],
            w_uv.at[s],
            w_sem.at[s],
        )
        for s in range(NXC)
    ]
    for load in [load for pair in loads for load in pair] + loads_w:
        load.start()

    ranks = [meta[RANK + z] for z in order]
    valids = [meta[VALID + z] for z in order]
    for r in range(per_group):
        held = [(ranks[z] == r) & (valids[z] > 0) for z in range(NZ)]

        @pl.when(jnp.logical_not(functools.reduce(jnp.logical_or, held)))
        def _():
            acc[r] = jnp.zeros(acc.shape[1:], F32)
            top[r] = jnp.full(top.shape[1:], NEG, F32)
            total[r] = jnp.zeros(total.shape[1:], F32)

    def one_page(i, r, valid, first):
        latent = pages[i, :block, :]
        tail = pages[i, block:, :]
        rope = jnp.concatenate([tail[:, :block], tail[:, block:]], axis=0)
        rope = jnp.concatenate([rope, rope], axis=0)
        q = query[r]
        score = lax.dot_general(q[:, :width], latent, NT, preferred_element_type=F32)
        score = score + jnp.dot(q[:, width:], rope, preferred_element_type=F32)
        token = lax.broadcasted_iota(jnp.int32, score.shape, 1)
        score = jnp.where(token < valid, score * (scale * LOG2E), NEG)
        new = jnp.max(score, axis=1, keepdims=True)
        if not first:
            old = top[r][:, :1]
            new = jnp.maximum(old, new)
            fade = jnp.exp2(old - new)
        expo = jnp.exp2(score - new)
        weight = jnp.sum(expo, axis=1, keepdims=True)
        value = jnp.dot(expo.astype(BF16), latent, preferred_element_type=F32)
        top[r] = jnp.broadcast_to(new, top.shape[1:])
        if first:
            total[r] = jnp.broadcast_to(weight, total.shape[1:])
            acc[r] = value
        else:
            total[r] = total[r] * fade + weight
            acc[r] = acc[r] * fade + value

    def one_step(i, carry):
        z = jnp.where(i & 1 == 1, (i + 1) // 2, (NZ - i // 2) & (NZ - 1))
        r, valid = meta[RANK + z], meta[VALID + z]
        earlier = [(p < i) & (ranks[p] == r) & (valids[p] > 0) for p in range(NZ)]
        again = functools.reduce(jnp.logical_or, earlier)

        @pl.when((valid > 0) & jnp.logical_not(again))
        def _():
            one_page(i, r, valid, True)

        @pl.when((valid > 0) & again)
        def _():
            one_page(i, r, valid, False)

        return carry

    for load in [load for pair in loads for load in pair]:
        load.wait()
    lax.fori_loop(0, NZ, one_step, 0)

    lane = lax.broadcasted_iota(jnp.int32, (rows, total.shape[2]), 1)
    weights = jnp.zeros(lane.shape, F32)
    highs = jnp.full(lane.shape, NEG, F32)
    for j in range(2 * NXC):
        part = slice(j * q_rows, (j + 1) * q_rows)
        weights = jnp.where(lane == j, total[:, part, :].reshape(lane.shape), weights)
        highs = jnp.where(lane == j, top[:, part, :].reshape(lane.shape), highs)
    some = weights > 0.0
    safe = jnp.where(some, weights, 1.0)
    shares = 1.0 / safe
    stats = jnp.where(some, highs * (1.0 / LOG2E) + jnp.log(safe), NEG).T
    for s in range(NXC):
        out = keep if s % 2 == 0 else send
        loads_w[s].wait()
        for h in range(2):
            j = 2 * s + h
            value = acc[:, j * q_rows : (j + 1) * q_rows, :].reshape(rows, width)
            value = (value * shares[:, j : j + 1]).astype(BF16)
            head = jnp.dot(value, w_uv[s, h * width : (h + 1) * width, :], preferred_element_type=F32)
            out[s // 2, :rows, h * DV : (h + 1) * DV] = head.astype(BF16)
        out[s // 2, rows:, :] = stored_stats([stats[2 * s + h : 2 * s + h + 1, :] for h in range(2)])


def merge(parts, tails):
    rows = parts[0].shape[0]
    stats = [read_stats(t) for t in tails]
    high = [functools.reduce(jnp.maximum, [s[h] for s in stats]) for h in range(2)]
    shares = [[jnp.exp(s[h] - high[h]) for s in stats] for h in range(2)]
    whole = [functools.reduce(jnp.add, shares[h]) for h in range(2)]
    lines = [w / whole[h] for h in range(2) for w in shares[h]]
    fill = jnp.zeros((128 - len(lines), rows), F32)
    table = jnp.concatenate(lines + [fill], axis=0).T
    halves = []
    for h in range(2):
        sides = [p[:, h * DV : (h + 1) * DV].astype(F32) for p in parts]
        first = h * len(parts)
        halves.append(sum(table[:, first + i : first + i + 1] * p for i, p in enumerate(sides)))
    return halves, [high[h] + jnp.log(whole[h]) for h in range(2)]


def chip_kernel(keep, got, *outs):
    for k, out in enumerate(outs):
        rows = out.shape[0] - TAIL
        halves, stats = merge(
            [keep[k, :rows, :], got[k, :rows, :]], [keep[k, rows:, :], got[k, rows:, :]]
        )
        for h, half in enumerate(halves):
            out[:rows, h * DV : (h + 1) * DV] = half.astype(BF16)
        out[rows:, :] = stored_stats(stats)


def heads_kernel(*refs):
    parts, out = refs[:-1], refs[-1]
    rows = out.shape[0]
    halves, _ = merge([p[:rows, :] for p in parts], [p[rows:, :] for p in parts])
    for h, half in enumerate(halves):
        out[:, h * DV : (h + 1) * DV] = half.astype(BF16)


def columns_kernel(w_hbm, out, wide, tall, sem):
    load = pltpu.make_async_copy(w_hbm, wide, sem)
    load.start()
    load.wait()
    step = 256
    for i in range(wide.shape[1] // step):
        tall[i * step : (i + 1) * step, :] = wide[:, i * step : (i + 1) * step].T
    share = out.shape[1] // NZ
    for z in range(NZ):
        for s in range(NXC):
            at = (z * NXC + s) * share
            out[s, z * share : (z + 1) * share, :] = tall[at : at + share, :]


def output_kernel(meta, weights, *refs):
    near, far, out = refs[:NX], *refs[NX:]
    block = out.shape[0] // NX
    for i in range(NX):
        part = slice(i * block, (i + 1) * block)
        mixed = None
        for s in range(NXC):
            heads = near[s // NC][...] if s % NC == 0 else far[s // NC]
            weight = weights[meta[PLACE] ^ s, part, :]
            term = lax.dot_general(weight, heads, NT, preferred_element_type=F32)
            mixed = term if mixed is None else mixed + term
        out[part, :] = mixed.astype(BF16)


def after(x, *others):
    return lax.optimization_barrier((x, *others))[0]


def in_hbm(x):
    return pltpu.with_memory_space_constraint(x, pltpu.HBM)


def sent(x, axis, size, k):
    return lax.ppermute(x, axis, [(i, i ^ k) for i in range(size)])


def shifted(x, k):
    return lax.ppermute(x, "z", [(i, (i + k) % NZ) for i in range(NZ)])


def local(
    pool_latent,
    pool_rope,
    q_nope,
    q_rope,
    w_uk,
    w_uv,
    w_o,
    block_table,
    lengths,
    preempted,
    assignment,
):
    groups = lax.axis_size("grp")
    group = lax.axis_index("grp")
    column = lax.axis_index(DEV)
    place = lax.axis_index(XC)
    pages_dev, block, width = pool_latent.shape
    requests = preempted.shape[0]
    blocks = block_table.shape[1]
    per_group = requests // groups
    query_rows = q_nope.shape[0] // requests
    rows = per_group * query_rows
    pair = 2 * query_rows
    scale = 1.0 / math.sqrt(DN + DR)
    page_rows = block + DR // 2

    small = pltpu.CompilerParams(vmem_limit_bytes=16 << 20)
    ids = jnp.stack([group, column]).astype(jnp.int32)
    page_type = jax.ShapeDtypeStruct((page_rows, width), BF16)
    copies = pl.pallas_call(
        package_kernel,
        out_shape=jax.ShapeDtypeStruct((NX, 3 * rows + 4 * width, DN), BF16),
        in_specs=[spec(SMEM)] + [spec(pltpu.HBM)] * 5,
        out_specs=spec(VMEM),
        scratch_shapes=[
            SMEM(assignment.shape, jnp.int32),
            SMEM((META,), jnp.int32),
            pltpu.SemaphoreType.DMA((per_group, 3)),
            pltpu.SemaphoreType.DMA((NX, 4)),
            pltpu.SemaphoreType.DMA,
        ],
        compiler_params=small,
        name="package",
    )(ids, *[in_hbm(a) for a in (assignment, q_nope, q_rope, w_uk, w_uv)])

    meta, *packed = pl.pallas_call(
        functools.partial(prepare_kernel, groups=groups),
        out_shape=[jax.ShapeDtypeStruct((META,), jnp.int32)] + [page_type] * groups,
        in_specs=[spec(SMEM)] + [spec(pltpu.HBM)] * 6,
        out_specs=[spec(SMEM)] + [spec(VMEM)] * groups,
        scratch_shapes=[
            SMEM(block_table.T.shape, jnp.int32),
            SMEM(lengths.shape, jnp.int32),
            SMEM(preempted.shape, jnp.int32),
            SMEM(assignment.shape, jnp.int32),
            VMEM(pool_latent.shape, BF16),
            VMEM(pool_rope.shape, BF16),
            pltpu.SemaphoreType.DMA((2,)),
            pltpu.SemaphoreType.DMA((4,)),
        ],
        compiler_params=small,
        name="prepare",
    )(ids, *[in_hbm(a) for a in (block_table.T, lengths, preempted, assignment, pool_latent, pool_rope)])

    arrived = [packed[0]] + [
        lax.ppermute(packed[k], "grp", [(i, (i + k) % groups) for i in range(groups)])
        for k in range(1, groups)
    ]
    near_x = lax.all_to_all(copies, "x", split_axis=0, concat_axis=0)

    share = w_o.shape[1] // (NZ * NXC)
    w_cols = pl.pallas_call(
        columns_kernel,
        out_shape=jax.ShapeDtypeStruct((NXC, NZ * share, w_o.shape[0]), BF16),
        in_specs=[spec(pltpu.HBM)],
        out_specs=spec(VMEM),
        scratch_shapes=[
            VMEM(w_o.shape, BF16),
            VMEM(w_o.shape[::-1], BF16),
            pltpu.SemaphoreType.DMA,
        ],
        compiler_params=pltpu.CompilerParams(vmem_limit_bytes=24 << 20),
        name="columns",
    )(in_hbm(after(w_o, packed[0])))
    arrived, w_cols = lax.optimization_barrier((arrived, w_cols))

    half_page = jax.ShapeDtypeStruct((page_rows // 2, width), BF16)
    halves = pl.pallas_call(
        pick_kernel,
        out_shape=[half_page] * 2,
        in_specs=[spec(SMEM)] + [spec(VMEM)] * groups,
        out_specs=[spec(VMEM)] * 2,
        compiler_params=small,
        name="pick",
    )(meta, *arrived)

    below, above = [halves], [halves]
    for k in range(1, NZ // 2):
        below.append([shifted(h, 1) for h in below[-1]])
        above.append([shifted(h, -1) for h in above[-1]])
    middle = [shifted(below[-1][0], 1), shifted(above[-1][1], -1)]
    pages = [halves] + above[1:] + [middle] + below[:0:-1]

    far_x = sent(after(near_x, above[1], below[1]), "c", NC, 1)
    w_cols = after(w_cols, near_x)
    weights = lax.all_to_all(w_cols, XC, split_axis=0, concat_axis=0)

    query = pl.pallas_call(
        query_kernel,
        out_shape=jax.ShapeDtypeStruct((per_group, NXC * pair, width + 2 * DR), BF16),
        in_specs=[spec(SMEM)] + [spec(pl.ANY)] * 2,
        out_specs=spec(VMEM),
        scratch_shapes=[
            VMEM((NXC, 3 * rows + 2 * width, DN), BF16),
            pltpu.SemaphoreType.DMA((NXC,)),
        ],
        compiler_params=small,
        name="query",
    )(meta, in_hbm(near_x), in_hbm(far_x))

    half_type = jax.ShapeDtypeStruct((NX, rows + TAIL, 2 * DV), BF16)
    keep, send = pl.pallas_call(
        functools.partial(attention_kernel, scale=scale),
        out_shape=[half_type, half_type],
        in_specs=[spec(SMEM), spec(VMEM)] + [spec(pl.ANY)] * (2 + 2 * NZ),
        out_specs=[spec(VMEM)] * 2,
        scratch_shapes=[
            VMEM((per_group, NXC * pair, width), F32),
            VMEM((per_group, NXC * pair, 128), F32),
            VMEM((per_group, NXC * pair, 128), F32),
            VMEM((NZ, page_rows, width), BF16),
            VMEM((NXC, 2 * width, DV), BF16),
            pltpu.SemaphoreType.DMA((NZ, 2)),
            pltpu.SemaphoreType.DMA((NXC,)),
        ],
        compiler_params=pltpu.CompilerParams(vmem_limit_bytes=32 << 20),
        name="attention",
    )(meta, query, in_hbm(near_x), in_hbm(far_x), *[p[0] for p in pages], *[p[1] for p in pages])

    got = sent(send, "c", NC, 1)
    part_type = jax.ShapeDtypeStruct((rows + TAIL, 2 * DV), BF16)
    chip = pl.pallas_call(
        chip_kernel,
        out_shape=[part_type] * NX,
        in_specs=[spec(VMEM)] * 2,
        out_specs=[spec(VMEM)] * NX,
        compiler_params=small,
        name="chip",
    )(keep, got)
    heads = pl.pallas_call(
        heads_kernel,
        out_shape=jax.ShapeDtypeStruct((rows, 2 * DV), BF16),
        in_specs=[spec(VMEM)] * NX,
        out_specs=spec(VMEM),
        compiler_params=small,
        name="heads",
    )(chip[0], *[sent(chip[k], "x", NX, k) for k in range(1, NX)])
    heads, weights = lax.optimization_barrier((heads, weights))
    near = [heads] + [sent(heads, "x", NX, k) for k in range(1, NX)]
    far = sent(jnp.stack(near), "c", NC, 1)
    mixed = pl.pallas_call(
        output_kernel,
        out_shape=jax.ShapeDtypeStruct((NZ * share, rows), BF16),
        in_specs=[spec(SMEM)] + [spec(VMEM)] * (NX + 2),
        out_specs=spec(VMEM),
        compiler_params=small,
        name="output",
    )(meta, weights, *near, far)
    mixed = lax.all_to_all(mixed, "z", split_axis=0, concat_axis=0, tiled=True)
    mixed = mixed.reshape(NZ, -1, rows).astype(F32).sum(axis=0)
    return mixed.T.astype(BF16)


def solution(mesh):
    split = Mesh(mesh.devices.reshape(mesh.shape["grp"], NZ, NX, NC), GRP_DEV)
    return jax.shard_map(
        local,
        mesh=split,
        in_specs=(
            P(GRP_DEV, None, None),
            P(GRP_DEV, None, None),
            P(None, DEV),
            P(None, DEV),
            P(None, DEV),
            P(None, DEV),
            P(DEV, None),
            P(),
            P(),
            P(),
            P(),
        ),
        out_specs=P("grp", DEV),
        check_vma=False,
    )
```

```python
import functools
import math

import jax
import jax.numpy as jnp
from jax import lax
from jax.experimental import pallas as pl
from jax.experimental.pallas import tpu as pltpu
from jax.sharding import Mesh
from jax.sharding import PartitionSpec as P

DR = 64
DN = 128
DV = 128
NEG = -1e30
LOG2E = math.log2(math.e)
NZ, NX, NC = 8, 4, 2
NXC = NX * NC
DEV = ("z", "x", "c")
GRP_DEV = ("grp", "z", "x", "c")
XC = ("x", "c")
SMEM = pltpu.SMEM
VMEM = pltpu.VMEM
F32 = jnp.float32
BF16 = jnp.bfloat16
NT = (((1,), (1,)), ((), ()))


def spec(space):
    return pl.BlockSpec(memory_space=space)


SEND, PICK, PLACE, SPOT, RANK, VALID, MEMBER, COUNT, SPARE = 0, 4, 5, 6, 8, 16, 24, 32, 40
META = 41
TAIL = 16


def fill_members(meta, ids, assignment):
    for i in range(SPARE):
        meta[i] = 0

    def one_request(i, carry):
        owner = assignment[i]
        rank = meta[COUNT + owner]
        meta[COUNT + owner] = rank + 1
        meta[jnp.where(owner == ids[0], MEMBER + rank, SPARE)] = i
        return carry

    lax.fori_loop(0, assignment.shape[0], one_request, 0)


def fill_table(meta, ids, table, lengths, preempted, assignment, *, groups, block, pages_dev):
    group, column = ids[0], ids[1]
    blocks = table.shape[0]
    columns = NZ * NXC
    me = group * columns + column
    place = column & (NXC - 1)
    plane = lax.shift_right_logical(column, NXC.bit_length() - 1)
    meta[PLACE] = place
    meta[SPOT] = lax.shift_right_logical(place, NC.bit_length() - 1)

    def one_request(i, carry):
        slot = preempted[i]
        owner = assignment[i]
        ahead = SEND + ((owner - group) & (groups - 1))
        for b in range(blocks):
            page = table[b, slot]
            holder = lax.shift_right_logical(page, pages_dev.bit_length() - 1)
            meta[jnp.where(holder == me, ahead, SPARE)] = page & (pages_dev - 1)

        return carry

    lax.fori_loop(0, preempted.shape[0], one_request, 0)

    def one_member(rank, carry):
        slot = preempted[meta[MEMBER + rank]]
        length = lengths[slot]
        for b in range(blocks):
            holder = lax.shift_right_logical(table[b, slot], pages_dev.bit_length() - 1)
            col = holder & (columns - 1)
            row = lax.shift_right_logical(holder, columns.bit_length() - 1)
            z = (lax.shift_right_logical(col, NXC.bit_length() - 1) - plane) & (NZ - 1)
            near = (col & (NXC - 1)) == place
            meta[jnp.where(near, RANK + z, SPARE)] = rank
            meta[jnp.where(near, VALID + z, SPARE)] = jnp.clip(length - b * block, 0, block)
            meta[jnp.where(col == column, PICK, SPARE)] = (group - row) & (groups - 1)

        return carry

    lax.fori_loop(0, preempted.shape[0] // groups, one_member, 0)


def prepare_kernel(ids, *refs, groups):
    tables_hbm, (latent_hbm, rope_hbm, q_nope, q_rope, w_uk, w_uv), rest = refs[:4], refs[4:10], refs[10:]
    meta, copies = rest[:2]
    outs = rest[2 : 2 + groups]
    table, lengths, preempted, assignment, latent, rope, sem, row_sem, table_sem, w_sem = rest[2 + groups :]
    tables = (table, lengths, preempted, assignment)
    pages_dev, block, _ = latent.shape
    half = rope.shape[1] // 2
    q_rows = q_nope.shape[0] // preempted.shape[0]
    depth = w_uk.shape[0]
    queries = copies.shape[1] - 4 * depth
    rows = queries // 3
    for_all = [
        pltpu.make_async_copy(
            w.at[:, pl.ds(h * DN, DN)],
            copies.at[k, pl.ds(queries + (2 * i + h) * depth, depth), :],
            w_sem.at[k, 2 * i + h],
        )
        for i, w in enumerate((w_uk, w_uv))
        for h in range(2)
        for k in range(copies.shape[0])
    ]
    loads = [
        pltpu.make_async_copy(latent_hbm, latent, sem.at[0]),
        pltpu.make_async_copy(rope_hbm, rope, sem.at[1]),
    ]
    first = [
        pltpu.make_async_copy(src, dst, table_sem.at[i])
        for i, (src, dst) in enumerate(zip(tables_hbm, tables))
    ]
    for load in first + loads + for_all:
        load.start()
    for load in first:
        load.wait()
    fill_members(meta, ids, assignment)
    moves = []
    for r in range(rows // q_rows):
        start = pl.multiple_of(meta[MEMBER + r] * q_rows, q_rows)
        for j in range(3):
            source = q_rope if j == 2 else q_nope.at[:, pl.ds(j * DN, DN)]
            moves.append(
                pltpu.make_async_copy(
                    source.at[pl.ds(start, q_rows), :],
                    copies.at[0, pl.ds(j * rows + r * q_rows, q_rows), :],
                    row_sem.at[r, j],
                )
            )
    for move in moves:
        move.start()
    fill_table(
        meta, ids, table, lengths, preempted, assignment,
        groups=groups, block=block, pages_dev=pages_dev,
    )
    for load in loads:
        load.wait()
    for k, out in enumerate(outs):
        page = meta[SEND + k]
        out[:block, :] = latent[page]
        out[block:, :block] = rope[page, :half, :]
        out[block:, block:] = rope[page, half:, :]
    for move in moves:
        move.wait()
    for k in range(1, copies.shape[0]):
        copies[k, :queries, :] = copies[0, :queries, :]
    for load in for_all:
        load.wait()


def pick_kernel(meta, *rest):
    sources, (first, second) = rest[:-2], rest[-2:]
    half = first.shape[0]
    for k, source in enumerate(sources):

        @pl.when(meta[PICK] == k)
        def _():
            first[...] = source[:half, :]
            second[...] = source[half:, :]


def placed(near, far, s, meta):
    return (near, far)[s % NC].at[meta[SPOT] ^ (s // NC)]


def query_kernel(meta, near, far, out, got, sem):
    per_group = out.shape[0]
    pair = out.shape[1] // NXC
    q_rows = pair // 2
    width = out.shape[2] - 2 * DR
    rows = per_group * q_rows
    loads = [
        pltpu.make_async_copy(
            placed(near, far, s, meta).at[pl.ds(0, got.shape[1]), :], got.at[s], sem.at[s]
        )
        for s in range(NXC)
    ]
    for load in loads:
        load.start()
    lane = lax.broadcasted_iota(jnp.int32, (rows, 2 * DR), 1)
    for s in range(NXC):
        loads[s].wait()
        hi = got[s, 2 * rows : 3 * rows, :]
        for h in range(2):
            live = (lane >= h * DR) & (lane < (h + 1) * DR)
            tail = jnp.where(live, hi, jnp.zeros_like(hi))
            key = 3 * rows + h * width
            lat = lax.dot_general(
                got[s, h * rows : (h + 1) * rows, :],
                got[s, key : key + width, :],
                NT,
                preferred_element_type=F32,
            ).astype(BF16)
            lo = s * pair + h * q_rows
            out[:, lo : lo + q_rows, :width] = lat.reshape(per_group, q_rows, width)
            out[:, lo : lo + q_rows, width:] = tail.reshape(per_group, q_rows, 2 * DR)


def three_parts(x):
    high = x.astype(BF16).astype(F32)
    rest = x - high
    middle = rest.astype(BF16).astype(F32)
    return [high, middle, rest - middle]


def stored_stats(stats):
    rows = [p for s in stats for p in three_parts(s)]
    fill = jnp.zeros((TAIL - len(rows), rows[0].shape[1]), F32)
    return jnp.concatenate(rows + [fill], axis=0).astype(BF16)


def read_stats(tail):
    tail = tail.astype(F32)
    return [tail[3 * h : 3 * h + 1] + tail[3 * h + 1 : 3 * h + 2] + tail[3 * h + 2 : 3 * h + 3] for h in range(2)]


def attention_kernel(meta, query, *rest, scale):
    near, far, firsts, seconds = *rest[:2], rest[2 : 2 + NZ], rest[2 + NZ : -9]
    keep, send, acc, top, total, pages, w_uv, sem, w_sem = rest[-9:]
    per_group, heads_rows, width = acc.shape
    q_rows = heads_rows // (2 * NXC)
    rows = per_group * q_rows
    block = pages.shape[1] * 8 // 9

    middle = NZ // 2
    order = [0] + [z for k in range(1, middle) for z in (k, NZ - k)] + [middle]
    split = pages.shape[1] // 2
    loads = [
        [
            pltpu.make_async_copy(firsts[z], pages.at[i, pl.ds(0, split), :], sem.at[i, 0]),
            pltpu.make_async_copy(seconds[z], pages.at[i, pl.ds(split, split), :], sem.at[i, 1]),
        ]
        for i, z in enumerate(order)
    ]
    loads_w = [
        pltpu.make_async_copy(
            placed(near, far, s, meta).at[pl.ds(near.shape[1] - 2 * width, 2 * width), :],
            w_uv.at[s],
            w_sem.at[s],
        )
        for s in range(NXC)
    ]
    for load in [load for pair in loads for load in pair] + loads_w:
        load.start()

    ranks = [meta[RANK + z] for z in order]
    valids = [meta[VALID + z] for z in order]
    for r in range(per_group):
        held = [(ranks[z] == r) & (valids[z] > 0) for z in range(NZ)]

        @pl.when(jnp.logical_not(functools.reduce(jnp.logical_or, held)))
        def _():
            acc[r] = jnp.zeros(acc.shape[1:], F32)
            top[r] = jnp.full(top.shape[1:], NEG, F32)
            total[r] = jnp.zeros(total.shape[1:], F32)

    def one_page(i, r, valid, first):
        latent = pages[i, :block, :]
        tail = pages[i, block:, :]
        rope = jnp.concatenate([tail[:, :block], tail[:, block:]], axis=0)
        rope = jnp.concatenate([rope, rope], axis=0)
        q = query[r]
        score = lax.dot_general(q[:, :width], latent, NT, preferred_element_type=F32)
        score = score + jnp.dot(q[:, width:], rope, preferred_element_type=F32)
        token = lax.broadcasted_iota(jnp.int32, score.shape, 1)
        score = jnp.where(token < valid, score * (scale * LOG2E), NEG)
        new = jnp.max(score, axis=1, keepdims=True)
        if not first:
            old = top[r][:, :1]
            new = jnp.maximum(old, new)
            fade = jnp.exp2(old - new)
        expo = jnp.exp2(score - new)
        weight = jnp.sum(expo, axis=1, keepdims=True)
        value = jnp.dot(expo.astype(BF16), latent, preferred_element_type=F32)
        top[r] = jnp.broadcast_to(new, top.shape[1:])
        if first:
            total[r] = jnp.broadcast_to(weight, total.shape[1:])
            acc[r] = value
        else:
            total[r] = total[r] * fade + weight
            acc[r] = acc[r] * fade + value

    def one_step(i, carry):
        z = jnp.where(i & 1 == 1, (i + 1) // 2, (NZ - i // 2) & (NZ - 1))
        r, valid = meta[RANK + z], meta[VALID + z]
        earlier = [(p < i) & (ranks[p] == r) & (valids[p] > 0) for p in range(NZ)]
        again = functools.reduce(jnp.logical_or, earlier)

        @pl.when((valid > 0) & jnp.logical_not(again))
        def _():
            one_page(i, r, valid, True)

        @pl.when((valid > 0) & again)
        def _():
            one_page(i, r, valid, False)

        return carry

    for load in [load for pair in loads for load in pair]:
        load.wait()
    lax.fori_loop(0, NZ, one_step, 0)

    lane = lax.broadcasted_iota(jnp.int32, (rows, total.shape[2]), 1)
    weights = jnp.zeros(lane.shape, F32)
    highs = jnp.full(lane.shape, NEG, F32)
    for j in range(2 * NXC):
        part = slice(j * q_rows, (j + 1) * q_rows)
        weights = jnp.where(lane == j, total[:, part, :].reshape(lane.shape), weights)
        highs = jnp.where(lane == j, top[:, part, :].reshape(lane.shape), highs)
    some = weights > 0.0
    safe = jnp.where(some, weights, 1.0)
    shares = 1.0 / safe
    stats = jnp.where(some, highs * (1.0 / LOG2E) + jnp.log(safe), NEG).T
    for s in range(NXC):
        out = keep if s % 2 == 0 else send
        loads_w[s].wait()
        for h in range(2):
            j = 2 * s + h
            value = acc[:, j * q_rows : (j + 1) * q_rows, :].reshape(rows, width)
            value = (value * shares[:, j : j + 1]).astype(BF16)
            head = jnp.dot(value, w_uv[s, h * width : (h + 1) * width, :], preferred_element_type=F32)
            out[s // 2, :rows, h * DV : (h + 1) * DV] = head.astype(BF16)
        out[s // 2, rows:, :] = stored_stats([stats[2 * s + h : 2 * s + h + 1, :] for h in range(2)])


def merge(parts, tails):
    rows = parts[0].shape[0]
    stats = [read_stats(t) for t in tails]
    high = [functools.reduce(jnp.maximum, [s[h] for s in stats]) for h in range(2)]
    shares = [[jnp.exp(s[h] - high[h]) for s in stats] for h in range(2)]
    whole = [functools.reduce(jnp.add, shares[h]) for h in range(2)]
    lines = [w / whole[h] for h in range(2) for w in shares[h]]
    fill = jnp.zeros((128 - len(lines), rows), F32)
    table = jnp.concatenate(lines + [fill], axis=0).T
    halves = []
    for h in range(2):
        sides = [p[:, h * DV : (h + 1) * DV].astype(F32) for p in parts]
        first = h * len(parts)
        halves.append(sum(table[:, first + i : first + i + 1] * p for i, p in enumerate(sides)))
    return halves, [high[h] + jnp.log(whole[h]) for h in range(2)]


def chip_kernel(keep, got, *outs):
    for k, out in enumerate(outs):
        rows = out.shape[0] - TAIL
        halves, stats = merge(
            [keep[k, :rows, :], got[k, :rows, :]], [keep[k, rows:, :], got[k, rows:, :]]
        )
        for h, half in enumerate(halves):
            out[:rows, h * DV : (h + 1) * DV] = half.astype(BF16)
        out[rows:, :] = stored_stats(stats)


def heads_kernel(*refs):
    parts, out = refs[:-1], refs[-1]
    rows = out.shape[0]
    halves, _ = merge([p[:rows, :] for p in parts], [p[rows:, :] for p in parts])
    for h, half in enumerate(halves):
        out[:, h * DV : (h + 1) * DV] = half.astype(BF16)


def columns_kernel(w_hbm, out, wide, tall, sem):
    load = pltpu.make_async_copy(w_hbm, wide, sem)
    load.start()
    load.wait()
    step = 256
    for i in range(wide.shape[1] // step):
        tall[i * step : (i + 1) * step, :] = wide[:, i * step : (i + 1) * step].T
    share = out.shape[1] // NZ
    for z in range(NZ):
        for s in range(NXC):
            at = (z * NXC + s) * share
            out[s, z * share : (z + 1) * share, :] = tall[at : at + share, :]


def output_kernel(meta, weights, near, far, out):
    block = out.shape[0] // NX
    spot = meta[SPOT]
    for c, sides in enumerate(((near, far), (far, near))):

        @pl.when((meta[PLACE] & (NC - 1)) == c)
        def _():
            heads = [sides[s % NC][spot ^ (s // NC)] for s in range(NXC)]
            for i in range(NX):
                part = slice(i * block, (i + 1) * block)
                mixed = None
                for s in range(NXC):
                    term = lax.dot_general(
                        weights[s, part, :], heads[s], NT, preferred_element_type=F32
                    )
                    mixed = term if mixed is None else mixed + term
                out[part, :] = mixed.astype(BF16)


def after(x, *others):
    return lax.optimization_barrier((x, *others))[0]


def in_hbm(x):
    return pltpu.with_memory_space_constraint(x, pltpu.HBM)


def sent(x, axis, size, k):
    return lax.ppermute(x, axis, [(i, i ^ k) for i in range(size)])


def shifted(x, k):
    return lax.ppermute(x, "z", [(i, (i + k) % NZ) for i in range(NZ)])


def local(
    pool_latent,
    pool_rope,
    q_nope,
    q_rope,
    w_uk,
    w_uv,
    w_o,
    block_table,
    lengths,
    preempted,
    assignment,
):
    groups = lax.axis_size("grp")
    group = lax.axis_index("grp")
    column = lax.axis_index(DEV)
    place = lax.axis_index(XC)
    pages_dev, block, width = pool_latent.shape
    requests = preempted.shape[0]
    blocks = block_table.shape[1]
    per_group = requests // groups
    query_rows = q_nope.shape[0] // requests
    rows = per_group * query_rows
    pair = 2 * query_rows
    scale = 1.0 / math.sqrt(DN + DR)
    page_rows = block + DR // 2

    small = pltpu.CompilerParams(vmem_limit_bytes=16 << 20)
    ids = jnp.stack([group, column]).astype(jnp.int32)
    page_type = jax.ShapeDtypeStruct((page_rows, width), BF16)
    meta, copies, *packed = pl.pallas_call(
        functools.partial(prepare_kernel, groups=groups),
        out_shape=[
            jax.ShapeDtypeStruct((META,), jnp.int32),
            jax.ShapeDtypeStruct((NX, 3 * rows + 4 * width, DN), BF16),
        ]
        + [page_type] * groups,
        in_specs=[spec(SMEM)] + [spec(pltpu.HBM)] * 10,
        out_specs=[spec(SMEM)] + [spec(VMEM)] * (1 + groups),
        scratch_shapes=[
            SMEM(block_table.T.shape, jnp.int32),
            SMEM(lengths.shape, jnp.int32),
            SMEM(preempted.shape, jnp.int32),
            SMEM(assignment.shape, jnp.int32),
            VMEM(pool_latent.shape, BF16),
            VMEM(pool_rope.shape, BF16),
            pltpu.SemaphoreType.DMA((2,)),
            pltpu.SemaphoreType.DMA((per_group, 3)),
            pltpu.SemaphoreType.DMA((4,)),
            pltpu.SemaphoreType.DMA((NX, 4)),
        ],
        compiler_params=small,
        name="prepare",
    )(ids, *[in_hbm(a) for a in (block_table.T, lengths, preempted, assignment, pool_latent, pool_rope, q_nope, q_rope, w_uk, w_uv)])

    arrived = [packed[0]] + [
        lax.ppermute(packed[k], "grp", [(i, (i + k) % groups) for i in range(groups)])
        for k in range(1, groups)
    ]
    near_x = lax.all_to_all(copies, "x", split_axis=0, concat_axis=0)

    share = w_o.shape[1] // (NZ * NXC)
    w_cols = pl.pallas_call(
        columns_kernel,
        out_shape=jax.ShapeDtypeStruct((NXC, NZ * share, w_o.shape[0]), BF16),
        in_specs=[spec(pltpu.HBM)],
        out_specs=spec(VMEM),
        scratch_shapes=[
            VMEM(w_o.shape, BF16),
            VMEM(w_o.shape[::-1], BF16),
            pltpu.SemaphoreType.DMA,
        ],
        compiler_params=pltpu.CompilerParams(vmem_limit_bytes=24 << 20),
        name="columns",
    )(in_hbm(after(w_o, packed[0])))
    arrived, w_cols = lax.optimization_barrier((arrived, w_cols))

    half_page = jax.ShapeDtypeStruct((page_rows // 2, width), BF16)
    halves = pl.pallas_call(
        pick_kernel,
        out_shape=[half_page] * 2,
        in_specs=[spec(SMEM)] + [spec(VMEM)] * groups,
        out_specs=[spec(VMEM)] * 2,
        compiler_params=small,
        name="pick",
    )(meta, *arrived)

    below, above = [halves], [halves]
    for k in range(1, NZ // 2):
        below.append([shifted(h, 1) for h in below[-1]])
        above.append([shifted(h, -1) for h in above[-1]])
    middle = [shifted(below[-1][0], 1), shifted(above[-1][1], -1)]
    pages = [halves] + above[1:] + [middle] + below[:0:-1]

    far_x = sent(after(near_x, above[2], below[2]), "c", NC, 1)
    w_cols = after(w_cols, near_x)
    weights = lax.all_to_all(w_cols, XC, split_axis=0, concat_axis=0)

    query = pl.pallas_call(
        query_kernel,
        out_shape=jax.ShapeDtypeStruct((per_group, NXC * pair, width + 2 * DR), BF16),
        in_specs=[spec(SMEM)] + [spec(pl.ANY)] * 2,
        out_specs=spec(VMEM),
        scratch_shapes=[
            VMEM((NXC, 3 * rows + 2 * width, DN), BF16),
            pltpu.SemaphoreType.DMA((NXC,)),
        ],
        compiler_params=small,
        name="query",
    )(meta, in_hbm(near_x), in_hbm(far_x))

    half_type = jax.ShapeDtypeStruct((NX, rows + TAIL, 2 * DV), BF16)
    keep, send = pl.pallas_call(
        functools.partial(attention_kernel, scale=scale),
        out_shape=[half_type, half_type],
        in_specs=[spec(SMEM), spec(VMEM)] + [spec(pl.ANY)] * (2 + 2 * NZ),
        out_specs=[spec(VMEM)] * 2,
        scratch_shapes=[
            VMEM((per_group, NXC * pair, width), F32),
            VMEM((per_group, NXC * pair, 128), F32),
            VMEM((per_group, NXC * pair, 128), F32),
            VMEM((NZ, page_rows, width), BF16),
            VMEM((NXC, 2 * width, DV), BF16),
            pltpu.SemaphoreType.DMA((NZ, 2)),
            pltpu.SemaphoreType.DMA((NXC,)),
        ],
        compiler_params=pltpu.CompilerParams(vmem_limit_bytes=32 << 20),
        name="attention",
    )(meta, query, in_hbm(near_x), in_hbm(far_x), *[p[0] for p in pages], *[p[1] for p in pages])

    got = sent(send, "c", NC, 1)
    part_type = jax.ShapeDtypeStruct((rows + TAIL, 2 * DV), BF16)
    chip = pl.pallas_call(
        chip_kernel,
        out_shape=[part_type] * NX,
        in_specs=[spec(VMEM)] * 2,
        out_specs=[spec(VMEM)] * NX,
        compiler_params=small,
        name="chip",
    )(keep, got)
    heads = pl.pallas_call(
        heads_kernel,
        out_shape=jax.ShapeDtypeStruct((rows, 2 * DV), BF16),
        in_specs=[spec(VMEM)] * NX,
        out_specs=spec(VMEM),
        compiler_params=small,
        name="heads",
    )(chip[0], *[sent(chip[k], "x", NX, k) for k in range(1, NX)])
    heads, weights = lax.optimization_barrier((heads, weights))
    near = [heads] + [sent(heads, "x", NX, k) for k in range(1, NX)]
    near = jnp.stack(near)
    mixed = pl.pallas_call(
        output_kernel,
        out_shape=jax.ShapeDtypeStruct((NZ * share, rows), BF16),
        in_specs=[spec(SMEM)] + [spec(VMEM)] * 3,
        out_specs=spec(VMEM),
        compiler_params=small,
        name="output",
    )(meta, weights, near, sent(near, "c", NC, 1))
    mixed = lax.all_to_all(mixed, "z", split_axis=0, concat_axis=0, tiled=True)
    mixed = mixed.reshape(NZ, -1, rows).astype(F32).sum(axis=0)
    return mixed.T.astype(BF16)


def solution(mesh):
    split = Mesh(mesh.devices.reshape(mesh.shape["grp"], NZ, NX, NC), GRP_DEV)
    return jax.shard_map(
        local,
        mesh=split,
        in_specs=(
            P(GRP_DEV, None, None),
            P(GRP_DEV, None, None),
            P(None, DEV),
            P(None, DEV),
            P(None, DEV),
            P(None, DEV),
            P(DEV, None),
            P(),
            P(),
            P(),
            P(),
        ),
        out_specs=P("grp", DEV),
        check_vma=False,
    )
```

```python
import functools
import math

import jax
import jax.numpy as jnp
from jax import lax
from jax.experimental import pallas as pl
from jax.experimental.pallas import tpu as pltpu
from jax.sharding import Mesh
from jax.sharding import PartitionSpec as P

DR = 64
DN = 128
DV = 128
NEG = -1e30
LOG2E = math.log2(math.e)
NZ, NX, NC = 8, 4, 2
NXC = NX * NC
DEV = ("z", "x", "c")
GRP_DEV = ("grp", "z", "x", "c")
XC = ("x", "c")
SMEM = pltpu.SMEM
VMEM = pltpu.VMEM
F32 = jnp.float32
BF16 = jnp.bfloat16
NT = (((1,), (1,)), ((), ()))


def spec(space):
    return pl.BlockSpec(memory_space=space)


SEND, PICK, PLACE, SPOT, RANK, VALID, MEMBER, COUNT, SPARE = 0, 4, 5, 6, 8, 16, 24, 32, 40
META = 41
TAIL = 16


def fill_members(meta, ids, assignment):
    for i in range(SPARE):
        meta[i] = 0

    def one_request(i, carry):
        owner = assignment[i]
        rank = meta[COUNT + owner]
        meta[COUNT + owner] = rank + 1
        meta[jnp.where(owner == ids[0], MEMBER + rank, SPARE)] = i
        return carry

    lax.fori_loop(0, assignment.shape[0], one_request, 0)


def fill_table(meta, ids, table, lengths, preempted, assignment, *, groups, block, pages_dev):
    group, column = ids[0], ids[1]
    blocks = table.shape[0]
    columns = NZ * NXC
    me = group * columns + column
    place = column & (NXC - 1)
    plane = lax.shift_right_logical(column, NXC.bit_length() - 1)
    meta[PLACE] = place
    meta[SPOT] = lax.shift_right_logical(place, NC.bit_length() - 1)

    def one_request(i, carry):
        slot = preempted[i]
        owner = assignment[i]
        ahead = SEND + ((owner - group) & (groups - 1))
        for b in range(blocks):
            page = table[b, slot]
            holder = lax.shift_right_logical(page, pages_dev.bit_length() - 1)
            meta[jnp.where(holder == me, ahead, SPARE)] = page & (pages_dev - 1)

        return carry

    lax.fori_loop(0, preempted.shape[0], one_request, 0)

    def one_member(rank, carry):
        slot = preempted[meta[MEMBER + rank]]
        length = lengths[slot]
        for b in range(blocks):
            holder = lax.shift_right_logical(table[b, slot], pages_dev.bit_length() - 1)
            col = holder & (columns - 1)
            row = lax.shift_right_logical(holder, columns.bit_length() - 1)
            z = (lax.shift_right_logical(col, NXC.bit_length() - 1) - plane) & (NZ - 1)
            near = (col & (NXC - 1)) == place
            meta[jnp.where(near, RANK + z, SPARE)] = rank
            meta[jnp.where(near, VALID + z, SPARE)] = jnp.clip(length - b * block, 0, block)
            meta[jnp.where(col == column, PICK, SPARE)] = (group - row) & (groups - 1)

        return carry

    lax.fori_loop(0, preempted.shape[0] // groups, one_member, 0)


def prepare_kernel(ids, *refs, groups):
    tables_hbm, (latent_hbm, rope_hbm, q_nope, q_rope, w_uk, w_uv), rest = refs[:4], refs[4:10], refs[10:]
    meta, copies = rest[:2]
    outs = rest[2 : 2 + groups]
    table, lengths, preempted, assignment, latent, rope, sem, row_sem, table_sem, w_sem = rest[2 + groups :]
    tables = (table, lengths, preempted, assignment)
    pages_dev, block, _ = latent.shape
    half = rope.shape[1] // 2
    q_rows = q_nope.shape[0] // preempted.shape[0]
    depth = w_uk.shape[0]
    queries = copies.shape[1] - 4 * depth
    rows = queries // 3
    for_all = [
        pltpu.make_async_copy(
            w.at[:, pl.ds(h * DN, DN)],
            copies.at[k, pl.ds(queries + (2 * i + h) * depth, depth), :],
            w_sem.at[k, 2 * i + h],
        )
        for i, w in enumerate((w_uk, w_uv))
        for h in range(2)
        for k in range(copies.shape[0])
    ]
    loads = [
        pltpu.make_async_copy(latent_hbm, latent, sem.at[0]),
        pltpu.make_async_copy(rope_hbm, rope, sem.at[1]),
    ]
    first = [
        pltpu.make_async_copy(src, dst, table_sem.at[i])
        for i, (src, dst) in enumerate(zip(tables_hbm, tables))
    ]
    for load in first + loads + for_all:
        load.start()
    for load in first:
        load.wait()
    fill_members(meta, ids, assignment)
    moves = []
    for r in range(rows // q_rows):
        start = pl.multiple_of(meta[MEMBER + r] * q_rows, q_rows)
        for j in range(3):
            source = q_rope if j == 2 else q_nope.at[:, pl.ds(j * DN, DN)]
            moves.append(
                pltpu.make_async_copy(
                    source.at[pl.ds(start, q_rows), :],
                    copies.at[0, pl.ds(j * rows + r * q_rows, q_rows), :],
                    row_sem.at[r, j],
                )
            )
    for move in moves:
        move.start()
    fill_table(
        meta, ids, table, lengths, preempted, assignment,
        groups=groups, block=block, pages_dev=pages_dev,
    )
    for load in loads:
        load.wait()
    for k, out in enumerate(outs):
        page = meta[SEND + k]
        out[:block, :] = latent[page]
        out[block:, :block] = rope[page, :half, :]
        out[block:, block:] = rope[page, half:, :]
    for move in moves:
        move.wait()
    for k in range(1, copies.shape[0]):
        copies[k, :queries, :] = copies[0, :queries, :]
    for load in for_all:
        load.wait()


def pick_kernel(meta, *rest):
    sources, (first, second) = rest[:-2], rest[-2:]
    half = first.shape[0]
    for k, source in enumerate(sources):

        @pl.when(meta[PICK] == k)
        def _():
            first[...] = source[:half, :]
            second[...] = source[half:, :]


def placed(near, far, s, meta):
    return (near, far)[s % NC].at[meta[SPOT] ^ (s // NC)]


def query_kernel(meta, near, far, out, got, sem):
    per_group = out.shape[0]
    pair = out.shape[1] // NXC
    q_rows = pair // 2
    width = out.shape[2] - 2 * DR
    rows = per_group * q_rows
    loads = [
        pltpu.make_async_copy(
            placed(near, far, s, meta).at[pl.ds(0, got.shape[1]), :], got.at[s], sem.at[s]
        )
        for s in range(NXC)
    ]
    for load in loads:
        load.start()
    lane = lax.broadcasted_iota(jnp.int32, (rows, 2 * DR), 1)
    for s in range(NXC):
        loads[s].wait()
        hi = got[s, 2 * rows : 3 * rows, :]
        for h in range(2):
            live = (lane >= h * DR) & (lane < (h + 1) * DR)
            tail = jnp.where(live, hi, jnp.zeros_like(hi))
            key = 3 * rows + h * width
            lat = lax.dot_general(
                got[s, h * rows : (h + 1) * rows, :],
                got[s, key : key + width, :],
                NT,
                preferred_element_type=F32,
            ).astype(BF16)
            lo = s * pair + h * q_rows
            out[:, lo : lo + q_rows, :width] = lat.reshape(per_group, q_rows, width)
            out[:, lo : lo + q_rows, width:] = tail.reshape(per_group, q_rows, 2 * DR)


def three_parts(x):
    high = x.astype(BF16).astype(F32)
    rest = x - high
    middle = rest.astype(BF16).astype(F32)
    return [high, middle, rest - middle]


def stored_stats(stats):
    rows = [p for s in stats for p in three_parts(s)]
    fill = jnp.zeros((TAIL - len(rows), rows[0].shape[1]), F32)
    return jnp.concatenate(rows + [fill], axis=0).astype(BF16)


def read_stats(tail):
    tail = tail.astype(F32)
    return [tail[3 * h : 3 * h + 1] + tail[3 * h + 1 : 3 * h + 2] + tail[3 * h + 2 : 3 * h + 3] for h in range(2)]


def attention_kernel(meta, query, *rest, scale):
    near, far, firsts, seconds = *rest[:2], rest[2 : 2 + NZ], rest[2 + NZ : -9]
    keep, send, acc, top, total, pages, w_uv, sem, w_sem = rest[-9:]
    per_group, heads_rows, width = acc.shape
    q_rows = heads_rows // (2 * NXC)
    rows = per_group * q_rows
    block = pages.shape[1] * 8 // 9

    middle = NZ // 2
    order = [0] + [z for k in range(1, middle) for z in (k, NZ - k)] + [middle]
    split = pages.shape[1] // 2
    loads = [
        [
            pltpu.make_async_copy(firsts[z], pages.at[i, pl.ds(0, split), :], sem.at[i, 0]),
            pltpu.make_async_copy(seconds[z], pages.at[i, pl.ds(split, split), :], sem.at[i, 1]),
        ]
        for i, z in enumerate(order)
    ]
    loads_w = [
        pltpu.make_async_copy(
            placed(near, far, s, meta).at[pl.ds(near.shape[1] - 2 * width, 2 * width), :],
            w_uv.at[s],
            w_sem.at[s],
        )
        for s in range(NXC)
    ]
    for load in [load for pair in loads for load in pair] + loads_w:
        load.start()

    ranks = [meta[RANK + z] for z in order]
    valids = [meta[VALID + z] for z in order]
    for r in range(per_group):
        held = [(ranks[z] == r) & (valids[z] > 0) for z in range(NZ)]

        @pl.when(jnp.logical_not(functools.reduce(jnp.logical_or, held)))
        def _():
            acc[r] = jnp.zeros(acc.shape[1:], F32)
            top[r] = jnp.full(top.shape[1:], NEG, F32)
            total[r] = jnp.zeros(total.shape[1:], F32)

    def one_page(i, r, valid, first):
        latent = pages[i, :block, :]
        tail = pages[i, block:, :]
        rope = jnp.concatenate([tail[:, :block], tail[:, block:]], axis=0)
        rope = jnp.concatenate([rope, rope], axis=0)
        q = query[r]
        score = lax.dot_general(q[:, :width], latent, NT, preferred_element_type=F32)
        score = score + jnp.dot(q[:, width:], rope, preferred_element_type=F32)
        token = lax.broadcasted_iota(jnp.int32, score.shape, 1)
        score = jnp.where(token < valid, score * (scale * LOG2E), NEG)
        new = jnp.max(score, axis=1, keepdims=True)
        if not first:
            old = top[r][:, :1]
            new = jnp.maximum(old, new)
            fade = jnp.exp2(old - new)
        expo = jnp.exp2(score - new)
        weight = jnp.sum(expo, axis=1, keepdims=True)
        value = jnp.dot(expo.astype(BF16), latent, preferred_element_type=F32)
        top[r] = jnp.broadcast_to(new, top.shape[1:])
        if first:
            total[r] = jnp.broadcast_to(weight, total.shape[1:])
            acc[r] = value
        else:
            total[r] = total[r] * fade + weight
            acc[r] = acc[r] * fade + value

    def one_step(i, carry):
        z = jnp.where(i & 1 == 1, (i + 1) // 2, (NZ - i // 2) & (NZ - 1))
        r, valid = meta[RANK + z], meta[VALID + z]
        earlier = [(p < i) & (ranks[p] == r) & (valids[p] > 0) for p in range(NZ)]
        again = functools.reduce(jnp.logical_or, earlier)

        @pl.when((valid > 0) & jnp.logical_not(again))
        def _():
            one_page(i, r, valid, True)

        @pl.when((valid > 0) & again)
        def _():
            one_page(i, r, valid, False)

        return carry

    for load in [load for pair in loads for load in pair]:
        load.wait()
    lax.fori_loop(0, NZ, one_step, 0)

    lane = lax.broadcasted_iota(jnp.int32, (rows, total.shape[2]), 1)
    weights = jnp.zeros(lane.shape, F32)
    highs = jnp.full(lane.shape, NEG, F32)
    for j in range(2 * NXC):
        part = slice(j * q_rows, (j + 1) * q_rows)
        weights = jnp.where(lane == j, total[:, part, :].reshape(lane.shape), weights)
        highs = jnp.where(lane == j, top[:, part, :].reshape(lane.shape), highs)
    some = weights > 0.0
    safe = jnp.where(some, weights, 1.0)
    shares = 1.0 / safe
    stats = jnp.where(some, highs * (1.0 / LOG2E) + jnp.log(safe), NEG).T
    for s in range(NXC):
        out = keep if s % 2 == 0 else send
        loads_w[s].wait()
        for h in range(2):
            j = 2 * s + h
            value = acc[:, j * q_rows : (j + 1) * q_rows, :].reshape(rows, width)
            value = (value * shares[:, j : j + 1]).astype(BF16)
            head = jnp.dot(value, w_uv[s, h * width : (h + 1) * width, :], preferred_element_type=F32)
            out[s // 2, :rows, h * DV : (h + 1) * DV] = head.astype(BF16)
        out[s // 2, rows:, :] = stored_stats([stats[2 * s + h : 2 * s + h + 1, :] for h in range(2)])


def merge(parts, tails):
    rows = parts[0].shape[0]
    stats = [read_stats(t) for t in tails]
    high = [functools.reduce(jnp.maximum, [s[h] for s in stats]) for h in range(2)]
    shares = [[jnp.exp(s[h] - high[h]) for s in stats] for h in range(2)]
    whole = [functools.reduce(jnp.add, shares[h]) for h in range(2)]
    lines = [w / whole[h] for h in range(2) for w in shares[h]]
    fill = jnp.zeros((128 - len(lines), rows), F32)
    table = jnp.concatenate(lines + [fill], axis=0).T
    halves = []
    for h in range(2):
        sides = [p[:, h * DV : (h + 1) * DV].astype(F32) for p in parts]
        first = h * len(parts)
        halves.append(sum(table[:, first + i : first + i + 1] * p for i, p in enumerate(sides)))
    return halves, [high[h] + jnp.log(whole[h]) for h in range(2)]


def chip_kernel(keep, got, *outs):
    for k, out in enumerate(outs):
        rows = out.shape[0] - TAIL
        halves, stats = merge(
            [keep[k, :rows, :], got[k, :rows, :]], [keep[k, rows:, :], got[k, rows:, :]]
        )
        for h, half in enumerate(halves):
            out[:rows, h * DV : (h + 1) * DV] = half.astype(BF16)
        out[rows:, :] = stored_stats(stats)


def heads_kernel(*refs):
    parts, out = refs[:-1], refs[-1]
    rows = out.shape[0]
    halves, _ = merge([p[:rows, :] for p in parts], [p[rows:, :] for p in parts])
    for h, half in enumerate(halves):
        out[:, h * DV : (h + 1) * DV] = half.astype(BF16)


def columns_kernel(w_hbm, out, wide, tall, sem):
    load = pltpu.make_async_copy(w_hbm, wide, sem)
    load.start()
    load.wait()
    step = 256
    for i in range(wide.shape[1] // step):
        tall[i * step : (i + 1) * step, :] = wide[:, i * step : (i + 1) * step].T
    share = out.shape[1] // NZ
    for z in range(NZ):
        for s in range(NXC):
            at = (z * NXC + s) * share
            out[s, z * share : (z + 1) * share, :] = tall[at : at + share, :]


def output_kernel(meta, weights, near, far, out):
    block = out.shape[0] // NX
    for place in range(NXC):

        @pl.when(meta[PLACE] == place)
        def _():
            for i in range(NX):
                part = slice(i * block, (i + 1) * block)
                mixed = None
                for s in range(NXC):
                    term = lax.dot_general(
                        weights[place ^ s, part, :],
                        (near, far)[s % NC][s // NC],
                        NT,
                        preferred_element_type=F32,
                    )
                    mixed = term if mixed is None else mixed + term
                out[part, :] = mixed.astype(BF16)


def after(x, *others):
    return lax.optimization_barrier((x, *others))[0]


def in_hbm(x):
    return pltpu.with_memory_space_constraint(x, pltpu.HBM)


def sent(x, axis, size, k):
    return lax.ppermute(x, axis, [(i, i ^ k) for i in range(size)])


def shifted(x, k):
    return lax.ppermute(x, "z", [(i, (i + k) % NZ) for i in range(NZ)])


def local(
    pool_latent,
    pool_rope,
    q_nope,
    q_rope,
    w_uk,
    w_uv,
    w_o,
    block_table,
    lengths,
    preempted,
    assignment,
):
    groups = lax.axis_size("grp")
    group = lax.axis_index("grp")
    column = lax.axis_index(DEV)
    place = lax.axis_index(XC)
    pages_dev, block, width = pool_latent.shape
    requests = preempted.shape[0]
    blocks = block_table.shape[1]
    per_group = requests // groups
    query_rows = q_nope.shape[0] // requests
    rows = per_group * query_rows
    pair = 2 * query_rows
    scale = 1.0 / math.sqrt(DN + DR)
    page_rows = block + DR // 2

    small = pltpu.CompilerParams(vmem_limit_bytes=16 << 20)
    ids = jnp.stack([group, column]).astype(jnp.int32)
    page_type = jax.ShapeDtypeStruct((page_rows, width), BF16)
    meta, copies, *packed = pl.pallas_call(
        functools.partial(prepare_kernel, groups=groups),
        out_shape=[
            jax.ShapeDtypeStruct((META,), jnp.int32),
            jax.ShapeDtypeStruct((NX, 3 * rows + 4 * width, DN), BF16),
        ]
        + [page_type] * groups,
        in_specs=[spec(SMEM)] + [spec(pltpu.HBM)] * 10,
        out_specs=[spec(SMEM)] + [spec(VMEM)] * (1 + groups),
        scratch_shapes=[
            SMEM(block_table.T.shape, jnp.int32),
            SMEM(lengths.shape, jnp.int32),
            SMEM(preempted.shape, jnp.int32),
            SMEM(assignment.shape, jnp.int32),
            VMEM(pool_latent.shape, BF16),
            VMEM(pool_rope.shape, BF16),
            pltpu.SemaphoreType.DMA((2,)),
            pltpu.SemaphoreType.DMA((per_group, 3)),
            pltpu.SemaphoreType.DMA((4,)),
            pltpu.SemaphoreType.DMA((NX, 4)),
        ],
        compiler_params=small,
        name="prepare",
    )(ids, *[in_hbm(a) for a in (block_table.T, lengths, preempted, assignment, pool_latent, pool_rope, q_nope, q_rope, w_uk, w_uv)])

    arrived = [packed[0]] + [
        lax.ppermute(packed[k], "grp", [(i, (i + k) % groups) for i in range(groups)])
        for k in range(1, groups)
    ]
    near_x = lax.all_to_all(copies, "x", split_axis=0, concat_axis=0)

    share = w_o.shape[1] // (NZ * NXC)
    w_cols = pl.pallas_call(
        columns_kernel,
        out_shape=jax.ShapeDtypeStruct((NXC, NZ * share, w_o.shape[0]), BF16),
        in_specs=[spec(pltpu.HBM)],
        out_specs=spec(VMEM),
        scratch_shapes=[
            VMEM(w_o.shape, BF16),
            VMEM(w_o.shape[::-1], BF16),
            pltpu.SemaphoreType.DMA,
        ],
        compiler_params=pltpu.CompilerParams(vmem_limit_bytes=24 << 20),
        name="columns",
    )(in_hbm(after(w_o, packed[0])))
    arrived, w_cols = lax.optimization_barrier((arrived, w_cols))

    half_page = jax.ShapeDtypeStruct((page_rows // 2, width), BF16)
    halves = pl.pallas_call(
        pick_kernel,
        out_shape=[half_page] * 2,
        in_specs=[spec(SMEM)] + [spec(VMEM)] * groups,
        out_specs=[spec(VMEM)] * 2,
        compiler_params=small,
        name="pick",
    )(meta, *arrived)

    below, above = [halves], [halves]
    for k in range(1, NZ // 2):
        below.append([shifted(h, 1) for h in below[-1]])
        above.append([shifted(h, -1) for h in above[-1]])
    middle = [shifted(below[-1][0], 1), shifted(above[-1][1], -1)]
    pages = [halves] + above[1:] + [middle] + below[:0:-1]

    far_x = sent(after(near_x, above[2], below[2]), "c", NC, 1)
    w_cols = after(w_cols, near_x)
    weights = lax.all_to_all(w_cols, XC, split_axis=0, concat_axis=0)

    query = pl.pallas_call(
        query_kernel,
        out_shape=jax.ShapeDtypeStruct((per_group, NXC * pair, width + 2 * DR), BF16),
        in_specs=[spec(SMEM)] + [spec(pl.ANY)] * 2,
        out_specs=spec(VMEM),
        scratch_shapes=[
            VMEM((NXC, 3 * rows + 2 * width, DN), BF16),
            pltpu.SemaphoreType.DMA((NXC,)),
        ],
        compiler_params=small,
        name="query",
    )(meta, in_hbm(near_x), in_hbm(far_x))

    half_type = jax.ShapeDtypeStruct((NX, rows + TAIL, 2 * DV), BF16)
    keep, send = pl.pallas_call(
        functools.partial(attention_kernel, scale=scale),
        out_shape=[half_type, half_type],
        in_specs=[spec(SMEM), spec(VMEM)] + [spec(pl.ANY)] * (2 + 2 * NZ),
        out_specs=[spec(VMEM)] * 2,
        scratch_shapes=[
            VMEM((per_group, NXC * pair, width), F32),
            VMEM((per_group, NXC * pair, 128), F32),
            VMEM((per_group, NXC * pair, 128), F32),
            VMEM((NZ, page_rows, width), BF16),
            VMEM((NXC, 2 * width, DV), BF16),
            pltpu.SemaphoreType.DMA((NZ, 2)),
            pltpu.SemaphoreType.DMA((NXC,)),
        ],
        compiler_params=pltpu.CompilerParams(vmem_limit_bytes=32 << 20),
        name="attention",
    )(meta, query, in_hbm(near_x), in_hbm(far_x), *[p[0] for p in pages], *[p[1] for p in pages])

    got = sent(send, "c", NC, 1)
    part_type = jax.ShapeDtypeStruct((rows + TAIL, 2 * DV), BF16)
    chip = pl.pallas_call(
        chip_kernel,
        out_shape=[part_type] * NX,
        in_specs=[spec(VMEM)] * 2,
        out_specs=[spec(VMEM)] * NX,
        compiler_params=small,
        name="chip",
    )(keep, got)
    heads = pl.pallas_call(
        heads_kernel,
        out_shape=jax.ShapeDtypeStruct((rows, 2 * DV), BF16),
        in_specs=[spec(VMEM)] * NX,
        out_specs=spec(VMEM),
        compiler_params=small,
        name="heads",
    )(chip[0], *[sent(chip[k], "x", NX, k) for k in range(1, NX)])
    heads, weights = lax.optimization_barrier((heads, weights))
    near = [heads] + [sent(heads, "x", NX, k) for k in range(1, NX)]
    near = jnp.stack(near)
    mixed = pl.pallas_call(
        output_kernel,
        out_shape=jax.ShapeDtypeStruct((NZ * share, rows), BF16),
        in_specs=[spec(SMEM)] + [spec(VMEM)] * 3,
        out_specs=spec(VMEM),
        compiler_params=small,
        name="output",
    )(meta, weights, near, sent(near, "c", NC, 1))
    mixed = lax.all_to_all(mixed, "z", split_axis=0, concat_axis=0, tiled=True)
    mixed = mixed.reshape(NZ, -1, rows).astype(F32).sum(axis=0)
    return mixed.T.astype(BF16)


def solution(mesh):
    split = Mesh(mesh.devices.reshape(mesh.shape["grp"], NZ, NX, NC), GRP_DEV)
    return jax.shard_map(
        local,
        mesh=split,
        in_specs=(
            P(GRP_DEV, None, None),
            P(GRP_DEV, None, None),
            P(None, DEV),
            P(None, DEV),
            P(None, DEV),
            P(None, DEV),
            P(DEV, None),
            P(),
            P(),
            P(),
            P(),
        ),
        out_specs=P("grp", DEV),
        check_vma=False,
    )
```

```python
import functools
import math

import jax
import jax.numpy as jnp
from jax import lax
from jax.experimental import pallas as pl
from jax.experimental.pallas import tpu as pltpu
from jax.sharding import Mesh
from jax.sharding import PartitionSpec as P

DR = 64
DN = 128
DV = 128
NEG = -1e30
LOG2E = math.log2(math.e)
NZ, NX, NC = 8, 4, 2
NXC = NX * NC
DEV = ("z", "x", "c")
GRP_DEV = ("grp", "z", "x", "c")
XC = ("x", "c")
SMEM = pltpu.SMEM
VMEM = pltpu.VMEM
F32 = jnp.float32
BF16 = jnp.bfloat16
NT = (((1,), (1,)), ((), ()))


def spec(space):
    return pl.BlockSpec(memory_space=space)


SEND, PICK, PLACE, SPOT, RANK, VALID, MEMBER, COUNT, SPARE = 0, 4, 5, 6, 8, 16, 24, 32, 40
META = 41
TAIL = 16


def fill_members(meta, ids, assignment):
    for i in range(SPARE):
        meta[i] = 0

    def one_request(i, carry):
        owner = assignment[i]
        rank = meta[COUNT + owner]
        meta[COUNT + owner] = rank + 1
        meta[jnp.where(owner == ids[0], MEMBER + rank, SPARE)] = i
        return carry

    lax.fori_loop(0, assignment.shape[0], one_request, 0)


def fill_table(meta, ids, table, lengths, preempted, assignment, *, groups, block, pages_dev):
    group, column = ids[0], ids[1]
    blocks = table.shape[0]
    columns = NZ * NXC
    me = group * columns + column
    place = column & (NXC - 1)
    plane = lax.shift_right_logical(column, NXC.bit_length() - 1)
    meta[PLACE] = place
    meta[SPOT] = lax.shift_right_logical(place, NC.bit_length() - 1)

    def one_request(i, carry):
        slot = preempted[i]
        owner = assignment[i]
        ahead = SEND + ((owner - group) & (groups - 1))
        for b in range(blocks):
            page = table[b, slot]
            holder = lax.shift_right_logical(page, pages_dev.bit_length() - 1)
            meta[jnp.where(holder == me, ahead, SPARE)] = page & (pages_dev - 1)

        return carry

    lax.fori_loop(0, preempted.shape[0], one_request, 0)

    def one_member(rank, carry):
        slot = preempted[meta[MEMBER + rank]]
        length = lengths[slot]
        for b in range(blocks):
            holder = lax.shift_right_logical(table[b, slot], pages_dev.bit_length() - 1)
            col = holder & (columns - 1)
            row = lax.shift_right_logical(holder, columns.bit_length() - 1)
            z = (lax.shift_right_logical(col, NXC.bit_length() - 1) - plane) & (NZ - 1)
            near = (col & (NXC - 1)) == place
            meta[jnp.where(near, RANK + z, SPARE)] = rank
            meta[jnp.where(near, VALID + z, SPARE)] = jnp.clip(length - b * block, 0, block)
            meta[jnp.where(col == column, PICK, SPARE)] = (group - row) & (groups - 1)

        return carry

    lax.fori_loop(0, preempted.shape[0] // groups, one_member, 0)


def prepare_kernel(ids, *refs, groups):
    tables_hbm, (latent_hbm, rope_hbm, q_nope, q_rope, w_uk, w_uv), rest = refs[:4], refs[4:10], refs[10:]
    meta, copies = rest[:2]
    outs = rest[2 : 2 + groups]
    table, lengths, preempted, assignment, latent, rope, sem, row_sem, table_sem, w_sem = rest[2 + groups :]
    tables = (table, lengths, preempted, assignment)
    pages_dev, block, _ = latent.shape
    half = rope.shape[1] // 2
    q_rows = q_nope.shape[0] // preempted.shape[0]
    depth = w_uk.shape[0]
    queries = copies.shape[1] - 4 * depth
    rows = queries // 3
    for_all = [
        pltpu.make_async_copy(
            w.at[:, pl.ds(h * DN, DN)],
            copies.at[k, pl.ds(queries + (2 * i + h) * depth, depth), :],
            w_sem.at[k, 2 * i + h],
        )
        for i, w in enumerate((w_uk, w_uv))
        for h in range(2)
        for k in range(copies.shape[0])
    ]
    loads = [
        pltpu.make_async_copy(latent_hbm, latent, sem.at[0]),
        pltpu.make_async_copy(rope_hbm, rope, sem.at[1]),
    ]
    first = [
        pltpu.make_async_copy(src, dst, table_sem.at[i])
        for i, (src, dst) in enumerate(zip(tables_hbm, tables))
    ]
    for load in first + loads + for_all:
        load.start()
    for load in first:
        load.wait()
    fill_members(meta, ids, assignment)
    moves = []
    for r in range(rows // q_rows):
        start = pl.multiple_of(meta[MEMBER + r] * q_rows, q_rows)
        for j in range(3):
            source = q_rope if j == 2 else q_nope.at[:, pl.ds(j * DN, DN)]
            moves.append(
                pltpu.make_async_copy(
                    source.at[pl.ds(start, q_rows), :],
                    copies.at[0, pl.ds(j * rows + r * q_rows, q_rows), :],
                    row_sem.at[r, j],
                )
            )
    for move in moves:
        move.start()
    fill_table(
        meta, ids, table, lengths, preempted, assignment,
        groups=groups, block=block, pages_dev=pages_dev,
    )
    for load in loads:
        load.wait()
    for k, out in enumerate(outs):
        page = meta[SEND + k]
        out[:block, :] = latent[page]
        out[block:, :block] = rope[page, :half, :]
        out[block:, block:] = rope[page, half:, :]
    for move in moves:
        move.wait()
    for k in range(1, copies.shape[0]):
        copies[k, :queries, :] = copies[0, :queries, :]
    for load in for_all:
        load.wait()


def pick_kernel(meta, *rest):
    sources, (first, second) = rest[:-2], rest[-2:]
    half = first.shape[0]
    for k, source in enumerate(sources):

        @pl.when(meta[PICK] == k)
        def _():
            first[...] = source[:half, :]
            second[...] = source[half:, :]


def placed(near, far, s, meta):
    return (near, far)[s % NC].at[meta[SPOT] ^ (s // NC)]


def query_kernel(meta, near, far, out, got, sem):
    per_group = out.shape[0]
    pair = out.shape[1] // NXC
    q_rows = pair // 2
    width = out.shape[2] - 2 * DR
    rows = per_group * q_rows
    loads = [
        pltpu.make_async_copy(
            placed(near, far, s, meta).at[pl.ds(0, got.shape[1]), :], got.at[s], sem.at[s]
        )
        for s in range(NXC)
    ]
    for load in loads:
        load.start()
    lane = lax.broadcasted_iota(jnp.int32, (rows, 2 * DR), 1)
    for s in range(NXC):
        loads[s].wait()
        hi = got[s, 2 * rows : 3 * rows, :]
        for h in range(2):
            live = (lane >= h * DR) & (lane < (h + 1) * DR)
            tail = jnp.where(live, hi, jnp.zeros_like(hi))
            key = 3 * rows + h * width
            lat = lax.dot_general(
                got[s, h * rows : (h + 1) * rows, :],
                got[s, key : key + width, :],
                NT,
                preferred_element_type=F32,
            ).astype(BF16)
            lo = s * pair + h * q_rows
            out[:, lo : lo + q_rows, :width] = lat.reshape(per_group, q_rows, width)
            out[:, lo : lo + q_rows, width:] = tail.reshape(per_group, q_rows, 2 * DR)


def three_parts(x):
    high = x.astype(BF16).astype(F32)
    rest = x - high
    middle = rest.astype(BF16).astype(F32)
    return [high, middle, rest - middle]


def stored_stats(stats):
    rows = [p for s in stats for p in three_parts(s)]
    fill = jnp.zeros((TAIL - len(rows), rows[0].shape[1]), F32)
    return jnp.concatenate(rows + [fill], axis=0).astype(BF16)


def read_stats(tail):
    tail = tail.astype(F32)
    return [tail[3 * h : 3 * h + 1] + tail[3 * h + 1 : 3 * h + 2] + tail[3 * h + 2 : 3 * h + 3] for h in range(2)]


def attention_kernel(meta, query, *rest, scale):
    near, far, firsts, seconds = *rest[:2], rest[2 : 2 + NZ], rest[2 + NZ : -9]
    keep, send, acc, top, total, pages, w_uv, sem, w_sem = rest[-9:]
    per_group, heads_rows, width = acc.shape
    q_rows = heads_rows // (2 * NXC)
    rows = per_group * q_rows
    block = pages.shape[1] * 8 // 9

    middle = NZ // 2
    order = [0] + [z for k in range(1, middle) for z in (k, NZ - k)] + [middle]
    split = pages.shape[1] // 2
    loads = [
        [
            pltpu.make_async_copy(firsts[z], pages.at[i, pl.ds(0, split), :], sem.at[i, 0]),
            pltpu.make_async_copy(seconds[z], pages.at[i, pl.ds(split, split), :], sem.at[i, 1]),
        ]
        for i, z in enumerate(order)
    ]
    loads_w = [
        pltpu.make_async_copy(
            placed(near, far, s, meta).at[pl.ds(near.shape[1] - 2 * width, 2 * width), :],
            w_uv.at[s],
            w_sem.at[s],
        )
        for s in range(NXC)
    ]
    for load in [load for pair in loads for load in pair] + loads_w:
        load.start()

    ranks = [meta[RANK + z] for z in order]
    valids = [meta[VALID + z] for z in order]
    for r in range(per_group):
        held = [(ranks[z] == r) & (valids[z] > 0) for z in range(NZ)]

        @pl.when(jnp.logical_not(functools.reduce(jnp.logical_or, held)))
        def _():
            acc[r] = jnp.zeros(acc.shape[1:], F32)
            top[r] = jnp.full(top.shape[1:], NEG, F32)
            total[r] = jnp.zeros(total.shape[1:], F32)

    def one_page(i, r, valid, first):
        latent = pages[i, :block, :]
        tail = pages[i, block:, :]
        rope = jnp.concatenate([tail[:, :block], tail[:, block:]], axis=0)
        rope = jnp.concatenate([rope, rope], axis=0)
        q = query[r]
        score = lax.dot_general(q[:, :width], latent, NT, preferred_element_type=F32)
        score = score + jnp.dot(q[:, width:], rope, preferred_element_type=F32)
        token = lax.broadcasted_iota(jnp.int32, score.shape, 1)
        score = jnp.where(token < valid, score * (scale * LOG2E), NEG)
        new = jnp.max(score, axis=1, keepdims=True)
        if not first:
            old = top[r][:, :1]
            new = jnp.maximum(old, new)
            fade = jnp.exp2(old - new)
        expo = jnp.exp2(score - new)
        weight = jnp.sum(expo, axis=1, keepdims=True)
        value = jnp.dot(expo.astype(BF16), latent, preferred_element_type=F32)
        top[r] = jnp.broadcast_to(new, top.shape[1:])
        if first:
            total[r] = jnp.broadcast_to(weight, total.shape[1:])
            acc[r] = value
        else:
            total[r] = total[r] * fade + weight
            acc[r] = acc[r] * fade + value

    def one_step(i, carry):
        z = jnp.where(i & 1 == 1, (i + 1) // 2, (NZ - i // 2) & (NZ - 1))
        r, valid = meta[RANK + z], meta[VALID + z]
        earlier = [(p < i) & (ranks[p] == r) & (valids[p] > 0) for p in range(NZ)]
        again = functools.reduce(jnp.logical_or, earlier)

        @pl.when((valid > 0) & jnp.logical_not(again))
        def _():
            one_page(i, r, valid, True)

        @pl.when((valid > 0) & again)
        def _():
            one_page(i, r, valid, False)

        return carry

    for lo, hi in ((0, 2), (2, NZ)):
        for load in [load for pair in loads[lo:hi] for load in pair]:
            load.wait()
        lax.fori_loop(lo, hi, one_step, 0)

    lane = lax.broadcasted_iota(jnp.int32, (rows, total.shape[2]), 1)
    weights = jnp.zeros(lane.shape, F32)
    highs = jnp.full(lane.shape, NEG, F32)
    for j in range(2 * NXC):
        part = slice(j * q_rows, (j + 1) * q_rows)
        weights = jnp.where(lane == j, total[:, part, :].reshape(lane.shape), weights)
        highs = jnp.where(lane == j, top[:, part, :].reshape(lane.shape), highs)
    some = weights > 0.0
    safe = jnp.where(some, weights, 1.0)
    shares = 1.0 / safe
    stats = jnp.where(some, highs * (1.0 / LOG2E) + jnp.log(safe), NEG).T
    for s in range(NXC):
        out = keep if s % 2 == 0 else send
        loads_w[s].wait()
        for h in range(2):
            j = 2 * s + h
            value = acc[:, j * q_rows : (j + 1) * q_rows, :].reshape(rows, width)
            value = (value * shares[:, j : j + 1]).astype(BF16)
            head = jnp.dot(value, w_uv[s, h * width : (h + 1) * width, :], preferred_element_type=F32)
            out[s // 2, :rows, h * DV : (h + 1) * DV] = head.astype(BF16)
        out[s // 2, rows:, :] = stored_stats([stats[2 * s + h : 2 * s + h + 1, :] for h in range(2)])


def merge(parts, tails):
    rows = parts[0].shape[0]
    stats = [read_stats(t) for t in tails]
    high = [functools.reduce(jnp.maximum, [s[h] for s in stats]) for h in range(2)]
    shares = [[jnp.exp(s[h] - high[h]) for s in stats] for h in range(2)]
    whole = [functools.reduce(jnp.add, shares[h]) for h in range(2)]
    lines = [w / whole[h] for h in range(2) for w in shares[h]]
    fill = jnp.zeros((128 - len(lines), rows), F32)
    table = jnp.concatenate(lines + [fill], axis=0).T
    halves = []
    for h in range(2):
        sides = [p[:, h * DV : (h + 1) * DV].astype(F32) for p in parts]
        first = h * len(parts)
        halves.append(sum(table[:, first + i : first + i + 1] * p for i, p in enumerate(sides)))
    return halves, [high[h] + jnp.log(whole[h]) for h in range(2)]


def chip_kernel(keep, got, *outs):
    for k, out in enumerate(outs):
        rows = out.shape[0] - TAIL
        halves, stats = merge(
            [keep[k, :rows, :], got[k, :rows, :]], [keep[k, rows:, :], got[k, rows:, :]]
        )
        for h, half in enumerate(halves):
            out[:rows, h * DV : (h + 1) * DV] = half.astype(BF16)
        out[rows:, :] = stored_stats(stats)


def heads_kernel(*refs):
    parts, out = refs[:-1], refs[-1]
    rows = out.shape[0]
    halves, _ = merge([p[:rows, :] for p in parts], [p[rows:, :] for p in parts])
    for h, half in enumerate(halves):
        out[:, h * DV : (h + 1) * DV] = half.astype(BF16)


def columns_kernel(w_hbm, out, wide, tall, sem):
    load = pltpu.make_async_copy(w_hbm, wide, sem)
    load.start()
    load.wait()
    step = 256
    for i in range(wide.shape[1] // step):
        tall[i * step : (i + 1) * step, :] = wide[:, i * step : (i + 1) * step].T
    share = out.shape[1] // NZ
    for z in range(NZ):
        for s in range(NXC):
            at = (z * NXC + s) * share
            out[s, z * share : (z + 1) * share, :] = tall[at : at + share, :]


def output_kernel(meta, weights, near, far, out):
    block = out.shape[0] // NX
    spot = meta[SPOT]
    for c, sides in enumerate(((near, far), (far, near))):

        @pl.when((meta[PLACE] & (NC - 1)) == c)
        def _():
            heads = [sides[s % NC][spot ^ (s // NC)] for s in range(NXC)]
            for i in range(NX):
                part = slice(i * block, (i + 1) * block)
                mixed = None
                for s in range(NXC):
                    term = lax.dot_general(
                        weights[s, part, :], heads[s], NT, preferred_element_type=F32
                    )
                    mixed = term if mixed is None else mixed + term
                out[part, :] = mixed.astype(BF16)


def after(x, *others):
    return lax.optimization_barrier((x, *others))[0]


def in_hbm(x):
    return pltpu.with_memory_space_constraint(x, pltpu.HBM)


def sent(x, axis, size, k):
    return lax.ppermute(x, axis, [(i, i ^ k) for i in range(size)])


def shifted(x, k):
    return lax.ppermute(x, "z", [(i, (i + k) % NZ) for i in range(NZ)])


def local(
    pool_latent,
    pool_rope,
    q_nope,
    q_rope,
    w_uk,
    w_uv,
    w_o,
    block_table,
    lengths,
    preempted,
    assignment,
):
    groups = lax.axis_size("grp")
    group = lax.axis_index("grp")
    column = lax.axis_index(DEV)
    place = lax.axis_index(XC)
    pages_dev, block, width = pool_latent.shape
    requests = preempted.shape[0]
    blocks = block_table.shape[1]
    per_group = requests // groups
    query_rows = q_nope.shape[0] // requests
    rows = per_group * query_rows
    pair = 2 * query_rows
    scale = 1.0 / math.sqrt(DN + DR)
    page_rows = block + DR // 2

    small = pltpu.CompilerParams(vmem_limit_bytes=16 << 20)
    ids = jnp.stack([group, column]).astype(jnp.int32)
    page_type = jax.ShapeDtypeStruct((page_rows, width), BF16)
    meta, copies, *packed = pl.pallas_call(
        functools.partial(prepare_kernel, groups=groups),
        out_shape=[
            jax.ShapeDtypeStruct((META,), jnp.int32),
            jax.ShapeDtypeStruct((NX, 3 * rows + 4 * width, DN), BF16),
        ]
        + [page_type] * groups,
        in_specs=[spec(SMEM)] + [spec(pltpu.HBM)] * 10,
        out_specs=[spec(SMEM)] + [spec(VMEM)] * (1 + groups),
        scratch_shapes=[
            SMEM(block_table.T.shape, jnp.int32),
            SMEM(lengths.shape, jnp.int32),
            SMEM(preempted.shape, jnp.int32),
            SMEM(assignment.shape, jnp.int32),
            VMEM(pool_latent.shape, BF16),
            VMEM(pool_rope.shape, BF16),
            pltpu.SemaphoreType.DMA((2,)),
            pltpu.SemaphoreType.DMA((per_group, 3)),
            pltpu.SemaphoreType.DMA((4,)),
            pltpu.SemaphoreType.DMA((NX, 4)),
        ],
        compiler_params=small,
        name="prepare",
    )(ids, *[in_hbm(a) for a in (block_table.T, lengths, preempted, assignment, pool_latent, pool_rope, q_nope, q_rope, w_uk, w_uv)])

    arrived = [packed[0]] + [
        lax.ppermute(packed[k], "grp", [(i, (i + k) % groups) for i in range(groups)])
        for k in range(1, groups)
    ]
    near_x = lax.all_to_all(copies, "x", split_axis=0, concat_axis=0)

    share = w_o.shape[1] // (NZ * NXC)
    w_cols = pl.pallas_call(
        columns_kernel,
        out_shape=jax.ShapeDtypeStruct((NXC, NZ * share, w_o.shape[0]), BF16),
        in_specs=[spec(pltpu.HBM)],
        out_specs=spec(VMEM),
        scratch_shapes=[
            VMEM(w_o.shape, BF16),
            VMEM(w_o.shape[::-1], BF16),
            pltpu.SemaphoreType.DMA,
        ],
        compiler_params=pltpu.CompilerParams(vmem_limit_bytes=24 << 20),
        name="columns",
    )(in_hbm(after(w_o, packed[0])))
    arrived, w_cols = lax.optimization_barrier((arrived, w_cols))

    half_page = jax.ShapeDtypeStruct((page_rows // 2, width), BF16)
    halves = pl.pallas_call(
        pick_kernel,
        out_shape=[half_page] * 2,
        in_specs=[spec(SMEM)] + [spec(VMEM)] * groups,
        out_specs=[spec(VMEM)] * 2,
        compiler_params=small,
        name="pick",
    )(meta, *arrived)

    below, above = [halves], [halves]
    for k in range(1, NZ // 2):
        below.append([shifted(h, 1) for h in below[-1]])
        above.append([shifted(h, -1) for h in above[-1]])
    middle = [shifted(below[-1][0], 1), shifted(above[-1][1], -1)]
    pages = [halves] + above[1:] + [middle] + below[:0:-1]

    far_x = sent(after(near_x, above[2], below[2]), "c", NC, 1)
    w_cols = after(w_cols, near_x)
    weights = lax.all_to_all(w_cols, XC, split_axis=0, concat_axis=0)

    query = pl.pallas_call(
        query_kernel,
        out_shape=jax.ShapeDtypeStruct((per_group, NXC * pair, width + 2 * DR), BF16),
        in_specs=[spec(SMEM)] + [spec(pl.ANY)] * 2,
        out_specs=spec(VMEM),
        scratch_shapes=[
            VMEM((NXC, 3 * rows + 2 * width, DN), BF16),
            pltpu.SemaphoreType.DMA((NXC,)),
        ],
        compiler_params=small,
        name="query",
    )(meta, in_hbm(near_x), in_hbm(far_x))

    half_type = jax.ShapeDtypeStruct((NX, rows + TAIL, 2 * DV), BF16)
    keep, send = pl.pallas_call(
        functools.partial(attention_kernel, scale=scale),
        out_shape=[half_type, half_type],
        in_specs=[spec(SMEM), spec(VMEM)] + [spec(pl.ANY)] * (2 + 2 * NZ),
        out_specs=[spec(VMEM)] * 2,
        scratch_shapes=[
            VMEM((per_group, NXC * pair, width), F32),
            VMEM((per_group, NXC * pair, 128), F32),
            VMEM((per_group, NXC * pair, 128), F32),
            VMEM((NZ, page_rows, width), BF16),
            VMEM((NXC, 2 * width, DV), BF16),
            pltpu.SemaphoreType.DMA((NZ, 2)),
            pltpu.SemaphoreType.DMA((NXC,)),
        ],
        compiler_params=pltpu.CompilerParams(vmem_limit_bytes=32 << 20),
        name="attention",
    )(meta, query, in_hbm(near_x), in_hbm(far_x), *[p[0] for p in pages], *[p[1] for p in pages])

    got = sent(send, "c", NC, 1)
    part_type = jax.ShapeDtypeStruct((rows + TAIL, 2 * DV), BF16)
    chip = pl.pallas_call(
        chip_kernel,
        out_shape=[part_type] * NX,
        in_specs=[spec(VMEM)] * 2,
        out_specs=[spec(VMEM)] * NX,
        compiler_params=small,
        name="chip",
    )(keep, got)
    heads = pl.pallas_call(
        heads_kernel,
        out_shape=jax.ShapeDtypeStruct((rows, 2 * DV), BF16),
        in_specs=[spec(VMEM)] * NX,
        out_specs=spec(VMEM),
        compiler_params=small,
        name="heads",
    )(chip[0], *[sent(chip[k], "x", NX, k) for k in range(1, NX)])
    heads, weights = lax.optimization_barrier((heads, weights))
    near = [heads] + [sent(heads, "x", NX, k) for k in range(1, NX)]
    near = jnp.stack(near)
    mixed = pl.pallas_call(
        output_kernel,
        out_shape=jax.ShapeDtypeStruct((NZ * share, rows), BF16),
        in_specs=[spec(SMEM)] + [spec(VMEM)] * 3,
        out_specs=spec(VMEM),
        compiler_params=small,
        name="output",
    )(meta, weights, near, sent(near, "c", NC, 1))
    mixed = lax.all_to_all(mixed, "z", split_axis=0, concat_axis=0, tiled=True)
    mixed = mixed.reshape(NZ, -1, rows).astype(F32).sum(axis=0)
    return mixed.T.astype(BF16)


def solution(mesh):
    split = Mesh(mesh.devices.reshape(mesh.shape["grp"], NZ, NX, NC), GRP_DEV)
    return jax.shard_map(
        local,
        mesh=split,
        in_specs=(
            P(GRP_DEV, None, None),
            P(GRP_DEV, None, None),
            P(None, DEV),
            P(None, DEV),
            P(None, DEV),
            P(None, DEV),
            P(DEV, None),
            P(),
            P(),
            P(),
            P(),
        ),
        out_specs=P("grp", DEV),
        check_vma=False,
    )
```
